32 devices in a mesh: seq: 8 (over z, x), fsdp: 4 (over y, core).
Axes of the slice: x: 2, y: 2, z: 4, core: 2. Of those that a mesh axis runs over, the one named last changes fastest.
Arguments:
- tokens: bfloat16 [4, 2048, 2048], P('fsdp', 'seq'), may hold values from -6 to 6
- routes: int32 [4, 2048, 8], P('fsdp', 'seq'), may hold values from 0 to 31, all different within a row; in each aligned block of 256 rows (0 to 255, 256 to 511, ..., all dimensions but the last counted through in order) at most 96 rows name the same one
- route_weights: float32 [4, 2048, 8], P('fsdp', 'seq'), may hold values from 0.05 to 0.5
- cotangent: bfloat16 [4, 2048, 2048], P('fsdp', 'seq'), may hold values from -6 to 6
- attn_gain: bfloat16 [2048], P('fsdp'), may hold values from 0.099609375 to 1.8984375
- query_gain: bfloat16 [2048], P('fsdp'), may hold values from 0.099609375 to 1.8984375
- key_gain: bfloat16 [2048], P('fsdp'), may hold values from 0.099609375 to 1.8984375
- ffn_gain: bfloat16 [2048], P('fsdp'), may hold values from 0.099609375 to 1.8984375
- w_query: bfloat16 [2048, 2048], P('fsdp'), may hold values from -0.125 to 0.125
- w_key: bfloat16 [2048, 2048], P('fsdp'), may hold values from -0.125 to 0.125
- w_value: bfloat16 [2048, 2048], P('fsdp'), may hold values from -0.125 to 0.125
- w_out: bfloat16 [2048, 2048], P('fsdp'), may hold values from -2 to 2
- w_gate: bfloat16 [2048, 32, 1024], P('fsdp', 'seq'), may hold values from -0.125 to 0.125
- w_up: bfloat16 [2048, 32, 1024], P('fsdp', 'seq'), may hold values from -0.125 to 0.125
- w_down: bfloat16 [2048, 32, 1024], P('fsdp', 'seq'), may hold values from -0.5 to 0.5
Outputs:
- block_out: bfloat16 [4, 2048, 2048], P('fsdp', 'seq')
- tokens_grad: float32 [4, 2048, 2048], P('fsdp', 'seq')
- attn_gain_grad: float32 [2048], P(('seq', 'fsdp'))
- query_gain_grad: float32 [2048], P(('seq', 'fsdp'))
- key_gain_grad: float32 [2048], P(('seq', 'fsdp'))
- ffn_gain_grad: float32 [2048], P(('seq', 'fsdp'))
- w_query_grad: float32 [2048, 2048], P(('seq', 'fsdp'))
- w_key_grad: float32 [2048, 2048], P(('seq', 'fsdp'))
- w_value_grad: float32 [2048, 2048], P(('seq', 'fsdp'))
- w_out_grad: float32 [2048, 2048], P(('seq', 'fsdp'))
- w_gate_grad: float32 [2048, 32, 1024], P('fsdp', 'seq')
- w_up_grad: float32 [2048, 32, 1024], P('fsdp', 'seq')
- w_down_grad: float32 [2048, 32, 1024], P('fsdp', 'seq')
The draws below stay inside these ranges and needn't reach their ends.
Inputs may be any that keep to these rules, and one draw needn't show every extreme that they name: `routes`: the 8 experts of a token differ. Among the 256 tokens of one device (aligned blocks in sequence order) no expert is named more than 96 times, and in every draw some expert is named exactly 96 times there.
All inputs are finite; a program needn't handle non-finite values.
Results may differ from the reference program's by a relative error of at most 0.017.
Values may be sent and summed in bfloat16 or wider, within the bound.
A program may use at most 448 MiB of HBM per device.

```python
import math
import jax
import jax.numpy as jnp
import numpy as np
from jax import lax

D = 2048
H = 16
FF = 1024
TOP = 8
TOK_DEV = 256
DH = 128
EXPERTS = 32
LEN = 2048
SEQS = 4
CAP = 96
N_SEQ = 8


def level_of(rng, dims, cuts, least, high):
    def one(axis_at, parts):
        heights = jax.random.uniform(jax.random.fold_in(jax.random.fold_in(rng, 6), axis_at), (parts,), jnp.float32, least / len(cuts), high / len(cuts))
        return jnp.repeat(jnp.exp(heights), dims[axis_at] // parts).reshape((-1,) + (1,) * (len(dims) - axis_at - 1))

    loudness = one(*cuts[0])
    for cut in cuts[1:]:
        loudness = loudness * one(*cut)
    return loudness


def deal_out(own_key, own, number, rows, amount, top, bound, skew):
    sequence = jax.random.permutation(own_key, amount)
    crowded, usual = load_shares(amount, rows * top, bound, skew, True), load_shares(amount, rows * top, bound, skew, False)
    places = jnp.arange(amount)

    def named(lengths, rotation):
        used = int((lengths > 0).sum())
        fixed = max(1, used // 4)
        passed = fixed + (places - fixed + rotation * (used - fixed)) % max(1, amount - fixed)
        return jnp.zeros((amount,), jnp.int32).at[sequence[jnp.where(places < fixed, places, passed)]].set(jnp.asarray(lengths, jnp.int32))

    lengths = jnp.where(number % 4 == 0, named(crowded, number // 4), named(usual, number - number // 4 - 1))
    mixed = jax.random.permutation(jax.random.fold_in(own, 3), amount)
    giver, taker = mixed[0:amount // 2 * 2:2], mixed[1:amount // 2 * 2:2]
    slack = jnp.minimum(lengths[giver] - 1, bound - lengths[taker]) // 2
    slack = jnp.where((giver == sequence[0]) | (taker == sequence[0]) | (lengths[taker] == 0), 0, jnp.maximum(slack, 0))
    passed = jax.random.randint(jax.random.fold_in(own, 4), (amount // 2,), 0, 1 << 20) % (slack + 1)
    lengths = lengths.at[giver].add(-passed).at[taker].add(passed)
    items = jnp.searchsorted(jnp.cumsum(lengths), jnp.arange(rows * top), side="right").astype(jnp.int32)
    grid = items.reshape(top, rows).T
    grid = grid[jax.random.permutation(jax.random.fold_in(own, 1), rows)]
    rotation = jax.random.randint(jax.random.fold_in(own, 2), (rows, 1), 0, top)
    return jnp.take_along_axis(grid, (jnp.arange(top)[None, :] + rotation) % top, axis=1)


def load_shares(amount, total, bound, skew, full):
    loads = [(1 << 20) // math.isqrt(standing ** skew) + 1 for standing in range(1, amount + 1)]
    largest = bound if full else min(bound, max(-(-total // amount), total * loads[0] // sum(loads)))
    least = 1 if total - largest >= amount - 1 else 0
    holding, spare = [largest] + [least] * (amount - 1), total - largest - least * (amount - 1)
    while spare > 0:
        movable = [i for i in range(1, amount) if holding[i] < largest] or [i for i in range(1, amount) if holding[i] < bound]
        pool, budget = sum([loads[i] for i in movable]), spare
        for i in movable:
            addition = min(bound - holding[i], max(1, budget * loads[i] // pool), spare)
            holding[i] = holding[i] + addition
            spare = spare - addition
    return np.array(holding)


def bell_draw(rng, shape, width, most, cuts=(), held_as=jnp.bfloat16):
    result = jax.random.normal(rng, shape, jnp.float32) * width
    if len(cuts) > 0:
        result = level_of(rng, shape, cuts, -0.22, 0.18) * result
    return jnp.clip(result, min=-most, max=most).astype(held_as)


def setup_inputs(seed: int = 0) -> dict:
    arg_keys = jax.random.split(jax.random.key(seed), 16)
    tokens = bell_draw(arg_keys[0], (SEQS, LEN, D), 1.0, 6.0, ((0, 4), (1, 8)))
    routes_keys = jax.random.split(jax.random.fold_in(arg_keys[1], 1), SEQS * LEN // TOK_DEV)
    routes_turns = jax.random.permutation(jax.random.fold_in(arg_keys[1], 3), SEQS * LEN // TOK_DEV)
    routes = jax.vmap(lambda own, number: deal_out(jax.random.fold_in(arg_keys[1], 2), own, number, TOK_DEV, EXPERTS, TOP, CAP, 2))(routes_keys, routes_turns).reshape((SEQS, LEN, TOP))
    route_weights = jnp.clip(jnp.exp(math.log(0.5) - 2.3025851 * jax.random.uniform(arg_keys[2], (SEQS, LEN, TOP), jnp.float32) ** level_of(arg_keys[2], (SEQS, LEN, TOP), ((0, 4), (1, 8)), -0.2, 0.2)), 0.05, 0.5)
    cotangent = bell_draw(arg_keys[3], (SEQS, LEN, D), 1.0, 6.0, ((0, 4), (1, 8)))
    attn_gain = jnp.clip(1.0 + 0.18 * jax.random.normal(arg_keys[4], (D,), jnp.float32), 0.099609375, 1.8984375).astype(jnp.bfloat16)
    query_gain = jnp.clip(1.0 + 0.18 * jax.random.normal(arg_keys[5], (D,), jnp.float32), 0.099609375, 1.8984375).astype(jnp.bfloat16)
    key_gain = jnp.clip(1.0 + 0.18 * jax.random.normal(arg_keys[6], (D,), jnp.float32), 0.099609375, 1.8984375).astype(jnp.bfloat16)
    ffn_gain = jnp.clip(1.0 + 0.18 * jax.random.normal(arg_keys[7], (D,), jnp.float32), 0.099609375, 1.8984375).astype(jnp.bfloat16)
    w_query = bell_draw(arg_keys[8], (D, D), D ** -0.5, 0.125, ((0, 4),))
    w_key = bell_draw(arg_keys[9], (D, D), D ** -0.5, 0.125, ((0, 4),))
    w_value = bell_draw(arg_keys[10], (D, D), D ** -0.5, 0.125, ((0, 4),))
    w_out = bell_draw(arg_keys[11], (D, D), (max(1, D // 256)) ** -0.5, 2.0, ((0, 4),))
    w_gate = bell_draw(arg_keys[12], (D, EXPERTS, FF), D ** -0.5, 0.125, ((0, 4), (1, 8)))
    w_up = bell_draw(arg_keys[13], (D, EXPERTS, FF), D ** -0.5, 0.125, ((0, 4), (1, 8)))
    w_down = bell_draw(arg_keys[14], (D, EXPERTS, FF), (max(1, FF // 8)) ** -0.5, 0.5, ((0, 4), (1, 8)))
    return {"tokens": tokens, "routes": routes, "route_weights": route_weights, "cotangent": cotangent, "attn_gain": attn_gain, "query_gain": query_gain, "key_gain": key_gain, "ffn_gain": ffn_gain, "w_query": w_query, "w_key": w_key, "w_value": w_value, "w_out": w_out, "w_gate": w_gate, "w_up": w_up, "w_down": w_down}


@jax.custom_vjp
def low(v):
    return lax.optimization_barrier(v.astype(jnp.bfloat16)).astype(jnp.float32)

@jax.custom_vjp
def low_back(v):
    return v

def low_keep(v):
    return (low(v), None)

def low_pass(kept, grad):
    return (grad,)

def back_keep(v):
    return (v, None)

def back_low(kept, grad):
    return (low(grad),)
low.defvjp(low_keep, low_pass)
low_back.defvjp(back_keep, back_low)
epsilon = 1e-05
highest = lax.Precision.HIGHEST

def inverse_norm(values):
    return lax.rsqrt(lax.optimization_barrier(jnp.mean(values * values, axis=-1, keepdims=True)) + epsilon)

def rope_tables(positions, head_dim):
    half = head_dim // 2
    frequency = jnp.power(10000.0, -2.0 * jnp.arange(half, dtype=jnp.float32) / head_dim)
    angle = positions.astype(jnp.float32)[:, None] * frequency[None, :]
    return (jnp.cos(angle)[:, None, :], jnp.sin(angle)[:, None, :])

def rotate(values, cosine, sine):
    half = values.shape[-1] // 2
    first = values[..., :half]
    second = values[..., half:]
    return jnp.concatenate([first * cosine - second * sine, second * cosine + first * sine], axis=-1)

def one_sequence(params, inputs, seq_routes, seq_weights):
    w_query, w_key, w_value, w_out, gain_attn, gain_query, gain_key, gain_ffn, w_gate, w_up, w_down = params
    seq_length = inputs.shape[0]
    normed = low(inputs * inverse_norm(inputs) * gain_attn)
    query_proj = low_back(jnp.dot(normed, w_query, precision=highest))
    key_proj = low_back(jnp.dot(normed, w_key, precision=highest))
    value_proj = jnp.dot(normed, w_value, precision=highest)
    query_normed = query_proj * inverse_norm(query_proj) * gain_query
    key_normed = key_proj * inverse_norm(key_proj) * gain_key
    cosine, sine = rope_tables(jnp.arange(seq_length, dtype=jnp.int32), DH)
    queries = low_back(low(rotate(query_normed.reshape(seq_length, H, DH), cosine, sine)))
    keys = low_back(low(rotate(key_normed.reshape(seq_length, H, DH), cosine, sine)))
    values = low_back(low(value_proj.reshape(seq_length, H, DH)))
    raw_scores = low_back(jnp.einsum('qhd,khd->hqk', queries, keys, precision=highest))
    scores = raw_scores * DH ** (-0.5)
    positions = jnp.arange(seq_length, dtype=jnp.int32)
    causal = positions[:, None] >= positions[None, :]
    scores = jnp.where(causal[None], scores, -1e+30)
    probs = low(jax.nn.softmax(scores, axis=-1))
    context = low_back(low(jnp.einsum('hqk,khd->qhd', probs, values, precision=highest))).reshape(seq_length, D)
    mid = inputs + low_back(jnp.dot(context, w_out, precision=highest))
    ffn_in = low(mid * inverse_norm(mid) * gain_ffn)
    experts = w_gate.shape[1]
    slots_per = N_SEQ * CAP
    flat_routes = seq_routes.reshape(-1).astype(jnp.int32)
    count = flat_routes.shape[0]
    one_hot = (flat_routes[:, None] == jnp.arange(experts, dtype=jnp.int32)[None, :]).astype(jnp.int32)
    running = jnp.cumsum(one_hot, axis=0).astype(jnp.int32) - 1
    rank = lax.optimization_barrier(jnp.sum(one_hot * running, axis=1)).astype(jnp.int32)
    slots = (flat_routes * slots_per + rank).astype(jnp.int32)
    owner = jnp.zeros((experts * slots_per,), jnp.int32).at[slots].set(jnp.arange(count, dtype=jnp.int32) // TOP)
    filled = jnp.zeros((experts * slots_per,), ffn_in.dtype).at[slots].set(1.0)
    expert_rows = low_back(ffn_in[owner] * filled[:, None]).reshape(experts, slots_per, D)
    gate = low_back(jnp.einsum('ecd,def->ecf', expert_rows, w_gate, precision=highest))
    up = low_back(jnp.einsum('ecd,def->ecf', expert_rows, w_up, precision=highest))
    hidden = low(jax.nn.silu(gate) * up)
    expert_out = low_back(low(jnp.einsum('ecf,def->ecd', hidden, w_down, precision=highest)))
    picked = expert_out.reshape(experts * slots_per, D)[slots].reshape(seq_length, TOP, D)
    ffn = lax.optimization_barrier(jnp.sum(picked * seq_weights[:, :, None], axis=1))
    return mid + ffn

def reference(tokens, routes, route_weights, cotangent, attn_gain, query_gain, key_gain, ffn_gain, w_query, w_key, w_value, w_out, w_gate, w_up, w_down):
    params = tuple((item.astype(jnp.float32) for item in (w_query, w_key, w_value, w_out, attn_gain, query_gain, key_gain, ffn_gain, w_gate, w_up, w_down)))
    inputs = tokens.astype(jnp.float32)
    mixing = route_weights.astype(jnp.float32)

    def forward(layer_in, weights):

        def step(carry, item):
            seq_in, seq_routes, seq_weights = item
            return (carry, jax.checkpoint(one_sequence)(weights, seq_in, seq_routes, seq_weights))
        unused, outs = lax.scan(step, jnp.zeros((), jnp.float32), (layer_in, routes, mixing))
        return outs
    outs, pullback = jax.vjp(forward, inputs, params)
    input_grad, param_grads = pullback(cotangent.astype(jnp.float32))
    g_query, g_key, g_value, g_out, g_attn, g_qgain, g_kgain, g_ffn, g_gate, g_up, g_down = param_grads
    return (outs.astype(jnp.bfloat16), input_grad, g_attn, g_qgain, g_kgain, g_ffn, g_query, g_key, g_value, g_out, g_gate, g_up, g_down)
```

```python
import functools
import jax
import jax.numpy as jnp
from jax import lax
from jax.experimental import pallas as pl
from jax.experimental.pallas import tpu as pltpu
from jax.sharding import PartitionSpec as P

MESH = pl.DeviceIdType.MESH
ANY = pl.ANY


def greet(peers):
    barrier = pltpu.get_barrier_semaphore()
    for peer in peers:
        pl.semaphore_signal(barrier, inc=1, device_id={"seq": peer}, device_id_type=MESH)
    pl.semaphore_wait(barrier, len(peers))


def push(src, dst, send, recv, peer):
    return pltpu.make_async_remote_copy(
        src_ref=src, dst_ref=dst, send_sem=send, recv_sem=recv,
        device_id={"seq": peer}, device_id_type=MESH)


def gather_kernel(n, pieces, own, out, send_sem, recv_sem, copy_sem):
    pair = 2
    lines = n // pair
    me = lax.axis_index("seq")
    a, b = me // pair, me % pair
    column = [((a + k) % lines) * pair + b for k in range(1, lines)]
    back = [((a + lines - k) % lines) * pair + b for k in range(1, lines)]
    across = a * pair + (1 - b)
    greet(column + [across])
    rows = own.shape[0] // pieces
    local = pltpu.make_async_copy(own, out.at[me], copy_sem)
    local.start()

    def piece(p):
        return pl.ds(p * rows, rows)

    sends = []
    for p in range(pieces):
        for k in range(lines):
            peer = across if k == 0 else column[k - 1]
            copy = push(own.at[piece(p)], out.at[me, piece(p)], send_sem.at[k, p], recv_sem.at[k, p], peer)
            copy.start()
            sends.append(copy)
    relays = []
    for p in range(pieces):
        for k in range(1, lines):
            src = back[k - 1]
            push(own.at[piece(p)], out.at[src, piece(p)], send_sem.at[k, p], recv_sem.at[k, p], across).wait_recv()
            slot = lines + k - 1
            copy = push(out.at[src, piece(p)], out.at[src, piece(p)], send_sem.at[slot, p], recv_sem.at[slot, p], across)
            copy.start()
            relays.append(copy)
    for p in range(pieces):
        push(own.at[piece(p)], out.at[across, piece(p)], send_sem.at[0, p], recv_sem.at[0, p], across).wait_recv()
    for copy in relays:
        copy.wait_recv()
    for copy in sends + relays:
        copy.wait_send()
    local.wait()


def gather_rows(x, n, pieces=4, collective_id=0):
    slots = n // 2 + n // 2 - 1
    return pl.pallas_call(
        functools.partial(gather_kernel, n, pieces),
        out_shape=jax.ShapeDtypeStruct((n,) + x.shape, x.dtype),
        in_specs=[pl.BlockSpec(memory_space=pltpu.VMEM)],
        out_specs=pl.BlockSpec(memory_space=ANY),
        scratch_shapes=[
            pltpu.SemaphoreType.DMA((slots, pieces)),
            pltpu.SemaphoreType.DMA((slots, pieces)),
            pltpu.SemaphoreType.DMA,
        ],
        compiler_params=pltpu.CompilerParams(collective_id=collective_id, has_side_effects=True),
        name="gather_rows",
    )(x)


def reduce_kernel(n, pieces, part, out, mine, got, sums, landed, send_sem, recv_sem, load_sem):
    pair = 2
    lines = n // pair
    me = lax.axis_index("seq")
    a, b = me // pair, me % pair
    column = [((a + k) % lines) * pair + b for k in range(1, lines)]
    across = a * pair + (1 - b)
    greet(column + [across])
    rows = out.shape[0] // pieces
    order = list(range(1, lines)) + [0]

    def piece(p):
        return pl.ds(p * rows, rows)

    firsts, loads = {}, {}
    for k in order:
        line = (a + k) % lines
        for p in range(pieces):
            copy = push(part.at[line * pair + (1 - b), piece(p)], got.at[k, piece(p)],
                        send_sem.at[k, p], recv_sem.at[k, p], across)
            copy.start()
            firsts[k, p] = copy
            load = pltpu.make_async_copy(part.at[line * pair + b, piece(p)], mine.at[k, piece(p)], load_sem.at[k, p])
            load.start()
            loads[k, p] = load
    seconds = {}
    for k in order:
        for p in range(pieces):
            firsts[k, p].wait_recv()
            loads[k, p].wait()
            total = mine[k, piece(p)].astype(jnp.float32) + got[k, piece(p)].astype(jnp.float32)
            if k:
                sums[k - 1, piece(p)] = total.astype(jnp.bfloat16)
                slot = lines + k - 1
                copy = push(sums.at[k - 1, piece(p)], landed.at[k - 1, piece(p)],
                            send_sem.at[slot, p], recv_sem.at[slot, p], column[k - 1])
                copy.start()
                seconds[k, p] = copy
            else:
                for j in range(1, lines):
                    seconds[j, p].wait_recv()
                    total += landed[j - 1, piece(p)].astype(jnp.float32)
                out[piece(p), :] = total
    for copy in list(firsts.values()) + list(seconds.values()):
        copy.wait_send()


def reduce_rows(part, n, pieces=4, collective_id=1):
    _, rows, width = part.shape
    lines = n // 2
    slots = lines + lines - 1
    return pl.pallas_call(
        functools.partial(reduce_kernel, n, pieces),
        out_shape=jax.ShapeDtypeStruct((rows, width), jnp.float32),
        in_specs=[pl.BlockSpec(memory_space=ANY)],
        out_specs=pl.BlockSpec(memory_space=pltpu.VMEM),
        scratch_shapes=[
            pltpu.VMEM((lines, rows, width), jnp.bfloat16),
            pltpu.VMEM((lines, rows, width), jnp.bfloat16),
            pltpu.VMEM((lines - 1, rows, width), jnp.bfloat16),
            pltpu.VMEM((lines - 1, rows, width), jnp.bfloat16),
            pltpu.SemaphoreType.DMA((slots, pieces)),
            pltpu.SemaphoreType.DMA((slots, pieces)),
            pltpu.SemaphoreType.DMA((lines, pieces)),
        ],
        compiler_params=pltpu.CompilerParams(collective_id=collective_id, has_side_effects=True),
        name="reduce_rows",
    )(part)


def sum_kernel(n, own, sent, out, taken, landed, send_sem, recv_sem, copy_sem):
    me = lax.axis_index("seq")
    peers = [(me + k) % n for k in range(1, n)]
    greet(peers)
    local = pltpu.make_async_copy(sent.at[me], taken.at[me], copy_sem)
    local.start()
    copies, swaps = [], []
    for k in range(1, n):
        copy = push(own, landed.at[k - 1], send_sem.at[0, k - 1], recv_sem.at[0, k - 1], peers[k - 1])
        copy.start()
        copies.append(copy)
        swap = push(sent.at[peers[k - 1]], taken.at[me], send_sem.at[1, k - 1], recv_sem.at[1, k - 1], peers[k - 1])
        swap.start()
        swaps.append(swap)
    total = own[...]
    for k in range(1, n):
        copies[k - 1].wait_recv()
        total = total + landed[k - 1]
    out[...] = total
    for copy in copies:
        copy.wait_send()
    for swap in swaps:
        swap.wait()
    local.wait()


def sum_rows(x, sent, n, collective_id):
    return pl.pallas_call(
        functools.partial(sum_kernel, n),
        out_shape=(
            jax.ShapeDtypeStruct(x.shape, x.dtype),
            jax.ShapeDtypeStruct(sent.shape, sent.dtype),
        ),
        in_specs=[pl.BlockSpec(memory_space=pltpu.VMEM)] * 2,
        out_specs=[pl.BlockSpec(memory_space=pltpu.VMEM)] * 2,
        scratch_shapes=[
            pltpu.VMEM((n - 1,) + x.shape, x.dtype),
            pltpu.SemaphoreType.DMA((2, n - 1)),
            pltpu.SemaphoreType.DMA((2, n - 1)),
            pltpu.SemaphoreType.DMA,
        ],
        compiler_params=pltpu.CompilerParams(collective_id=collective_id, has_side_effects=True),
        name="sum_rows",
    )(x, sent)


H = 16
epsilon = 1e-05


def inverse_norm(values):
    return lax.rsqrt(jnp.mean(values * values, axis=-1, keepdims=True) + epsilon)


def norm_backward(values, factor, gain, upstream):
    normal = values * factor
    weighted = upstream * gain
    gain_term = jnp.sum(upstream * normal, axis=0)
    back = factor * (weighted - normal * jnp.mean(weighted * normal, axis=-1, keepdims=True))
    return (back, gain_term)


def rope_tables(positions, head_dim):
    half = head_dim // 2
    frequency = jnp.power(10000.0, -2.0 * jnp.arange(half, dtype=jnp.float32) / head_dim)
    angle = positions.astype(jnp.float32)[:, None] * frequency[None, :]
    return (jnp.cos(angle)[:, None, :], jnp.sin(angle)[:, None, :])


def rotate(values, cosine, sine):
    half = values.shape[-1] // 2
    first = values[..., :half]
    second = values[..., half:]
    return jnp.concatenate(
        [first * cosine - second * sine, second * cosine + first * sine], axis=-1
    )


def unrotate(grads, cosine, sine):
    half = grads.shape[-1] // 2
    first = grads[..., :half]
    second = grads[..., half:]
    return jnp.concatenate(
        [first * cosine + second * sine, second * cosine - first * sine], axis=-1
    )


def block_scores(start, query_rows, keys, scale):
    scores = (
        jnp.einsum("qhd,khd->hqk", query_rows, keys, preferred_element_type=jnp.float32) * scale
    )
    query_pos = start + jnp.arange(query_rows.shape[0], dtype=jnp.int32)
    key_pos = jnp.arange(keys.shape[0], dtype=jnp.int32)
    causal = query_pos[:, None] >= key_pos[None, :]
    return jnp.where(causal[None], scores, -1e30)


def gather_async(x, n):
    pair = 2
    lines = n // pair
    across = [(a * pair + b, a * pair + 1 - b) for a in range(lines) for b in range(pair)]
    column = [x]
    for k in range(1, lines):
        column.append(
            lax.ppermute(
                x, "seq", [(a * pair + b, (a + k) % lines * pair + b) for a in range(lines) for b in range(pair)]
            )
        )
    other = [lax.ppermute(c, "seq", across) for c in column]
    me = lax.axis_index("seq")
    a, b = me // pair, me % pair
    out = jnp.zeros((n,) + x.shape, x.dtype)
    for k in range(lines):
        line = (a + lines - k) % lines
        out = lax.dynamic_update_index_in_dim(out, column[k], line * pair + b, 0)
        out = lax.dynamic_update_index_in_dim(out, other[k], line * pair + 1 - b, 0)
    return out


def reduce_async(part, n):
    pair = 2
    lines = n // pair
    me = lax.axis_index("seq")
    a, b = me // pair, me % pair
    across = [(c * pair + d, c * pair + 1 - d) for c in range(lines) for d in range(pair)]
    halves = part.reshape(lines, pair, *part.shape[1:])
    give = lax.dynamic_index_in_dim(halves, 1 - b, 1, keepdims=False)
    keep = lax.dynamic_index_in_dim(halves, b, 1, keepdims=False)
    got = lax.ppermute(give, "seq", across)
    sums = (keep.astype(jnp.float32) + got.astype(jnp.float32)).astype(part.dtype)
    total = lax.dynamic_index_in_dim(sums, a, 0, keepdims=False).astype(jnp.float32)
    for k in range(1, lines):
        shift = [(c * pair + d, (c + k) % lines * pair + d) for c in range(lines) for d in range(pair)]
        piece = lax.dynamic_index_in_dim(sums, (a + k) % lines, 0, keepdims=False)
        total = total + lax.ppermute(piece, "seq", shift).astype(jnp.float32)
    return total


def local(
    tokens, routes, route_weights, cotangent, attn_gain, query_gain, key_gain, ffn_gain,
    w_query, w_key, w_value, w_out, w_gate, w_up, w_down,
):
    n = lax.axis_size("seq")
    groups = lax.axis_size("fsdp")
    me = lax.axis_index("seq")
    width = tokens.shape[-1]
    own_tokens = tokens.reshape(-1, width)
    rows = own_tokens.shape[0]
    length = rows * n
    picks = routes.shape[-1]
    shard = w_query.shape[0]
    local_experts = w_gate.shape[1]
    experts = local_experts * n
    hidden_width = w_gate.shape[2]
    capacity = 3 * rows * picks // (2 * experts)
    head_dim = width // H
    heads = H // n
    span = heads * head_dim
    scale = head_dim ** (-0.5)
    bf, f32 = jnp.bfloat16, jnp.float32

    cols = lambda w: lax.dynamic_slice_in_dim(w, me * span, span, 1)
    w_heads = jnp.concatenate([cols(w_query), cols(w_key), cols(w_value)], axis=1)
    w_heads = lax.all_gather(w_heads, "fsdp", axis=0, tiled=True)
    full_out = lax.all_gather(w_out, "fsdp", axis=0, tiled=True)
    gains = lax.all_gather(
        jnp.stack([attn_gain, query_gain, key_gain, ffn_gain]), "fsdp", axis=1, tiled=True
    ).astype(f32)
    gain_attn, gain_ffn = gains[0], gains[3]
    gain_query = lax.dynamic_slice_in_dim(gains[1], me * span, span, 0)
    gain_key = lax.dynamic_slice_in_dim(gains[2], me * span, span, 0)
    by_expert = lambda w: lax.all_gather(jnp.swapaxes(w, 0, 1), "fsdp", axis=1, tiled=True)
    full_gate, full_up, full_down = by_expert(w_gate), by_expert(w_up), by_expert(w_down)

    expert_ids = jnp.arange(experts, dtype=jnp.int32)
    named = routes.reshape(rows, picks)[None] == expert_ids[:, None, None]
    mixing = route_weights.reshape(rows, picks)[None]
    sent = jnp.sum(jnp.where(named, mixing, 0.0), axis=-1).reshape(n, local_experts, rows)

    inputs_all = gather_rows(own_tokens, n, 8, 0).reshape(length, width)
    cot_own, inputs_all = lax.optimization_barrier((cotangent.reshape(rows, width), inputs_all))
    cot_all = gather_async(cot_own, n)
    inputs_all = inputs_all.astype(f32)
    norm_all = inverse_norm(inputs_all)
    normed = (inputs_all * norm_all * gain_attn).astype(bf)
    proj = jnp.dot(normed, w_heads, preferred_element_type=f32)
    query_proj, key_proj, value_proj = proj[:, :span], proj[:, span : 2 * span], proj[:, 2 * span :]
    squares = jnp.stack([jnp.sum(query_proj**2, -1), jnp.sum(key_proj**2, -1)]).reshape(-1, 128)
    squares, weights = sum_rows(squares, sent, n, 1)
    factors = lax.rsqrt(squares.reshape(2, length, 1) / width + epsilon)
    query_factor, key_factor = factors[0], factors[1]
    cosine, sine = rope_tables(jnp.arange(length, dtype=jnp.int32), head_dim)
    split = lambda v: v.reshape(length, heads, head_dim)
    queries = rotate(split(query_proj * query_factor * gain_query), cosine, sine).astype(bf)
    keys = rotate(split(key_proj * key_factor * gain_key), cosine, sine).astype(bf)
    values = split(value_proj).astype(bf)

    block = min(512, length)
    block_ids = jnp.arange(length // block, dtype=jnp.int32)

    def forward_block(index):
        start = index * block
        query_rows = lax.dynamic_slice_in_dim(queries, start, block, 0)
        scores = block_scores(start, query_rows, keys, scale)
        peak = jnp.max(scores, axis=-1, keepdims=True)
        total = jnp.log(jnp.sum(jnp.exp(scores - peak), axis=-1, keepdims=True)) + peak
        probs = jnp.exp(scores - total).astype(bf)
        result = jnp.einsum("hqk,khd->qhd", probs, values, preferred_element_type=f32)
        return (result.astype(bf), total[..., 0])

    heads_out, log_totals = lax.map(forward_block, block_ids)
    heads_out = heads_out.reshape(length, heads, head_dim)
    context = lax.all_to_all(
        heads_out.reshape(length, span), "seq", split_axis=0, concat_axis=1, tiled=True
    )
    inputs = own_tokens.astype(f32)
    mid = inputs + jnp.dot(context, full_out, preferred_element_type=f32)
    norm_two = inverse_norm(mid)
    ffn_in = (mid * norm_two * gain_ffn).astype(bf)

    ffn_all = gather_rows(ffn_in, n, 8, 2)
    taken = weights > 0
    tri = (jnp.arange(rows)[:, None] <= jnp.arange(rows)[None, :]).astype(bf)
    rank = jnp.einsum("cet,tu->ceu", taken.astype(bf), tri, preferred_element_type=f32) - 1.0
    slot_ids = jnp.arange(capacity, dtype=f32)
    hit = (rank[:, :, None, :] == slot_ids[None, None, :, None]) & taken[:, :, None, :]
    place = hit.astype(bf)
    slot_weight = jnp.sum(jnp.where(hit, weights[:, :, None, :], 0.0), axis=-1)
    slot_weight = jnp.swapaxes(slot_weight, 0, 1)[..., None]
    place_rows = lambda v: jnp.einsum("cert,ctd->ecrd", place, v, preferred_element_type=f32)
    received = place_rows(ffn_all).astype(bf)
    gate = jnp.einsum("ecrd,edf->ecrf", received, full_gate, preferred_element_type=f32)
    up_part = jnp.einsum("ecrd,edf->ecrf", received, full_up, preferred_element_type=f32)
    sigmoid_gate = jax.nn.sigmoid(gate)
    activated = gate * sigmoid_gate
    hidden = (activated * up_part).astype(bf)
    expert_out = jnp.einsum("ecrf,edf->ecrd", hidden, full_down, preferred_element_type=f32)
    expert_out = (expert_out * slot_weight).astype(bf)
    unplace = lambda v: jnp.einsum("cert,ecrd->ctd", place, v, preferred_element_type=f32).astype(bf)
    ffn_out = reduce_async(unplace(expert_out), n)
    block_out = (mid + ffn_out).astype(bf)

    out_grad = cotangent.reshape(rows, width).astype(f32)
    down_received = (place_rows(cot_all) * slot_weight).astype(bf)
    hidden_grad = jnp.einsum("ecrd,edf->ecrf", down_received, full_down, preferred_element_type=f32)
    slope = sigmoid_gate * (1.0 + gate * (1.0 - sigmoid_gate))
    gate_grad = (hidden_grad * up_part * slope).astype(bf)
    up_grad = (hidden_grad * activated).astype(bf)
    rows_grad = (
        jnp.einsum("ecrf,edf->ecrd", gate_grad, full_gate, preferred_element_type=f32)
        + jnp.einsum("ecrf,edf->ecrd", up_grad, full_up, preferred_element_type=f32)
    ).astype(bf)
    term = lambda a, b: jnp.einsum("ecrd,ecrf->edf", a, b, preferred_element_type=f32).astype(bf)
    scatter = lambda v: jnp.swapaxes(
        lax.psum_scatter(v, "fsdp", scatter_dimension=1, tiled=True).astype(f32), 0, 1
    )
    rows_part, down_term, gate_term, up_term = lax.optimization_barrier(
        (
            unplace(rows_grad),
            term(down_received, hidden),
            term(received, gate_grad),
            term(received, up_grad),
        )
    )
    down_sum, gate_sum, up_sum = scatter(down_term), scatter(gate_term), scatter(up_term)
    ffn_in_grad = reduce_rows(rows_part, n, 8, 4)
    mid_back, ffn_gain_term = norm_backward(mid, norm_two, gain_ffn, ffn_in_grad)
    mid_grad = out_grad + mid_back
    branch_grad = mid_grad.astype(bf)

    branch_all = gather_rows(branch_grad, n, 8, 5).reshape(length, width)
    out_rows = lax.dynamic_slice_in_dim(full_out, me * span, span, 0)
    heads_grad = split(
        jnp.einsum("te,de->td", branch_all, out_rows, preferred_element_type=f32).astype(bf)
    )
    out_term = jnp.einsum(
        "td,te->de", heads_out.reshape(length, span), branch_all, preferred_element_type=f32
    )
    out_sum = lax.psum_scatter(out_term, "fsdp", scatter_dimension=0, tiled=True)

    def backward_block(carry, index):
        key_acc, value_acc = carry
        start = index * block
        query_rows = lax.dynamic_slice_in_dim(queries, start, block, 0)
        grad_rows = lax.dynamic_slice_in_dim(heads_grad, start, block, 0)
        scores = block_scores(start, query_rows, keys, scale)
        probs = jnp.exp(scores - log_totals[index][..., None])
        probs_low = probs.astype(bf)
        probs_grad = jnp.einsum("qhd,khd->hqk", grad_rows, values, preferred_element_type=f32)
        shifted = probs_grad - jnp.sum(probs * probs_grad, axis=-1, keepdims=True)
        score_grad = (probs * shifted * scale).astype(bf)
        query_part = jnp.einsum("hqk,khd->qhd", score_grad, keys, preferred_element_type=f32)
        key_acc = key_acc + jnp.einsum(
            "hqk,qhd->khd", score_grad, query_rows, preferred_element_type=f32
        )
        value_acc = value_acc + jnp.einsum(
            "hqk,qhd->khd", probs_low, grad_rows, preferred_element_type=f32
        )
        return ((key_acc, value_acc), query_part.astype(bf))

    zero_heads = jnp.zeros((length, heads, head_dim), f32)
    (key_acc, value_acc), query_parts = lax.scan(
        backward_block, (zero_heads, zero_heads), block_ids
    )
    query_back = query_parts.reshape(length, heads, head_dim).astype(f32)
    key_back = key_acc.astype(bf).astype(f32)
    value_grad = value_acc.astype(bf).reshape(length, span)
    query_up = unrotate(query_back, cosine, sine).reshape(length, span)
    key_up = unrotate(key_back, cosine, sine).reshape(length, span)
    query_normal, key_normal = query_proj * query_factor, key_proj * key_factor
    query_weighted, key_weighted = query_up * gain_query, key_up * gain_key
    means = jnp.stack(
        [jnp.sum(query_weighted * query_normal, -1), jnp.sum(key_weighted * key_normal, -1)]
    ).reshape(-1, 128)
    means, _ = sum_rows(means, jnp.zeros((n, 8, 128), f32), n, 6)
    means = means.reshape(2, length, 1) / width
    query_grad = (query_factor * (query_weighted - query_normal * means[0])).astype(bf)
    key_grad = (key_factor * (key_weighted - key_normal * means[1])).astype(bf)
    head_gains = jnp.stack(
        [jnp.sum(query_up * query_normal, axis=0), jnp.sum(key_up * key_normal, axis=0)]
    )
    proj_grad = jnp.concatenate([query_grad, key_grad, value_grad], axis=1)
    normed_part = jnp.einsum("te,de->td", proj_grad, w_heads, preferred_element_type=f32).astype(bf)
    normed_grad = reduce_rows(normed_part.reshape(n, rows, width), n, 8, 7)
    input_back, attn_gain_term = norm_backward(inputs, inverse_norm(inputs), gain_attn, normed_grad)
    tokens_grad = mid_grad + input_back
    head_term = jnp.einsum("td,te->de", normed, proj_grad, preferred_element_type=f32)
    part = width // (n * groups)
    head_term = lax.psum_scatter(
        head_term.astype(bf).reshape(n, groups, part, 3 * span).swapaxes(0, 1),
        "fsdp",
        scatter_dimension=0,
        tiled=True,
    ).reshape(n, part, 3, span)
    head_term = lax.all_to_all(head_term, "seq", split_axis=0, concat_axis=0, tiled=True)
    head_sums = [
        head_term[:, :, i].swapaxes(0, 1).reshape(part, width).astype(f32) for i in range(3)
    ]
    gain_terms = lax.psum_scatter(
        jnp.stack([attn_gain_term, ffn_gain_term]), ("seq", "fsdp"), scatter_dimension=1, tiled=True
    )
    head_gains = lax.psum_scatter(head_gains, "fsdp", scatter_dimension=1, tiled=True)
    return (
        block_out.reshape(tokens.shape),
        tokens_grad.reshape(tokens.shape),
        gain_terms[0],
        head_gains[0],
        head_gains[1],
        gain_terms[1],
        head_sums[0],
        head_sums[1],
        head_sums[2],
        out_sum,
        gate_sum,
        up_sum,
        down_sum,
    )


def solution(mesh):
    rows3 = P("fsdp", "seq", None)
    both = P(("seq", "fsdp"))
    both2 = P(("seq", "fsdp"), None)
    placed = (rows3,) * 4 + (P("fsdp"),) * 4 + (P("fsdp", None),) * 4 + (rows3,) * 3
    return jax.shard_map(
        local,
        mesh=mesh,
        in_specs=placed,
        out_specs=(rows3,) * 2 + (both,) * 4 + (both2,) * 4 + (rows3,) * 3,
        check_vma=False,
    )
```

```python
import functools
import jax
import jax.numpy as jnp
from jax import lax
from jax.experimental import pallas as pl
from jax.experimental.pallas import tpu as pltpu
from jax.sharding import PartitionSpec as P

MESH = pl.DeviceIdType.MESH
ANY = pl.ANY
H = 16
epsilon = 1e-05


def work(us):
    return pl.CostEstimate(flops=int(us * 6e8), bytes_accessed=0, transcendentals=0)


def greet(peers):
    barrier = pltpu.get_barrier_semaphore()
    for peer in peers:
        pl.semaphore_signal(barrier, inc=1, device_id={"seq": peer}, device_id_type=MESH)
    pl.semaphore_wait(barrier, len(peers))


def push(src, dst, send, recv, peer):
    return pltpu.make_async_remote_copy(
        src_ref=src, dst_ref=dst, send_sem=send, recv_sem=recv,
        device_id={"seq": peer}, device_id_type=MESH)


def gather_kernel(n, pieces, own, out, send_sem, recv_sem, copy_sem):
    pair = 2
    lines = n // pair
    me = lax.axis_index("seq")
    a, b = me // pair, me % pair
    column = [((a + k) % lines) * pair + b for k in range(1, lines)]
    back = [((a + lines - k) % lines) * pair + b for k in range(1, lines)]
    across = a * pair + (1 - b)
    greet(column + [across])
    rows = own.shape[0] // pieces
    local = pltpu.make_async_copy(own, out.at[me], copy_sem)
    local.start()

    def piece(p):
        return pl.ds(p * rows, rows)

    sends = []
    for p in range(pieces):
        for k in range(lines):
            peer = across if k == 0 else column[k - 1]
            copy = push(own.at[piece(p)], out.at[me, piece(p)], send_sem.at[k, p], recv_sem.at[k, p], peer)
            copy.start()
            sends.append(copy)
    relays = []
    for p in range(pieces):
        for k in range(1, lines):
            src = back[k - 1]
            push(own.at[piece(p)], out.at[src, piece(p)], send_sem.at[k, p], recv_sem.at[k, p], across).wait_recv()
            slot = lines + k - 1
            copy = push(out.at[src, piece(p)], out.at[src, piece(p)], send_sem.at[slot, p], recv_sem.at[slot, p], across)
            copy.start()
            relays.append(copy)
    for p in range(pieces):
        push(own.at[piece(p)], out.at[across, piece(p)], send_sem.at[0, p], recv_sem.at[0, p], across).wait_recv()
    for copy in relays:
        copy.wait_recv()
    for copy in sends + relays:
        copy.wait_send()
    local.wait()


def gather_rows(x, n, pieces=4, collective_id=0):
    slots = n // 2 + n // 2 - 1
    return pl.pallas_call(
        functools.partial(gather_kernel, n, pieces),
        out_shape=jax.ShapeDtypeStruct((n,) + x.shape, x.dtype),
        in_specs=[pl.BlockSpec(memory_space=pltpu.VMEM)],
        out_specs=pl.BlockSpec(memory_space=ANY),
        scratch_shapes=[
            pltpu.SemaphoreType.DMA((slots, pieces)),
            pltpu.SemaphoreType.DMA((slots, pieces)),
            pltpu.SemaphoreType.DMA,
        ],
        compiler_params=pltpu.CompilerParams(collective_id=collective_id, has_side_effects=True),
        cost_estimate=work(105),
        name="gather_rows",
    )(x)


def reduce_kernel(n, pieces, part, out, mine, got, sums, landed, send_sem, recv_sem, load_sem):
    pair = 2
    lines = n // pair
    me = lax.axis_index("seq")
    a, b = me // pair, me % pair
    column = [((a + k) % lines) * pair + b for k in range(1, lines)]
    across = a * pair + (1 - b)
    greet(column + [across])
    rows = out.shape[0] // pieces
    order = list(range(1, lines)) + [0]

    def piece(p):
        return pl.ds(p * rows, rows)

    firsts, loads = {}, {}
    for k in order:
        line = (a + k) % lines
        for p in range(pieces):
            copy = push(part.at[line * pair + (1 - b), piece(p)], got.at[k, piece(p)],
                        send_sem.at[k, p], recv_sem.at[k, p], across)
            copy.start()
            firsts[k, p] = copy
            load = pltpu.make_async_copy(part.at[line * pair + b, piece(p)], mine.at[k, piece(p)], load_sem.at[k, p])
            load.start()
            loads[k, p] = load
    seconds = {}
    for k in order:
        for p in range(pieces):
            firsts[k, p].wait_recv()
            loads[k, p].wait()
            total = mine[k, piece(p)].astype(jnp.float32) + got[k, piece(p)].astype(jnp.float32)
            if k:
                sums[k - 1, piece(p)] = total.astype(jnp.bfloat16)
                slot = lines + k - 1
                copy = push(sums.at[k - 1, piece(p)], landed.at[k - 1, piece(p)],
                            send_sem.at[slot, p], recv_sem.at[slot, p], column[k - 1])
                copy.start()
                seconds[k, p] = copy
            else:
                for j in range(1, lines):
                    seconds[j, p].wait_recv()
                    total += landed[j - 1, piece(p)].astype(jnp.float32)
                out[piece(p), :] = total
    for copy in list(firsts.values()) + list(seconds.values()):
        copy.wait_send()


def reduce_rows(part, n, pieces=4, collective_id=1):
    _, rows, width = part.shape
    lines = n // 2
    slots = lines + lines - 1
    return pl.pallas_call(
        functools.partial(reduce_kernel, n, pieces),
        out_shape=jax.ShapeDtypeStruct((rows, width), jnp.float32),
        in_specs=[pl.BlockSpec(memory_space=ANY)],
        out_specs=pl.BlockSpec(memory_space=pltpu.VMEM),
        scratch_shapes=[
            pltpu.VMEM((lines, rows, width), jnp.bfloat16),
            pltpu.VMEM((lines, rows, width), jnp.bfloat16),
            pltpu.VMEM((lines - 1, rows, width), jnp.bfloat16),
            pltpu.VMEM((lines - 1, rows, width), jnp.bfloat16),
            pltpu.SemaphoreType.DMA((slots, pieces)),
            pltpu.SemaphoreType.DMA((slots, pieces)),
            pltpu.SemaphoreType.DMA((lines, pieces)),
        ],
        compiler_params=pltpu.CompilerParams(collective_id=collective_id, has_side_effects=True),
        cost_estimate=work(98),
        name="reduce_rows",
    )(part)


def gains_kernel(n, groups, sent, own, out, taken, summed, landed, send_sem, recv_sem, side_send, side_recv):
    me, group = lax.axis_index("seq"), lax.axis_index("fsdp")
    barrier = pltpu.get_barrier_semaphore()
    peers = [(me + k) % n for k in range(1, n)]
    mates = [(group + k) % groups for k in range(1, groups)]
    for peer in peers:
        pl.semaphore_signal(barrier, inc=1, device_id={"seq": peer}, device_id_type=MESH)
    for mate in mates:
        pl.semaphore_signal(barrier, inc=1, device_id={"fsdp": mate}, device_id_type=MESH)
    pl.semaphore_wait(barrier, n - 1 + groups - 1)
    copies = []
    for k in range(1, n):
        copy = push(sent.at[peers[k - 1]], taken.at[k - 1], send_sem.at[k - 1], recv_sem.at[k - 1], peers[k - 1])
        copy.start()
        copies.append(copy)
    total = sent[me] + own[...]
    for k in range(1, n):
        copies[k - 1].wait_recv()
        total = total + taken[k - 1]
    summed[...] = total
    sides = []
    for k in range(1, groups):
        side = pltpu.make_async_remote_copy(
            src_ref=summed, dst_ref=landed.at[k - 1], send_sem=side_send.at[k - 1], recv_sem=side_recv.at[k - 1],
            device_id={"fsdp": mates[k - 1]}, device_id_type=MESH)
        side.start()
        sides.append(side)
    for k in range(1, groups):
        sides[k - 1].wait_recv()
        total = total + landed[k - 1]
    out[...] = total
    for copy in copies + sides:
        copy.wait_send()


def sum_gains(sent, own, n, groups, collective_id):
    shape = own.shape
    return pl.pallas_call(
        functools.partial(gains_kernel, n, groups),
        out_shape=jax.ShapeDtypeStruct(shape, own.dtype),
        in_specs=[pl.BlockSpec(memory_space=pltpu.VMEM)] * 2,
        out_specs=pl.BlockSpec(memory_space=pltpu.VMEM),
        scratch_shapes=[
            pltpu.VMEM((n - 1,) + shape, own.dtype),
            pltpu.VMEM(shape, own.dtype),
            pltpu.VMEM((groups - 1,) + shape, own.dtype),
            pltpu.SemaphoreType.DMA((n - 1,)),
            pltpu.SemaphoreType.DMA((n - 1,)),
            pltpu.SemaphoreType.DMA((groups - 1,)),
            pltpu.SemaphoreType.DMA((groups - 1,)),
        ],
        compiler_params=pltpu.CompilerParams(collective_id=collective_id, has_side_effects=True),
        cost_estimate=work(10),
        name="sum_gains",
    )(sent, own)


def widen_kernel(x_ref, o_ref):
    for e in range(x_ref.shape[0]):
        o_ref[:, e, :] = x_ref[e].astype(jnp.float32)


def widen(x):
    experts, rows, columns = x.shape
    step = min(128, rows)
    return pl.pallas_call(
        widen_kernel,
        grid=(rows // step,),
        out_shape=jax.ShapeDtypeStruct((rows, experts, columns), jnp.float32),
        in_specs=[pl.BlockSpec((experts, step, columns), lambda i: (0, i, 0))],
        out_specs=pl.BlockSpec((step, experts, columns), lambda i: (i, 0, 0)),
        cost_estimate=work(5),
        name="widen",
    )(x)


def masked(block):
    keys = lax.broadcasted_iota(jnp.int32, (block, block), 0)
    rows = lax.broadcasted_iota(jnp.int32, (block, block), 1)
    return keys <= rows


def across_lanes(a, b):
    return lax.dot_general(a, b, (((1,), (1,)), ((), ())), preferred_element_type=jnp.float32)


def down_rows(a, b):
    return lax.dot_general(a, b, (((0,), (0,)), ((), ())), preferred_element_type=jnp.float32)


LOG2E = 1.4426950408889634


def attend_kernel(block, scale, q_ref, k_ref, v_ref, o_ref, lse_ref, s_ref, acc_ref):
    length, dim = q_ref.shape

    def rows(i):
        return pl.ds(pl.multiple_of(i * block, block), block)

    def one_block(i, _):
        q = q_ref[rows(i), :]
        diag = across_lanes(k_ref[rows(i), :], q) * (scale * LOG2E)
        diag = jnp.where(masked(block), diag, -1e30)
        s_ref[rows(i), :] = diag
        peak = jnp.max(diag, axis=0, keepdims=True)

        def score(j, peak):
            s = across_lanes(k_ref[rows(j), :], q) * (scale * LOG2E)
            s_ref[rows(j), :] = s
            return jnp.maximum(peak, jnp.max(s, axis=0, keepdims=True))

        peak = lax.fori_loop(0, i, score, peak)
        acc_ref[...] = jnp.zeros_like(acc_ref)

        def weigh(j, total):
            p = jnp.exp2(s_ref[rows(j), :] - peak)
            acc_ref[...] += down_rows(v_ref[rows(j), :], p.astype(jnp.bfloat16))
            return total + jnp.sum(p, axis=0, keepdims=True)

        total = lax.fori_loop(0, i + 1, weigh, jnp.zeros_like(peak))
        o_ref[rows(i), :] = (acc_ref[...] / total).T.astype(o_ref.dtype)
        lse_ref[0, :, rows(i)] = peak + jnp.log2(total)
        return 0

    lax.fori_loop(0, length // block, one_block, 0)


def attend(q, k, v, heads, block, scale):
    length, width = q.shape
    dim = width // heads
    spec = pl.BlockSpec((length, dim), lambda h: (0, h))
    return pl.pallas_call(
        functools.partial(attend_kernel, block, scale),
        grid=(heads,),
        out_shape=(
            jax.ShapeDtypeStruct(q.shape, q.dtype),
            jax.ShapeDtypeStruct((heads, 1, length), jnp.float32),
        ),
        in_specs=[spec] * 3,
        out_specs=[spec, pl.BlockSpec((1, 1, length), lambda h: (h, 0, 0))],
        scratch_shapes=[
            pltpu.VMEM((length, block), jnp.float32),
            pltpu.VMEM((dim, block), jnp.float32),
        ],
        cost_estimate=work(25),
        name="attend",
    )(q, k, v)


def attend_back_kernel(
    block, scale, q_ref, k_ref, v_ref, g_ref, o_ref, lse_ref, dq_ref, dk_ref, dv_ref, dk_acc, dv_acc, dq_acc
):
    length, dim = q_ref.shape
    dk_acc[...] = jnp.zeros_like(dk_acc)
    dv_acc[...] = jnp.zeros_like(dv_acc)

    def rows(i):
        return pl.ds(pl.multiple_of(i * block, block), block)

    def one_block(i, _):
        q, g = q_ref[rows(i), :], g_ref[rows(i), :]
        lse = lse_ref[0, :, rows(i)]
        products = g.astype(jnp.float32) * o_ref[rows(i), :].astype(jnp.float32)
        shift = lax.dot_general(
            jnp.ones((8, dim), jnp.float32), products, (((1,), (1,)), ((), ())),
            precision=lax.Precision.HIGHEST, preferred_element_type=jnp.float32,
        )[:1]

        def pair(j, keep):
            k, v = k_ref[rows(j), :], v_ref[rows(j), :]
            p = jnp.exp2(across_lanes(k, q) * (scale * LOG2E) - lse)
            if keep is not None:
                p = jnp.where(keep, p, 0.0)
            ds = (p * (across_lanes(v, g) - shift) * scale).astype(jnp.bfloat16)
            dv_acc[rows(j), :] += jnp.dot(p.astype(jnp.bfloat16), g, preferred_element_type=jnp.float32)
            dk_acc[rows(j), :] += jnp.dot(ds, q, preferred_element_type=jnp.float32)
            dq_acc[...] += down_rows(k, ds)

        dq_acc[...] = jnp.zeros_like(dq_acc)
        pair(i, masked(block))

        def body(j, _):
            pair(j, None)
            return 0

        lax.fori_loop(0, i, body, 0)
        dq_ref[rows(i), :] = dq_acc[...].T.astype(dq_ref.dtype)
        return 0

    lax.fori_loop(0, length // block, one_block, 0)
    dk_ref[...] = dk_acc[...].astype(dk_ref.dtype)
    dv_ref[...] = dv_acc[...].astype(dv_ref.dtype)


def attend_back(q, k, v, g, o, lse, heads, block, scale):
    length, width = q.shape
    dim = width // heads
    spec = pl.BlockSpec((length, dim), lambda h: (0, h))
    return pl.pallas_call(
        functools.partial(attend_back_kernel, block, scale),
        grid=(heads,),
        out_shape=(jax.ShapeDtypeStruct(q.shape, q.dtype),) * 3,
        in_specs=[spec] * 5 + [pl.BlockSpec((1, 1, length), lambda h: (h, 0, 0))],
        out_specs=[spec] * 3,
        scratch_shapes=[
            pltpu.VMEM((length, dim), jnp.float32),
            pltpu.VMEM((length, dim), jnp.float32),
            pltpu.VMEM((dim, block), jnp.float32),
        ],
        cost_estimate=work(60),
        name="attend_back",
    )(q, k, v, g, o, lse)


def project_kernel(
    n, groups, pieces, own, w_query, w_key, w_value, gain_own,
    normed, proj, squares, w_ref, gains, held, send_sem, recv_sem, side_send, side_recv, copy_sem
):
    pair = 2
    lines = n // pair
    me, group = lax.axis_index("seq"), lax.axis_index("fsdp")
    a, b = me // pair, me % pair
    column = [((a + k) % lines) * pair + b for k in range(1, lines)]
    back = [((a + lines - k) % lines) * pair + b for k in range(1, lines)]
    across = a * pair + (1 - b)
    mates = [(group + k) % groups for k in range(1, groups)]
    barrier = pltpu.get_barrier_semaphore()
    for peer in column + [across]:
        pl.semaphore_signal(barrier, inc=1, device_id={"seq": peer}, device_id_type=MESH)
    for mate in mates:
        pl.semaphore_signal(barrier, inc=1, device_id={"fsdp": mate}, device_id_type=MESH)
    pl.semaphore_wait(barrier, lines + groups - 1)
    rows, width = own.shape
    step = rows // pieces
    span = w_ref.shape[1] // 3
    shard = w_query.shape[0]

    def piece(p):
        return pl.ds(p * step, step)

    sends = []
    for p in range(pieces):
        for k in range(lines):
            peer = across if k == 0 else column[k - 1]
            copy = push(own.at[piece(p)], held.at[me, piece(p)], send_sem.at[k, p], recv_sem.at[k, p], peer)
            copy.start()
            sends.append(copy)

    shard_rows = pl.ds(pl.multiple_of(group * shard, shard), shard)
    mine = pl.ds(pl.multiple_of(me * span, span), span)
    blocks = [
        (w.at[:, mine], w_ref.at[shard_rows, part * span : (part + 1) * span])
        for part, w in enumerate((w_query, w_key, w_value))
    ]
    blocks.append((gain_own, gains.at[:, shard_rows]))
    locals_, sides = [], []
    for i, (src, dst) in enumerate(blocks):
        for k in range(1, groups):
            side = pltpu.make_async_remote_copy(
                src_ref=src, dst_ref=dst, send_sem=side_send.at[i, k - 1], recv_sem=side_recv.at[i, k - 1],
                device_id={"fsdp": mates[k - 1]}, device_id_type=MESH)
            side.start()
            sides.append(side)
        local = pltpu.make_async_copy(src, dst, copy_sem.at[i])
        local.start()
        locals_.append(local)
    for copy in locals_:
        copy.wait()
    for side in sides:
        side.wait_recv()

    def project(src, chunk):
        x = chunk[...].astype(jnp.float32)
        factor = lax.rsqrt(jnp.mean(x * x, axis=-1, keepdims=True) + epsilon)
        place = pl.ds(pl.multiple_of(src * rows, rows), rows)
        normed[place, :] = (x * factor * gains[0:1, :]).astype(jnp.bfloat16)
        for part in range(3):
            cols = slice(part * span, (part + 1) * span)
            out = jnp.dot(normed[place, :], w_ref[:, cols], preferred_element_type=jnp.float32)
            proj[place, cols] = out
            if part < 2:
                sums = lax.dot_general(
                    jnp.ones((8, span), jnp.float32), out * out, (((1,), (1,)), ((), ())),
                    precision=lax.Precision.HIGHEST, preferred_element_type=jnp.float32,
                )
                squares[pl.ds(part * n + src, 1), :] = sums[:1]

    relays = []
    for p in range(pieces):
        for k in range(1, lines):
            src = back[k - 1]
            push(own.at[piece(p)], held.at[src, piece(p)], send_sem.at[k, p], recv_sem.at[k, p], across).wait_recv()
            slot = lines + k - 1
            copy = push(held.at[src, piece(p)], held.at[src, piece(p)], send_sem.at[slot, p], recv_sem.at[slot, p], across)
            copy.start()
            relays.append(copy)
        if p == pieces // 2 - 1:
            project(me, own)
    for p in range(pieces):
        push(own.at[piece(p)], held.at[across, piece(p)], send_sem.at[0, p], recv_sem.at[0, p], across).wait_recv()
    project(across, held.at[across])
    for k in range(1, lines):
        project(back[k - 1], held.at[back[k - 1]])
    for k in range(1, lines):
        for p in range(pieces):
            relays[p * (lines - 1) + k - 1].wait_recv()
        src = ((a + lines - k) % lines) * pair + 1 - b
        project(src, held.at[src])
    for copy in sends + relays + sides:
        copy.wait_send()


def project_rows(x, w_query, w_key, w_value, gains, n, groups, pieces, collective_id):
    rows, width = x.shape
    span = w_query.shape[1] // n
    slots = n // 2 + n // 2 - 1
    vmem = pl.BlockSpec(memory_space=pltpu.VMEM)
    hbm = pl.BlockSpec(memory_space=ANY)
    return pl.pallas_call(
        functools.partial(project_kernel, n, groups, pieces),
        out_shape=(
            jax.ShapeDtypeStruct((n * rows, width), jnp.bfloat16),
            jax.ShapeDtypeStruct((n * rows, 3 * span), jnp.float32),
            jax.ShapeDtypeStruct((2 * n, rows), jnp.float32),
            jax.ShapeDtypeStruct((width, 3 * span), jnp.bfloat16),
            jax.ShapeDtypeStruct((8, width), jnp.float32),
        ),
        in_specs=[vmem, hbm, hbm, hbm, vmem],
        out_specs=[vmem] * 5,
        scratch_shapes=[
            pltpu.VMEM((n, rows, width), jnp.bfloat16),
            pltpu.SemaphoreType.DMA((slots, pieces)),
            pltpu.SemaphoreType.DMA((slots, pieces)),
            pltpu.SemaphoreType.DMA((4, groups - 1)),
            pltpu.SemaphoreType.DMA((4, groups - 1)),
            pltpu.SemaphoreType.DMA((4,)),
        ],
        compiler_params=pltpu.CompilerParams(
            collective_id=collective_id, has_side_effects=True, vmem_limit_bytes=50 << 20
        ),
        cost_estimate=work(110),
        name="project_rows",
    )(x, w_query, w_key, w_value, gains)


def as_columns(row, lanes):
    return jnp.broadcast_to(row, (lanes, row.shape[1])).T


def turn_tables(c, near_cos, near_sin, far_cos, far_sin):
    far_c, far_s = far_cos[pl.ds(c, 1), :], far_sin[pl.ds(c, 1), :]
    cosine = near_cos[...] * far_c - near_sin[...] * far_s
    sine = near_sin[...] * far_c + near_cos[...] * far_s
    first = lax.broadcasted_iota(jnp.int32, sine.shape, 1) < sine.shape[1] // 2
    return cosine, jnp.where(first, -sine, sine)


def add_over_seq(n, own, landed, send_sem, recv_sem, peers):
    copies = []
    for k in range(1, n):
        copy = push(own, landed.at[k - 1], send_sem.at[k - 1], recv_sem.at[k - 1], peers[k - 1])
        copy.start()
        copies.append(copy)
    return copies


def rotate_kernel(
    n, full, squares, sent, proj, gains, near_cos, near_sin, far_cos, far_sin,
    queries, keys, values, factors, taken, landed, send_sem, recv_sem, copy_sem
):
    me = lax.axis_index("seq")
    peers = [(me + k) % n for k in range(1, n)]
    greet(peers)
    local = pltpu.make_async_copy(sent.at[me], taken.at[me], copy_sem)
    local.start()
    copies = add_over_seq(n, squares, landed, send_sem.at[0], recv_sem.at[0], peers)
    swaps = []
    for k in range(1, n):
        swap = push(sent.at[peers[k - 1]], taken.at[me], send_sem.at[1, k - 1], recv_sem.at[1, k - 1], peers[k - 1])
        swap.start()
        swaps.append(swap)
    span = queries.shape[1]
    rows = squares.shape[1]
    lanes = near_cos.shape[1]
    total = squares[...]
    for k in range(1, n):
        copies[k - 1].wait_recv()
        total = total + landed[k - 1]
    factors[...] = lax.rsqrt(total / full + epsilon)

    def chunk(c, _):
        place = pl.ds(pl.multiple_of(c * rows, rows), rows)
        cosine, sine = turn_tables(c, near_cos, near_sin, far_cos, far_sin)
        for part, out in ((0, queries), (1, keys)):
            factor = as_columns(factors[pl.ds(part * n + c, 1), :], lanes)
            for h in range(span // lanes):
                cols = slice(part * span + h * lanes, part * span + (h + 1) * lanes)
                x = proj[place, cols] * factor * gains[part : part + 1, h * lanes : (h + 1) * lanes]
                turned = x * cosine + pltpu.roll(x, lanes // 2, 1) * sine
                out[place, h * lanes : (h + 1) * lanes] = turned.astype(jnp.bfloat16)
        values[place, :] = proj[place, 2 * span :].astype(jnp.bfloat16)
        return 0

    lax.fori_loop(0, n, chunk, 0)
    for copy in copies:
        copy.wait_send()
    for swap in swaps:
        swap.wait()
    local.wait()


def rotate_rows(squares, sent, proj, gains, tables, n, full, collective_id):
    length, outs = proj.shape
    span = outs // 3
    vmem = pl.BlockSpec(memory_space=pltpu.VMEM)
    heads = jax.ShapeDtypeStruct((length, span), jnp.bfloat16)
    return pl.pallas_call(
        functools.partial(rotate_kernel, n, full),
        out_shape=(
            heads, heads, heads,
            jax.ShapeDtypeStruct(squares.shape, jnp.float32),
            jax.ShapeDtypeStruct(sent.shape, sent.dtype),
        ),
        in_specs=[vmem] * 8,
        out_specs=[vmem] * 5,
        scratch_shapes=[
            pltpu.VMEM((n - 1,) + squares.shape, jnp.float32),
            pltpu.SemaphoreType.DMA((2, n - 1)),
            pltpu.SemaphoreType.DMA((2, n - 1)),
            pltpu.SemaphoreType.DMA,
        ],
        compiler_params=pltpu.CompilerParams(
            collective_id=collective_id, has_side_effects=True, vmem_limit_bytes=40 << 20
        ),
        cost_estimate=work(15),
        name="rotate_rows",
    )(squares, sent, proj, gains, *tables)


def heads_back_kernel(
    n, full, dq, dk, dv, proj, factors, gains, near_cos, near_sin, far_cos, far_sin,
    grads, gain_grads, sums, landed, send_sem, recv_sem
):
    me = lax.axis_index("seq")
    peers = [(me + k) % n for k in range(1, n)]
    greet(peers)
    span = dq.shape[1]
    rows = sums.shape[1]
    lanes = near_cos.shape[1]
    count = span // lanes

    def parts(c, part, h, grad):
        place = pl.ds(pl.multiple_of(c * rows, rows), rows)
        cosine, sine = turn_tables(c, near_cos, near_sin, far_cos, far_sin)
        g = grad[place, h * lanes : (h + 1) * lanes].astype(jnp.float32)
        up = g * cosine + pltpu.roll(g * sine, lanes // 2, 1)
        factor = as_columns(factors[pl.ds(part * n + c, 1), :], lanes)
        cols = slice(part * span + h * lanes, part * span + (h + 1) * lanes)
        normal = proj[place, cols] * factor
        weighted = up * gains[part : part + 1, h * lanes : (h + 1) * lanes]
        return place, cols, up, factor, normal, weighted

    def first(c, _):
        for part, grad in ((0, dq), (1, dk)):
            products = 0.0
            for h in range(count):
                _, _, up, _, normal, weighted = parts(c, part, h, grad)
                products = products + weighted * normal
            total = lax.dot_general(
                jnp.ones((8, lanes), jnp.float32), products, (((1,), (1,)), ((), ())),
                precision=lax.Precision.HIGHEST, preferred_element_type=jnp.float32,
            )
            sums[pl.ds(part * n + c, 1), :] = total[:1]
        return 0

    lax.fori_loop(0, n, first, 0)
    copies = add_over_seq(n, sums, landed, send_sem, recv_sem, peers)
    gain_grads[...] = jnp.zeros_like(gain_grads)

    def gain_sum(c, _):
        for part, grad in ((0, dq), (1, dk)):
            for h in range(count):
                _, _, up, _, normal, _ = parts(c, part, h, grad)
                cell = (slice(part + 2, part + 3), slice(h * lanes, (h + 1) * lanes))
                gain_grads[cell] += jnp.sum(up * normal, axis=0, keepdims=True)
        place = pl.ds(pl.multiple_of(c * rows, rows), rows)
        grads[place, 2 * span :] = dv[place, :]
        return 0

    lax.fori_loop(0, n, gain_sum, 0)
    total = sums[...]
    for k in range(1, n):
        copies[k - 1].wait_recv()
        total = total + landed[k - 1]
    landed[0] = total / full

    def last(c, _):
        for part, grad in ((0, dq), (1, dk)):
            mean = as_columns(landed[0, pl.ds(part * n + c, 1), :], lanes)
            for h in range(count):
                place, cols, _, factor, normal, weighted = parts(c, part, h, grad)
                grads[place, cols] = (factor * (weighted - normal * mean)).astype(jnp.bfloat16)
        return 0

    lax.fori_loop(0, n, last, 0)
    for copy in copies:
        copy.wait_send()


def heads_back(dq, dk, dv, proj, factors, gains, tables, n, full, collective_id):
    length, span = dq.shape
    vmem = pl.BlockSpec(memory_space=pltpu.VMEM)
    return pl.pallas_call(
        functools.partial(heads_back_kernel, n, full),
        out_shape=(
            jax.ShapeDtypeStruct((length, 3 * span), jnp.bfloat16),
            jax.ShapeDtypeStruct((8, span), jnp.float32),
        ),
        in_specs=[vmem] * 10,
        out_specs=[vmem] * 2,
        scratch_shapes=[
            pltpu.VMEM(factors.shape, jnp.float32),
            pltpu.VMEM((n - 1,) + factors.shape, jnp.float32),
            pltpu.SemaphoreType.DMA((n - 1,)),
            pltpu.SemaphoreType.DMA((n - 1,)),
        ],
        compiler_params=pltpu.CompilerParams(
            collective_id=collective_id, has_side_effects=True, vmem_limit_bytes=40 << 20
        ),
        cost_estimate=work(20),
        name="heads_back",
    )(dq, dk, dv, proj, factors, gains, *tables)


def turn_parts(rows, n, dim):
    half = dim // 2
    frequency = jnp.power(10000.0, -2.0 * jnp.arange(half, dtype=jnp.float32) / dim)
    frequency = jnp.concatenate([frequency, frequency])[None]
    near = jnp.arange(rows, dtype=jnp.float32)[:, None] * frequency
    far = (rows * jnp.arange(n)).astype(jnp.float32)[:, None] * frequency
    return jnp.cos(near), jnp.sin(near), jnp.cos(far), jnp.sin(far)


def inverse_norm(values):
    return lax.rsqrt(jnp.mean(values * values, axis=-1, keepdims=True) + epsilon)


def norm_backward(values, factor, gain, upstream):
    normal = values * factor
    weighted = upstream * gain
    gain_term = jnp.sum(upstream * normal, axis=0)
    back = factor * (weighted - normal * jnp.mean(weighted * normal, axis=-1, keepdims=True))
    return (back, gain_term)


def across_pairs(lines, pair):
    return [(a * pair + b, a * pair + 1 - b) for a in range(lines) for b in range(pair)]


def along_lines(lines, pair, k):
    return [(a * pair + b, (a + k) % lines * pair + b) for a in range(lines) for b in range(pair)]


def gather_column(x, n):
    lines = n // 2
    return [x] + [lax.ppermute(x, "seq", along_lines(lines, 2, k)) for k in range(1, lines)]


def gather_across(column, n):
    return [lax.ppermute(c, "seq", across_pairs(n // 2, 2)) for c in column]


def gather_join(column, other, n):
    lines = n // 2
    me = lax.axis_index("seq")
    a, b = me // 2, me % 2
    out = jnp.zeros((n,) + column[0].shape, column[0].dtype)
    for k in range(lines):
        line = (a + lines - k) % lines
        out = lax.dynamic_update_index_in_dim(out, column[k], line * 2 + b, 0)
        out = lax.dynamic_update_index_in_dim(out, other[k], line * 2 + 1 - b, 0)
    return out


def reduce_across(part, n):
    pair = 2
    b = lax.axis_index("seq") % pair
    halves = part.reshape(n // pair, pair, *part.shape[1:])
    give = lax.dynamic_index_in_dim(halves, 1 - b, 1, keepdims=False)
    keep = lax.dynamic_index_in_dim(halves, b, 1, keepdims=False)
    return keep, lax.ppermute(give, "seq", across_pairs(n // pair, pair))


def reduce_column(keep, got, n):
    lines = n // 2
    a = lax.axis_index("seq") // 2
    sums = (keep.astype(jnp.float32) + got.astype(jnp.float32)).astype(keep.dtype)
    pieces = [lax.dynamic_index_in_dim(sums, a, 0, keepdims=False)]
    for k in range(1, lines):
        piece = lax.dynamic_index_in_dim(sums, (a + k) % lines, 0, keepdims=False)
        pieces.append(lax.ppermute(piece, "seq", along_lines(lines, 2, k)))
    return pieces


def local(
    tokens, routes, route_weights, cotangent, attn_gain, query_gain, key_gain, ffn_gain,
    w_query, w_key, w_value, w_out, w_gate, w_up, w_down,
):
    n = lax.axis_size("seq")
    groups = lax.axis_size("fsdp")
    me = lax.axis_index("seq")
    width = tokens.shape[-1]
    own_tokens = tokens.reshape(-1, width)
    rows = own_tokens.shape[0]
    length = rows * n
    picks = routes.shape[-1]
    local_experts = w_gate.shape[1]
    experts = local_experts * n
    capacity = 3 * rows * picks // (2 * experts)
    head_dim = width // H
    heads = H // n
    span = heads * head_dim
    part = width // (n * groups)
    scale = head_dim ** (-0.5)
    bf, f32 = jnp.bfloat16, jnp.float32
    barrier = lax.optimization_barrier

    own_gains = jnp.stack([attn_gain, query_gain, key_gain, ffn_gain]).astype(f32)
    own_gains = jnp.pad(own_gains, ((0, 4), (0, 0)))
    full_out = lax.all_gather(w_out, "fsdp", axis=0, tiled=True)
    by_expert = lambda w: lax.all_gather(jnp.swapaxes(w, 0, 1), "fsdp", axis=1, tiled=True)
    full_gate = by_expert(w_gate)
    normed, proj, squares, w_heads, gains = project_rows(
        own_tokens, w_query, w_key, w_value, own_gains, n, groups, 8, 0
    )
    cot_own, w_up, w_down, squares = barrier((cotangent.reshape(rows, width), w_up, w_down, squares))
    full_up, full_down = by_expert(w_up), by_expert(w_down)
    cot_column = gather_column(cot_own, n)
    gain_attn, gain_ffn = gains[0], gains[3]
    head_gains = lax.dynamic_slice(gains, (1, me * span), (2, span))

    expert_ids = jnp.arange(experts, dtype=jnp.int32)
    named = routes.reshape(rows, picks)[None] == expert_ids[:, None, None]
    mixing = route_weights.reshape(rows, picks)[None]
    sent = jnp.sum(jnp.where(named, mixing, 0.0), axis=-1).reshape(n, local_experts, rows)
    tables = turn_parts(rows, n, head_dim)
    queries, keys, values, factors, weights = rotate_rows(
        squares, sent, proj, head_gains, tables, n, width, 1
    )
    block = min(512, length)
    heads_out, log_totals = attend(queries, keys, values, heads, block, scale)
    context = lax.all_to_all(heads_out, "seq", split_axis=0, concat_axis=1, tiled=True)
    inputs = own_tokens.astype(f32)
    mid = inputs + jnp.dot(context, full_out, preferred_element_type=f32)
    norm_two = inverse_norm(mid)
    ffn_in = (mid * norm_two * gain_ffn).astype(bf)

    ffn_all = gather_rows(ffn_in, n, 8, 2)
    cot_column, ffn_all = barrier((cot_column, ffn_all))
    cot_other = gather_across(cot_column, n)
    taken = weights > 0
    tri = (jnp.arange(rows)[:, None] <= jnp.arange(rows)[None, :]).astype(bf)
    rank = jnp.einsum("cet,tu->ceu", taken.astype(bf), tri, preferred_element_type=f32) - 1.0
    slot_ids = jnp.arange(capacity, dtype=f32)
    hit = (rank[:, :, None, :] == slot_ids[None, None, :, None]) & taken[:, :, None, :]
    place = hit.astype(bf)
    slot_weight = jnp.sum(jnp.where(hit, weights[:, :, None, :], 0.0), axis=-1)
    slot_weight = jnp.swapaxes(slot_weight, 0, 1)[..., None]
    place_rows = lambda v: jnp.einsum("cert,ctd->ecrd", place, v, preferred_element_type=f32)
    unplace = lambda v: jnp.einsum("cert,ecrd->ctd", place, v, preferred_element_type=f32).astype(bf)
    received = place_rows(ffn_all).astype(bf)
    gate = jnp.einsum("ecrd,edf->ecrf", received, full_gate, preferred_element_type=f32)
    up_part = jnp.einsum("ecrd,edf->ecrf", received, full_up, preferred_element_type=f32)
    sigmoid_gate = jax.nn.sigmoid(gate)
    activated = gate * sigmoid_gate
    hidden = (activated * up_part).astype(bf)
    expert_out = jnp.einsum("ecrf,edf->ecrd", hidden, full_down, preferred_element_type=f32)
    expert_out = (expert_out * slot_weight).astype(bf)
    ffn_part = unplace(expert_out)
    ffn_part, cot_other = barrier((ffn_part, cot_other))
    cot_all = gather_join(cot_column, cot_other, n)
    ffn_keep, ffn_got = reduce_across(ffn_part, n)

    out_grad = cotangent.reshape(rows, width).astype(f32)
    down_received = (place_rows(cot_all) * slot_weight).astype(bf)
    hidden_grad = jnp.einsum("ecrd,edf->ecrf", down_received, full_down, preferred_element_type=f32)
    slope = sigmoid_gate * (1.0 + gate * (1.0 - sigmoid_gate))
    gate_grad = (hidden_grad * up_part * slope).astype(bf)
    up_grad = (hidden_grad * activated).astype(bf)
    rows_grad = (
        jnp.einsum("ecrf,edf->ecrd", gate_grad, full_gate, preferred_element_type=f32)
        + jnp.einsum("ecrf,edf->ecrd", up_grad, full_up, preferred_element_type=f32)
    ).astype(bf)
    term = lambda a, b: jnp.einsum("ecrd,ecrf->edf", a, b, preferred_element_type=f32).astype(bf)
    scatter = lambda v: lax.psum_scatter(v, "fsdp", scatter_dimension=1, tiled=True)
    rows_part, ffn_keep, ffn_got, down_term, gate_term, up_term = barrier(
        (
            unplace(rows_grad),
            ffn_keep,
            ffn_got,
            term(down_received, hidden),
            term(received, gate_grad),
            term(received, up_grad),
        )
    )
    scattered = [scatter(down_term), scatter(gate_term), scatter(up_term)]
    ffn_in_grad = reduce_rows(rows_part, n, 8, 4)
    mid_back, ffn_gain_term = norm_backward(mid, norm_two, gain_ffn, ffn_in_grad)
    mid_grad = out_grad + mid_back
    branch_grad = mid_grad.astype(bf)

    branch_all = gather_rows(branch_grad, n, 8, 5).reshape(length, width)
    branch_all, ffn_keep, ffn_got = barrier((branch_all, ffn_keep, ffn_got))
    ffn_pieces = reduce_column(ffn_keep, ffn_got, n)
    out_rows = lax.dynamic_slice_in_dim(full_out, me * span, span, 0)
    heads_grad = jnp.einsum("te,de->td", branch_all, out_rows, preferred_element_type=f32).astype(bf)
    out_term = jnp.einsum("td,te->de", heads_out, branch_all, preferred_element_type=f32).astype(bf)
    query_back, key_back, value_back = attend_back(
        queries, keys, values, heads_grad, heads_out, log_totals, heads, block, scale
    )
    proj_grad, gain_terms = heads_back(
        query_back, key_back, value_back, proj, factors, head_gains, tables, n, width, 6
    )
    normed_part = jnp.einsum("te,de->td", proj_grad, w_heads, preferred_element_type=f32).astype(bf)
    head_term = jnp.einsum("td,te->de", normed, proj_grad, preferred_element_type=f32).astype(bf)
    head_term = head_term.reshape(n, groups, part, 3 * span).swapaxes(0, 1)
    normed_part, ffn_pieces, out_term, head_term, down_sum, gate_sum = barrier(
        (normed_part, ffn_pieces, out_term, head_term, *scattered[:2])
    )
    block_out = mid + sum(piece.astype(f32) for piece in ffn_pieces)
    out_sum = lax.psum_scatter(out_term, "fsdp", scatter_dimension=0, tiled=True).astype(f32)
    gate_sum, down_sum = widen(gate_sum), widen(down_sum)
    normed_grad = reduce_rows(normed_part.reshape(n, rows, width), n, 8, 7)
    input_back, attn_gain_term = norm_backward(inputs, inverse_norm(inputs), gain_attn, normed_grad)
    tokens_grad = mid_grad + input_back
    head_term, up_sum = barrier((head_term, scattered[2]))
    up_sum = widen(up_sum)
    head_term = lax.psum_scatter(head_term, "fsdp", scatter_dimension=0, tiled=True)
    head_term = head_term.reshape(n, part, 3, span)
    head_term = lax.all_to_all(head_term, "seq", split_axis=0, concat_axis=0, tiled=True)
    head_sums = [
        head_term[:, :, i].swapaxes(0, 1).reshape(part, width).astype(f32) for i in range(3)
    ]
    by_span = lambda v: v.reshape(n, 1, span)
    sent_gains = jnp.concatenate([by_span(attn_gain_term), by_span(ffn_gain_term)], axis=1)
    sent_gains = jnp.pad(sent_gains, ((0, 0), (0, 6), (0, 0)))
    gain_sums = sum_gains(sent_gains, gain_terms, n, groups, 8)
    gain_sums = lax.dynamic_slice_in_dim(gain_sums, lax.axis_index("fsdp") * part, part, 1)
    return (
        block_out.astype(bf).reshape(tokens.shape),
        tokens_grad.reshape(tokens.shape),
        gain_sums[0],
        gain_sums[2],
        gain_sums[3],
        gain_sums[1],
        head_sums[0],
        head_sums[1],
        head_sums[2],
        out_sum,
        gate_sum,
        up_sum,
        down_sum,
    )


def solution(mesh):
    rows3 = P("fsdp", "seq", None)
    both = P(("seq", "fsdp"))
    both2 = P(("seq", "fsdp"), None)
    placed = (rows3,) * 4 + (P("fsdp"),) * 4 + (P("fsdp", None),) * 4 + (rows3,) * 3
    return jax.shard_map(
        local,
        mesh=mesh,
        in_specs=placed,
        out_specs=(rows3,) * 2 + (both,) * 4 + (both2,) * 4 + (rows3,) * 3,
        check_vma=False,
    )
```

```python
import functools
import jax
import jax.numpy as jnp
from jax import lax
from jax.experimental import pallas as pl
from jax.experimental.pallas import tpu as pltpu
from jax.sharding import PartitionSpec as P

MESH = pl.DeviceIdType.MESH
ANY = pl.ANY
H = 16
epsilon = 1e-05


def work(us):
    return pl.CostEstimate(flops=int(us * 6e8), bytes_accessed=0, transcendentals=0)


def greet(peers):
    barrier = pltpu.get_barrier_semaphore()
    for peer in peers:
        pl.semaphore_signal(barrier, inc=1, device_id={"seq": peer}, device_id_type=MESH)
    pl.semaphore_wait(barrier, len(peers))


def push(src, dst, send, recv, peer):
    return pltpu.make_async_remote_copy(
        src_ref=src, dst_ref=dst, send_sem=send, recv_sem=recv,
        device_id={"seq": peer}, device_id_type=MESH)


def gather_kernel(n, pieces, by_index, own, out, send_sem, recv_sem, copy_sem):
    pair = 2
    lines = n // pair
    me = lax.axis_index("seq")
    a, b = me // pair, me % pair
    column = [((a + k) % lines) * pair + b for k in range(1, lines)]
    across = a * pair + (1 - b)
    greet(column + [across])
    rows = own.shape[0] // pieces
    if by_index:
        here = [((a + lines - k) % lines) * pair + b for k in range(lines)]
        there = [((a + lines - k) % lines) * pair + 1 - b for k in range(lines)]
        sent = [me] * lines
        relayed = here
    else:
        here, there = list(range(lines)), list(range(lines, n))
        sent = here
        relayed = there
    local = pltpu.make_async_copy(own, out.at[here[0]], copy_sem)
    local.start()

    def piece(p):
        return pl.ds(p * rows, rows)

    sends = []
    for p in range(pieces):
        for k in range(lines):
            peer = across if k == 0 else column[k - 1]
            place = relayed[0] if k == 0 else sent[k]
            copy = push(own.at[piece(p)], out.at[place, piece(p)], send_sem.at[k, p], recv_sem.at[k, p], peer)
            copy.start()
            sends.append(copy)
    relays = []
    for p in range(pieces):
        for k in range(1, lines):
            push(own.at[piece(p)], out.at[here[k], piece(p)], send_sem.at[k, p], recv_sem.at[k, p], across).wait_recv()
            slot = lines + k - 1
            copy = push(
                out.at[here[k], piece(p)], out.at[relayed[k], piece(p)], send_sem.at[slot, p], recv_sem.at[slot, p], across
            )
            copy.start()
            relays.append(copy)
    for p in range(pieces):
        push(own.at[piece(p)], out.at[there[0], piece(p)], send_sem.at[0, p], recv_sem.at[0, p], across).wait_recv()
    for copy in relays:
        copy.wait_recv()
    for copy in sends + relays:
        copy.wait_send()
    local.wait()


def gather_rows(x, n, pieces, by_index, collective_id):
    slots = n // 2 + n // 2 - 1
    return pl.pallas_call(
        functools.partial(gather_kernel, n, pieces, by_index),
        out_shape=jax.ShapeDtypeStruct((n,) + x.shape, x.dtype),
        in_specs=[pl.BlockSpec(memory_space=pltpu.VMEM)],
        out_specs=pl.BlockSpec(memory_space=ANY),
        scratch_shapes=[
            pltpu.SemaphoreType.DMA((slots, pieces)),
            pltpu.SemaphoreType.DMA((slots, pieces)),
            pltpu.SemaphoreType.DMA,
        ],
        compiler_params=pltpu.CompilerParams(collective_id=collective_id, has_side_effects=True),
        cost_estimate=work(105),
        name="gather_rows",
    )(x)


def reduce_kernel(n, pieces, by_index, part, out, mine, got, sums, landed, send_sem, recv_sem, load_sem):
    pair = 2
    lines = n // pair
    me = lax.axis_index("seq")
    a, b = me // pair, me % pair
    column = [((a + lines - k) % lines) * pair + b for k in range(1, lines)]
    across = a * pair + (1 - b)
    greet(column + [across])
    rows = out.shape[0] // pieces
    order = list(range(1, lines)) + [0]
    if by_index:
        here = [((a + lines - k) % lines) * pair + b for k in range(lines)]
        there = [((a + lines - k) % lines) * pair + 1 - b for k in range(lines)]
    else:
        here, there = list(range(lines)), list(range(lines, n))

    def piece(p):
        return pl.ds(p * rows, rows)

    firsts, loads = {}, {}
    for k in order:
        for p in range(pieces):
            copy = push(part.at[there[k], piece(p)], got.at[k, piece(p)],
                        send_sem.at[k, p], recv_sem.at[k, p], across)
            copy.start()
            firsts[k, p] = copy
            load = pltpu.make_async_copy(part.at[here[k], piece(p)], mine.at[k, piece(p)], load_sem.at[k, p])
            load.start()
            loads[k, p] = load
    seconds = {}
    for k in order:
        for p in range(pieces):
            firsts[k, p].wait_recv()
            loads[k, p].wait()
            total = mine[k, piece(p)].astype(jnp.float32) + got[k, piece(p)].astype(jnp.float32)
            if k:
                sums[k - 1, piece(p)] = total.astype(jnp.bfloat16)
                slot = lines + k - 1
                copy = push(sums.at[k - 1, piece(p)], landed.at[k - 1, piece(p)],
                            send_sem.at[slot, p], recv_sem.at[slot, p], column[k - 1])
                copy.start()
                seconds[k, p] = copy
            else:
                for j in range(1, lines):
                    seconds[j, p].wait_recv()
                    total += landed[j - 1, piece(p)].astype(jnp.float32)
                out[piece(p), :] = total
    for copy in list(firsts.values()) + list(seconds.values()):
        copy.wait_send()


def reduce_rows(part, n, pieces, by_index, collective_id):
    _, rows, width = part.shape
    lines = n // 2
    slots = lines + lines - 1
    return pl.pallas_call(
        functools.partial(reduce_kernel, n, pieces, by_index),
        out_shape=jax.ShapeDtypeStruct((rows, width), jnp.float32),
        in_specs=[pl.BlockSpec(memory_space=ANY)],
        out_specs=pl.BlockSpec(memory_space=pltpu.VMEM),
        scratch_shapes=[
            pltpu.VMEM((lines, rows, width), jnp.bfloat16),
            pltpu.VMEM((lines, rows, width), jnp.bfloat16),
            pltpu.VMEM((lines - 1, rows, width), jnp.bfloat16),
            pltpu.VMEM((lines - 1, rows, width), jnp.bfloat16),
            pltpu.SemaphoreType.DMA((slots, pieces)),
            pltpu.SemaphoreType.DMA((slots, pieces)),
            pltpu.SemaphoreType.DMA((lines, pieces)),
        ],
        compiler_params=pltpu.CompilerParams(collective_id=collective_id, has_side_effects=True),
        cost_estimate=work(98),
        name="reduce_rows",
    )(part)


def gains_kernel(n, groups, sent, own, out, taken, summed, landed, send_sem, recv_sem, side_send, side_recv):
    me, group = lax.axis_index("seq"), lax.axis_index("fsdp")
    barrier = pltpu.get_barrier_semaphore()
    peers = [(me + k) % n for k in range(1, n)]
    mates = [(group + k) % groups for k in range(1, groups)]
    for peer in peers:
        pl.semaphore_signal(barrier, inc=1, device_id={"seq": peer}, device_id_type=MESH)
    for mate in mates:
        pl.semaphore_signal(barrier, inc=1, device_id={"fsdp": mate}, device_id_type=MESH)
    pl.semaphore_wait(barrier, n - 1 + groups - 1)
    copies = []
    for k in range(1, n):
        copy = push(sent.at[peers[k - 1]], taken.at[k - 1], send_sem.at[k - 1], recv_sem.at[k - 1], peers[k - 1])
        copy.start()
        copies.append(copy)
    total = sent[me] + own[...]
    for k in range(1, n):
        copies[k - 1].wait_recv()
        total = total + taken[k - 1]
    summed[...] = total
    sides = []
    for k in range(1, groups):
        side = pltpu.make_async_remote_copy(
            src_ref=summed, dst_ref=landed.at[k - 1], send_sem=side_send.at[k - 1], recv_sem=side_recv.at[k - 1],
            device_id={"fsdp": mates[k - 1]}, device_id_type=MESH)
        side.start()
        sides.append(side)
    for k in range(1, groups):
        sides[k - 1].wait_recv()
        total = total + landed[k - 1]
    out[...] = total
    for copy in copies + sides:
        copy.wait_send()


def sum_gains(sent, own, n, groups, collective_id):
    shape = own.shape
    return pl.pallas_call(
        functools.partial(gains_kernel, n, groups),
        out_shape=jax.ShapeDtypeStruct(shape, own.dtype),
        in_specs=[pl.BlockSpec(memory_space=pltpu.VMEM)] * 2,
        out_specs=pl.BlockSpec(memory_space=pltpu.VMEM),
        scratch_shapes=[
            pltpu.VMEM((n - 1,) + shape, own.dtype),
            pltpu.VMEM(shape, own.dtype),
            pltpu.VMEM((groups - 1,) + shape, own.dtype),
            pltpu.SemaphoreType.DMA((n - 1,)),
            pltpu.SemaphoreType.DMA((n - 1,)),
            pltpu.SemaphoreType.DMA((groups - 1,)),
            pltpu.SemaphoreType.DMA((groups - 1,)),
        ],
        compiler_params=pltpu.CompilerParams(collective_id=collective_id, has_side_effects=True),
        cost_estimate=work(10),
        name="sum_gains",
    )(sent, own)


def widen_kernel(x_ref, o_ref):
    for e in range(x_ref.shape[0]):
        o_ref[:, e, :] = x_ref[e].astype(jnp.float32)


def widen(x):
    experts, rows, columns = x.shape
    step = min(128, rows)
    return pl.pallas_call(
        widen_kernel,
        grid=(rows // step,),
        out_shape=jax.ShapeDtypeStruct((rows, experts, columns), jnp.float32),
        in_specs=[pl.BlockSpec((experts, step, columns), lambda i: (0, i, 0))],
        out_specs=pl.BlockSpec((step, experts, columns), lambda i: (i, 0, 0)),
        cost_estimate=work(5),
        name="widen",
    )(x)


def masked(block):
    keys = lax.broadcasted_iota(jnp.int32, (block, block), 0)
    rows = lax.broadcasted_iota(jnp.int32, (block, block), 1)
    return keys <= rows


def across_lanes(a, b):
    return lax.dot_general(a, b, (((1,), (1,)), ((), ())), preferred_element_type=jnp.float32)


def down_rows(a, b):
    return lax.dot_general(a, b, (((0,), (0,)), ((), ())), preferred_element_type=jnp.float32)


LOG2E = 1.4426950408889634


def attend_kernel(block, scale, q_ref, k_ref, v_ref, o_ref, lse_ref, s_ref, acc_ref):
    length, dim = q_ref.shape

    def rows(i):
        return pl.ds(pl.multiple_of(i * block, block), block)

    def one_block(i, _):
        q = q_ref[rows(i), :]
        diag = across_lanes(k_ref[rows(i), :], q) * (scale * LOG2E)
        diag = jnp.where(masked(block), diag, -1e30)
        s_ref[rows(i), :] = diag
        peak = jnp.max(diag, axis=0, keepdims=True)

        def score(j, peak):
            s = across_lanes(k_ref[rows(j), :], q) * (scale * LOG2E)
            s_ref[rows(j), :] = s
            return jnp.maximum(peak, jnp.max(s, axis=0, keepdims=True))

        peak = lax.fori_loop(0, i, score, peak)
        acc_ref[...] = jnp.zeros_like(acc_ref)

        def weigh(j, total):
            p = jnp.exp2(s_ref[rows(j), :] - peak)
            acc_ref[...] += down_rows(v_ref[rows(j), :], p.astype(jnp.bfloat16))
            return total + jnp.sum(p, axis=0, keepdims=True)

        total = lax.fori_loop(0, i + 1, weigh, jnp.zeros_like(peak))
        o_ref[rows(i), :] = (acc_ref[...] / total).T.astype(o_ref.dtype)
        lse_ref[0, :, rows(i)] = peak + jnp.log2(total)
        return 0

    lax.fori_loop(0, length // block, one_block, 0)


def attend(q, k, v, heads, block, scale):
    length, width = q.shape
    dim = width // heads
    spec = pl.BlockSpec((length, dim), lambda h: (0, h))
    return pl.pallas_call(
        functools.partial(attend_kernel, block, scale),
        grid=(heads,),
        out_shape=(
            jax.ShapeDtypeStruct(q.shape, q.dtype),
            jax.ShapeDtypeStruct((heads, 1, length), jnp.float32),
        ),
        in_specs=[spec] * 3,
        out_specs=[spec, pl.BlockSpec((1, 1, length), lambda h: (h, 0, 0))],
        scratch_shapes=[
            pltpu.VMEM((length, block), jnp.float32),
            pltpu.VMEM((dim, block), jnp.float32),
        ],
        cost_estimate=work(25),
        name="attend",
    )(q, k, v)


def attend_back_kernel(
    block, scale, q_ref, k_ref, v_ref, g_ref, o_ref, lse_ref, dq_ref, dk_ref, dv_ref, dk_acc, dv_acc, dq_acc
):
    length, dim = q_ref.shape
    dk_acc[...] = jnp.zeros_like(dk_acc)
    dv_acc[...] = jnp.zeros_like(dv_acc)

    def rows(i):
        return pl.ds(pl.multiple_of(i * block, block), block)

    def one_block(i, _):
        q, g = q_ref[rows(i), :], g_ref[rows(i), :]
        lse = lse_ref[0, :, rows(i)]
        products = g.astype(jnp.float32) * o_ref[rows(i), :].astype(jnp.float32)
        shift = lax.dot_general(
            jnp.ones((8, dim), jnp.float32), products, (((1,), (1,)), ((), ())),
            precision=lax.Precision.HIGHEST, preferred_element_type=jnp.float32,
        )[:1]

        def pair(j, keep):
            k, v = k_ref[rows(j), :], v_ref[rows(j), :]
            p = jnp.exp2(across_lanes(k, q) * (scale * LOG2E) - lse)
            if keep is not None:
                p = jnp.where(keep, p, 0.0)
            ds = (p * (across_lanes(v, g) - shift) * scale).astype(jnp.bfloat16)
            dv_acc[rows(j), :] += jnp.dot(p.astype(jnp.bfloat16), g, preferred_element_type=jnp.float32)
            dk_acc[rows(j), :] += jnp.dot(ds, q, preferred_element_type=jnp.float32)
            dq_acc[...] += down_rows(k, ds)

        dq_acc[...] = jnp.zeros_like(dq_acc)
        pair(i, masked(block))

        def body(j, _):
            pair(j, None)
            return 0

        lax.fori_loop(0, i, body, 0)
        dq_ref[rows(i), :] = dq_acc[...].T.astype(dq_ref.dtype)
        return 0

    lax.fori_loop(0, length // block, one_block, 0)
    dk_ref[...] = dk_acc[...].astype(dk_ref.dtype)
    dv_ref[...] = dv_acc[...].astype(dv_ref.dtype)


def attend_back(q, k, v, g, o, lse, heads, block, scale):
    length, width = q.shape
    dim = width // heads
    spec = pl.BlockSpec((length, dim), lambda h: (0, h))
    return pl.pallas_call(
        functools.partial(attend_back_kernel, block, scale),
        grid=(heads,),
        out_shape=(jax.ShapeDtypeStruct(q.shape, q.dtype),) * 3,
        in_specs=[spec] * 5 + [pl.BlockSpec((1, 1, length), lambda h: (h, 0, 0))],
        out_specs=[spec] * 3,
        scratch_shapes=[
            pltpu.VMEM((length, dim), jnp.float32),
            pltpu.VMEM((length, dim), jnp.float32),
            pltpu.VMEM((dim, block), jnp.float32),
        ],
        cost_estimate=work(60),
        name="attend_back",
    )(q, k, v, g, o, lse)


def project_kernel(
    n, groups, pieces, own, w_query, w_key, w_value, gain_own,
    normed, proj, squares, w_ref, gains, held, send_sem, recv_sem, side_send, side_recv, copy_sem
):
    pair = 2
    lines = n // pair
    me, group = lax.axis_index("seq"), lax.axis_index("fsdp")
    a, b = me // pair, me % pair
    column = [((a + k) % lines) * pair + b for k in range(1, lines)]
    back = [((a + lines - k) % lines) * pair + b for k in range(1, lines)]
    across = a * pair + (1 - b)
    mates = [(group + k) % groups for k in range(1, groups)]
    barrier = pltpu.get_barrier_semaphore()
    for peer in column + [across]:
        pl.semaphore_signal(barrier, inc=1, device_id={"seq": peer}, device_id_type=MESH)
    for mate in mates:
        pl.semaphore_signal(barrier, inc=1, device_id={"fsdp": mate}, device_id_type=MESH)
    pl.semaphore_wait(barrier, lines + groups - 1)
    rows, width = own.shape
    step = rows // pieces
    span = w_ref.shape[1] // 3
    shard = w_query.shape[0]

    def piece(p):
        return pl.ds(p * step, step)

    sends = []
    for p in range(pieces):
        for k in range(lines):
            peer = across if k == 0 else column[k - 1]
            copy = push(own.at[piece(p)], held.at[me, piece(p)], send_sem.at[k, p], recv_sem.at[k, p], peer)
            copy.start()
            sends.append(copy)

    shard_rows = pl.ds(pl.multiple_of(group * shard, shard), shard)
    mine = pl.ds(pl.multiple_of(me * span, span), span)
    blocks = [
        (w.at[:, mine], w_ref.at[shard_rows, part * span : (part + 1) * span])
        for part, w in enumerate((w_query, w_key, w_value))
    ]
    blocks.append((gain_own, gains.at[:, shard_rows]))
    locals_, sides = [], []
    for i, (src, dst) in enumerate(blocks):
        for k in range(1, groups):
            side = pltpu.make_async_remote_copy(
                src_ref=src, dst_ref=dst, send_sem=side_send.at[i, k - 1], recv_sem=side_recv.at[i, k - 1],
                device_id={"fsdp": mates[k - 1]}, device_id_type=MESH)
            side.start()
            sides.append(side)
        local = pltpu.make_async_copy(src, dst, copy_sem.at[i])
        local.start()
        locals_.append(local)

    def project(src, chunk):
        x = chunk[...].astype(jnp.float32)
        factor = lax.rsqrt(jnp.mean(x * x, axis=-1, keepdims=True) + epsilon)
        place = pl.ds(pl.multiple_of(src * rows, rows), rows)
        normed[place, :] = (x * factor * gains[0:1, :]).astype(jnp.bfloat16)
        for part in range(3):
            cols = slice(part * span, (part + 1) * span)
            out = jnp.dot(normed[place, :], w_ref[:, cols], preferred_element_type=jnp.float32)
            proj[place, cols] = out
            if part < 2:
                sums = lax.dot_general(
                    jnp.ones((8, span), jnp.float32), out * out, (((1,), (1,)), ((), ())),
                    precision=lax.Precision.HIGHEST, preferred_element_type=jnp.float32,
                )
                squares[pl.ds(part * n + src, 1), :] = sums[:1]

    relays = []
    for p in range(pieces):
        for k in range(1, lines):
            src = back[k - 1]
            push(own.at[piece(p)], held.at[src, piece(p)], send_sem.at[k, p], recv_sem.at[k, p], across).wait_recv()
            slot = lines + k - 1
            copy = push(held.at[src, piece(p)], held.at[src, piece(p)], send_sem.at[slot, p], recv_sem.at[slot, p], across)
            copy.start()
            relays.append(copy)
    for copy in locals_:
        copy.wait()
    for side in sides:
        side.wait_recv()
    project(me, own)
    for p in range(pieces):
        push(own.at[piece(p)], held.at[across, piece(p)], send_sem.at[0, p], recv_sem.at[0, p], across).wait_recv()
    project(across, held.at[across])
    for k in range(1, lines):
        project(back[k - 1], held.at[back[k - 1]])
    for k in range(1, lines):
        for p in range(pieces):
            relays[p * (lines - 1) + k - 1].wait_recv()
        src = ((a + lines - k) % lines) * pair + 1 - b
        project(src, held.at[src])
    for copy in sends + relays + sides:
        copy.wait_send()


def project_rows(x, w_query, w_key, w_value, gains, n, groups, pieces, collective_id):
    rows, width = x.shape
    span = w_query.shape[1] // n
    slots = n // 2 + n // 2 - 1
    vmem = pl.BlockSpec(memory_space=pltpu.VMEM)
    hbm = pl.BlockSpec(memory_space=ANY)
    return pl.pallas_call(
        functools.partial(project_kernel, n, groups, pieces),
        out_shape=(
            jax.ShapeDtypeStruct((n * rows, width), jnp.bfloat16),
            jax.ShapeDtypeStruct((n * rows, 3 * span), jnp.float32),
            jax.ShapeDtypeStruct((2 * n, rows), jnp.float32),
            jax.ShapeDtypeStruct((width, 3 * span), jnp.bfloat16),
            jax.ShapeDtypeStruct((8, width), jnp.float32),
        ),
        in_specs=[vmem, hbm, hbm, hbm, vmem],
        out_specs=[vmem] * 5,
        scratch_shapes=[
            pltpu.VMEM((n, rows, width), jnp.bfloat16),
            pltpu.SemaphoreType.DMA((slots, pieces)),
            pltpu.SemaphoreType.DMA((slots, pieces)),
            pltpu.SemaphoreType.DMA((4, groups - 1)),
            pltpu.SemaphoreType.DMA((4, groups - 1)),
            pltpu.SemaphoreType.DMA((4,)),
        ],
        compiler_params=pltpu.CompilerParams(
            collective_id=collective_id, has_side_effects=True, vmem_limit_bytes=50 << 20
        ),
        cost_estimate=work(110),
        name="project_rows",
    )(x, w_query, w_key, w_value, gains)


def as_columns(row, lanes):
    return jnp.broadcast_to(row, (lanes, row.shape[1])).T


def turn_tables(c, near_cos, near_sin, far_cos, far_sin):
    far_c, far_s = far_cos[pl.ds(c, 1), :], far_sin[pl.ds(c, 1), :]
    cosine = near_cos[...] * far_c - near_sin[...] * far_s
    sine = near_sin[...] * far_c + near_cos[...] * far_s
    first = lax.broadcasted_iota(jnp.int32, sine.shape, 1) < sine.shape[1] // 2
    return cosine, jnp.where(first, -sine, sine)


def add_over_seq(n, own, landed, send_sem, recv_sem, peers):
    copies = []
    for k in range(1, n):
        copy = push(own, landed.at[k - 1], send_sem.at[k - 1], recv_sem.at[k - 1], peers[k - 1])
        copy.start()
        copies.append(copy)
    return copies


def rotate_kernel(
    n, full, squares, sent, proj, gains, near_cos, near_sin, far_cos, far_sin,
    queries, keys, values, factors, taken, landed, send_sem, recv_sem, copy_sem
):
    me = lax.axis_index("seq")
    peers = [(me + k) % n for k in range(1, n)]
    greet(peers)
    local = pltpu.make_async_copy(sent.at[me], taken.at[me], copy_sem)
    local.start()
    copies = add_over_seq(n, squares, landed, send_sem.at[0], recv_sem.at[0], peers)
    swaps = []
    for k in range(1, n):
        swap = push(sent.at[peers[k - 1]], taken.at[me], send_sem.at[1, k - 1], recv_sem.at[1, k - 1], peers[k - 1])
        swap.start()
        swaps.append(swap)
    span = queries.shape[1]
    rows = squares.shape[1]
    lanes = near_cos.shape[1]
    total = squares[...]
    for k in range(1, n):
        copies[k - 1].wait_recv()
        total = total + landed[k - 1]
    factors[...] = lax.rsqrt(total / full + epsilon)

    def chunk(c, _):
        place = pl.ds(pl.multiple_of(c * rows, rows), rows)
        cosine, sine = turn_tables(c, near_cos, near_sin, far_cos, far_sin)
        for part, out in ((0, queries), (1, keys)):
            factor = as_columns(factors[pl.ds(part * n + c, 1), :], lanes)
            for h in range(span // lanes):
                cols = slice(part * span + h * lanes, part * span + (h + 1) * lanes)
                x = proj[place, cols] * factor * gains[part : part + 1, h * lanes : (h + 1) * lanes]
                turned = x * cosine + pltpu.roll(x, lanes // 2, 1) * sine
                out[place, h * lanes : (h + 1) * lanes] = turned.astype(jnp.bfloat16)
        values[place, :] = proj[place, 2 * span :].astype(jnp.bfloat16)
        return 0

    lax.fori_loop(0, n, chunk, 0)
    for copy in copies:
        copy.wait_send()
    for swap in swaps:
        swap.wait()
    local.wait()


def rotate_rows(squares, sent, proj, gains, tables, n, full, collective_id):
    length, outs = proj.shape
    span = outs // 3
    vmem = pl.BlockSpec(memory_space=pltpu.VMEM)
    heads = jax.ShapeDtypeStruct((length, span), jnp.bfloat16)
    return pl.pallas_call(
        functools.partial(rotate_kernel, n, full),
        out_shape=(
            heads, heads, heads,
            jax.ShapeDtypeStruct(squares.shape, jnp.float32),
            jax.ShapeDtypeStruct(sent.shape, sent.dtype),
        ),
        in_specs=[vmem] * 8,
        out_specs=[vmem] * 5,
        scratch_shapes=[
            pltpu.VMEM((n - 1,) + squares.shape, jnp.float32),
            pltpu.SemaphoreType.DMA((2, n - 1)),
            pltpu.SemaphoreType.DMA((2, n - 1)),
            pltpu.SemaphoreType.DMA,
        ],
        compiler_params=pltpu.CompilerParams(
            collective_id=collective_id, has_side_effects=True, vmem_limit_bytes=40 << 20
        ),
        cost_estimate=work(15),
        name="rotate_rows",
    )(squares, sent, proj, gains, *tables)


def heads_back_kernel(
    n, full, dq, dk, dv, proj, factors, gains, near_cos, near_sin, far_cos, far_sin,
    grads, gain_grads, sums, landed, send_sem, recv_sem
):
    me = lax.axis_index("seq")
    peers = [(me + k) % n for k in range(1, n)]
    greet(peers)
    span = dq.shape[1]
    rows = sums.shape[1]
    lanes = near_cos.shape[1]
    count = span // lanes

    def parts(c, part, h, grad):
        place = pl.ds(pl.multiple_of(c * rows, rows), rows)
        cosine, sine = turn_tables(c, near_cos, near_sin, far_cos, far_sin)
        g = grad[place, h * lanes : (h + 1) * lanes].astype(jnp.float32)
        up = g * cosine + pltpu.roll(g * sine, lanes // 2, 1)
        factor = as_columns(factors[pl.ds(part * n + c, 1), :], lanes)
        cols = slice(part * span + h * lanes, part * span + (h + 1) * lanes)
        normal = proj[place, cols] * factor
        weighted = up * gains[part : part + 1, h * lanes : (h + 1) * lanes]
        return place, cols, up, factor, normal, weighted

    def first(c, _):
        for part, grad in ((0, dq), (1, dk)):
            products = 0.0
            for h in range(count):
                _, _, up, _, normal, weighted = parts(c, part, h, grad)
                products = products + weighted * normal
            total = lax.dot_general(
                jnp.ones((8, lanes), jnp.float32), products, (((1,), (1,)), ((), ())),
                precision=lax.Precision.HIGHEST, preferred_element_type=jnp.float32,
            )
            sums[pl.ds(part * n + c, 1), :] = total[:1]
        return 0

    lax.fori_loop(0, n, first, 0)
    copies = add_over_seq(n, sums, landed, send_sem, recv_sem, peers)
    gain_grads[...] = jnp.zeros_like(gain_grads)

    def gain_sum(c, _):
        for part, grad in ((0, dq), (1, dk)):
            for h in range(count):
                _, _, up, _, normal, _ = parts(c, part, h, grad)
                cell = (slice(part + 2, part + 3), slice(h * lanes, (h + 1) * lanes))
                gain_grads[cell] += jnp.sum(up * normal, axis=0, keepdims=True)
        place = pl.ds(pl.multiple_of(c * rows, rows), rows)
        grads[place, 2 * span :] = dv[place, :]
        return 0

    lax.fori_loop(0, n, gain_sum, 0)
    total = sums[...]
    for k in range(1, n):
        copies[k - 1].wait_recv()
        total = total + landed[k - 1]
    landed[0] = total / full

    def last(c, _):
        for part, grad in ((0, dq), (1, dk)):
            mean = as_columns(landed[0, pl.ds(part * n + c, 1), :], lanes)
            for h in range(count):
                place, cols, _, factor, normal, weighted = parts(c, part, h, grad)
                grads[place, cols] = (factor * (weighted - normal * mean)).astype(jnp.bfloat16)
        return 0

    lax.fori_loop(0, n, last, 0)
    for copy in copies:
        copy.wait_send()


def heads_back(dq, dk, dv, proj, factors, gains, tables, n, full, collective_id):
    length, span = dq.shape
    vmem = pl.BlockSpec(memory_space=pltpu.VMEM)
    return pl.pallas_call(
        functools.partial(heads_back_kernel, n, full),
        out_shape=(
            jax.ShapeDtypeStruct((length, 3 * span), jnp.bfloat16),
            jax.ShapeDtypeStruct((8, span), jnp.float32),
        ),
        in_specs=[vmem] * 10,
        out_specs=[vmem] * 2,
        scratch_shapes=[
            pltpu.VMEM(factors.shape, jnp.float32),
            pltpu.VMEM((n - 1,) + factors.shape, jnp.float32),
            pltpu.SemaphoreType.DMA((n - 1,)),
            pltpu.SemaphoreType.DMA((n - 1,)),
        ],
        compiler_params=pltpu.CompilerParams(
            collective_id=collective_id, has_side_effects=True, vmem_limit_bytes=40 << 20
        ),
        cost_estimate=work(20),
        name="heads_back",
    )(dq, dk, dv, proj, factors, gains, *tables)


def turn_parts(rows, n, dim):
    half = dim // 2
    frequency = jnp.power(10000.0, -2.0 * jnp.arange(half, dtype=jnp.float32) / dim)
    frequency = jnp.concatenate([frequency, frequency])[None]
    near = jnp.arange(rows, dtype=jnp.float32)[:, None] * frequency
    far = (rows * jnp.arange(n)).astype(jnp.float32)[:, None] * frequency
    return jnp.cos(near), jnp.sin(near), jnp.cos(far), jnp.sin(far)


def inverse_norm(values):
    return lax.rsqrt(jnp.mean(values * values, axis=-1, keepdims=True) + epsilon)


def norm_backward(values, factor, gain, upstream):
    normal = values * factor
    weighted = upstream * gain
    gain_term = jnp.sum(upstream * normal, axis=0)
    back = factor * (weighted - normal * jnp.mean(weighted * normal, axis=-1, keepdims=True))
    return (back, gain_term)


def across_pairs(lines, pair):
    return [(a * pair + b, a * pair + 1 - b) for a in range(lines) for b in range(pair)]


def along_lines(lines, pair, k):
    return [(a * pair + b, (a + k) % lines * pair + b) for a in range(lines) for b in range(pair)]


def by_place(v, n):
    lines = n // 2
    me = lax.axis_index("seq")
    a, b = me // 2, me % 2
    column = [((a + lines - k) % lines) * 2 for k in range(lines)]
    order = jnp.stack([c + b for c in column] + [c + 1 - b for c in column])
    return v[order]


def gather_column(x, n):
    lines = n // 2
    return [lax.ppermute(x, "seq", along_lines(lines, 2, k)) for k in range(1, lines)]


def gather_across(column, n):
    return [lax.ppermute(c, "seq", across_pairs(n // 2, 2)) for c in column]


def reduce_column(sums, n):
    lines = n // 2
    pieces = [lax.ppermute(sums[k], "seq", along_lines(lines, 2, lines - k)) for k in range(1, lines)]
    return [sums[0]] + pieces


def local(
    tokens, routes, route_weights, cotangent, attn_gain, query_gain, key_gain, ffn_gain,
    w_query, w_key, w_value, w_out, w_gate, w_up, w_down,
):
    n = lax.axis_size("seq")
    groups = lax.axis_size("fsdp")
    me = lax.axis_index("seq")
    width = tokens.shape[-1]
    own_tokens = tokens.reshape(-1, width)
    rows = own_tokens.shape[0]
    length = rows * n
    picks = routes.shape[-1]
    local_experts = w_gate.shape[1]
    experts = local_experts * n
    capacity = 3 * rows * picks // (2 * experts)
    head_dim = width // H
    heads = H // n
    span = heads * head_dim
    part = width // (n * groups)
    scale = head_dim ** (-0.5)
    bf, f32 = jnp.bfloat16, jnp.float32
    barrier = lax.optimization_barrier

    own_gains = jnp.stack([attn_gain, query_gain, key_gain, ffn_gain]).astype(f32)
    own_gains = jnp.pad(own_gains, ((0, 4), (0, 0)))
    full_out = lax.all_gather(w_out, "fsdp", axis=0, tiled=True)
    by_expert = lambda w: lax.all_gather(jnp.swapaxes(w, 0, 1), "fsdp", axis=1, tiled=True)
    full_gate = by_expert(w_gate)
    normed, proj, squares, w_heads, gains = project_rows(
        own_tokens, w_query, w_key, w_value, own_gains, n, groups, 8, 0
    )
    w_up, w_down, squares = barrier((w_up, w_down, squares))
    full_up, full_down = by_expert(w_up), by_expert(w_down)
    gain_attn, gain_ffn = gains[0], gains[3]
    head_gains = lax.dynamic_slice(gains, (1, me * span), (2, span))

    expert_ids = jnp.arange(experts, dtype=jnp.int32)
    named = routes.reshape(rows, picks)[None] == expert_ids[:, None, None]
    mixing = route_weights.reshape(rows, picks)[None]
    sent = jnp.sum(jnp.where(named, mixing, 0.0), axis=-1).reshape(n, local_experts, rows)
    tables = turn_parts(rows, n, head_dim)
    queries, keys, values, factors, weights = rotate_rows(
        squares, sent, proj, head_gains, tables, n, width, 1
    )
    block = min(512, length)
    heads_out, log_totals = attend(queries, keys, values, heads, block, scale)
    context = lax.all_to_all(heads_out, "seq", split_axis=0, concat_axis=1, tiled=True)
    inputs = own_tokens.astype(f32)
    mid = inputs + jnp.dot(context, full_out, preferred_element_type=f32)
    norm_two = inverse_norm(mid)
    ffn_in = (mid * norm_two * gain_ffn).astype(bf)

    ffn_all = gather_rows(ffn_in, n, 8, False, 2)
    cot_own, ffn_all = barrier((cotangent.reshape(rows, width), ffn_all))
    half = rows // 2
    cot_halves = [cot_own[:half], cot_own[half:]]
    cot_columns = [gather_column(v, n) for v in cot_halves]
    cot_others = [gather_across([v], n) for v in cot_halves]
    weights = by_place(weights, n)
    taken = weights > 0
    tri = (jnp.arange(rows)[:, None] <= jnp.arange(rows)[None, :]).astype(bf)
    rank = jnp.einsum("cet,tu->ceu", taken.astype(bf), tri, preferred_element_type=f32) - 1.0
    slot_ids = jnp.arange(capacity, dtype=f32)
    hit = (rank[:, :, None, :] == slot_ids[None, None, :, None]) & taken[:, :, None, :]
    place = hit.astype(bf)
    slot_weight = jnp.sum(jnp.where(hit, weights[:, :, None, :], 0.0), axis=-1)
    slot_weight = jnp.swapaxes(slot_weight, 0, 1)[..., None]
    place_rows = lambda v: jnp.einsum("cert,ctd->ecrd", place, v, preferred_element_type=f32)
    unplace = lambda v: jnp.einsum("cert,ecrd->ctd", place, v, preferred_element_type=f32).astype(bf)
    received = place_rows(ffn_all).astype(bf)
    gate = jnp.einsum("ecrd,edf->ecrf", received, full_gate, preferred_element_type=f32)
    received, gate, cot_columns[0] = barrier((received, gate, cot_columns[0]))
    cot_others[0] += gather_across(cot_columns[0], n)
    up_part = jnp.einsum("ecrd,edf->ecrf", received, full_up, preferred_element_type=f32)
    sigmoid_gate = jax.nn.sigmoid(gate)
    activated = gate * sigmoid_gate
    hidden = (activated * up_part).astype(bf)
    expert_out = jnp.einsum("ecrf,edf->ecrd", hidden, full_down, preferred_element_type=f32)
    expert_out = (expert_out * slot_weight).astype(bf)
    expert_out, cot_columns[1], cot_others[0] = barrier((expert_out, cot_columns[1], cot_others[0]))
    cot_others[1] += gather_across(cot_columns[1], n)
    ffn_part = unplace(expert_out)
    ffn_part, cot_others = barrier((ffn_part, cot_others))
    cot_all = jnp.stack(
        [jnp.concatenate(v) for v in zip(*(([h] + c + o) for h, c, o in zip(cot_halves, cot_columns, cot_others)))]
    )
    ffn_keep, ffn_got = ffn_part[: n // 2], gather_across([ffn_part[n // 2 :]], n)[0]

    out_grad = cotangent.reshape(rows, width).astype(f32)
    down_received = (place_rows(cot_all) * slot_weight).astype(bf)
    hidden_grad = jnp.einsum("ecrd,edf->ecrf", down_received, full_down, preferred_element_type=f32)
    slope = sigmoid_gate * (1.0 + gate * (1.0 - sigmoid_gate))
    gate_grad = (hidden_grad * up_part * slope).astype(bf)
    up_grad = (hidden_grad * activated).astype(bf)
    rows_grad = (
        jnp.einsum("ecrf,edf->ecrd", gate_grad, full_gate, preferred_element_type=f32)
        + jnp.einsum("ecrf,edf->ecrd", up_grad, full_up, preferred_element_type=f32)
    ).astype(bf)
    term = lambda a, b: jnp.einsum("ecrd,ecrf->edf", a, b, preferred_element_type=f32).astype(bf)
    scatter = lambda v: lax.psum_scatter(v, "fsdp", scatter_dimension=1, tiled=True)
    rows_grad, ffn_keep, ffn_got = barrier((rows_grad, ffn_keep, ffn_got))
    ffn_pieces = reduce_column((ffn_keep.astype(f32) + ffn_got.astype(f32)).astype(bf), n)
    rows_part, ffn_pieces, down_term, gate_term, up_term = barrier(
        (
            unplace(rows_grad),
            ffn_pieces,
            term(down_received, hidden),
            term(received, gate_grad),
            term(received, up_grad),
        )
    )
    scattered = [scatter(down_term), scatter(gate_term), scatter(up_term)]
    ffn_in_grad = reduce_rows(rows_part, n, 8, False, 4)
    mid_back, ffn_gain_term = norm_backward(mid, norm_two, gain_ffn, ffn_in_grad)
    mid_grad = out_grad + mid_back
    branch_grad = mid_grad.astype(bf)

    branch_all = gather_rows(branch_grad, n, 8, True, 5).reshape(length, width)
    out_rows = lax.dynamic_slice_in_dim(full_out, me * span, span, 0)
    heads_grad = jnp.einsum("te,de->td", branch_all, out_rows, preferred_element_type=f32).astype(bf)
    out_term = jnp.einsum("td,te->de", heads_out, branch_all, preferred_element_type=f32).astype(bf)
    query_back, key_back, value_back = attend_back(
        queries, keys, values, heads_grad, heads_out, log_totals, heads, block, scale
    )
    proj_grad, gain_terms = heads_back(
        query_back, key_back, value_back, proj, factors, head_gains, tables, n, width, 6
    )
    normed_part = jnp.einsum("te,de->td", proj_grad, w_heads, preferred_element_type=f32).astype(bf)
    head_term = jnp.einsum("td,te->de", normed, proj_grad, preferred_element_type=f32).astype(bf)
    head_term = head_term.reshape(n, groups, part, 3 * span).swapaxes(0, 1)
    normed_part, out_term, head_term = barrier((normed_part, out_term, head_term))
    block_out = mid + sum(piece.astype(f32) for piece in ffn_pieces)
    normed_grad = reduce_rows(normed_part.reshape(n, rows, width), n, 8, True, 7)
    out_term, head_term, (down_sum, gate_sum, up_sum), normed_grad = barrier(
        (out_term, head_term, scattered, normed_grad)
    )
    out_sum = lax.psum_scatter(out_term, "fsdp", scatter_dimension=0, tiled=True).astype(f32)
    gate_sum, up_sum, down_sum = widen(gate_sum), widen(up_sum), widen(down_sum)
    input_back, attn_gain_term = norm_backward(inputs, inverse_norm(inputs), gain_attn, normed_grad)
    tokens_grad = mid_grad + input_back
    head_term = lax.psum_scatter(head_term, "fsdp", scatter_dimension=0, tiled=True)
    head_term = head_term.reshape(n, part, 3, span)
    head_term = lax.all_to_all(head_term, "seq", split_axis=0, concat_axis=0, tiled=True)
    head_sums = [
        head_term[:, :, i].swapaxes(0, 1).reshape(part, width).astype(f32) for i in range(3)
    ]
    by_span = lambda v: v.reshape(n, 1, span)
    sent_gains = jnp.concatenate([by_span(attn_gain_term), by_span(ffn_gain_term)], axis=1)
    sent_gains = jnp.pad(sent_gains, ((0, 0), (0, 6), (0, 0)))
    gain_sums = sum_gains(sent_gains, gain_terms, n, groups, 8)
    gain_sums = lax.dynamic_slice_in_dim(gain_sums, lax.axis_index("fsdp") * part, part, 1)
    return (
        block_out.astype(bf).reshape(tokens.shape),
        tokens_grad.reshape(tokens.shape),
        gain_sums[0],
        gain_sums[2],
        gain_sums[3],
        gain_sums[1],
        head_sums[0],
        head_sums[1],
        head_sums[2],
        out_sum,
        gate_sum,
        up_sum,
        down_sum,
    )


def solution(mesh):
    rows3 = P("fsdp", "seq", None)
    both = P(("seq", "fsdp"))
    both2 = P(("seq", "fsdp"), None)
    placed = (rows3,) * 4 + (P("fsdp"),) * 4 + (P("fsdp", None),) * 4 + (rows3,) * 3
    return jax.shard_map(
        local,
        mesh=mesh,
        in_specs=placed,
        out_specs=(rows3,) * 2 + (both,) * 4 + (both2,) * 4 + (rows3,) * 3,
        check_vma=False,
    )
```

```python
import functools
import jax
import jax.numpy as jnp
from jax import lax
from jax.experimental import pallas as pl
from jax.experimental.pallas import tpu as pltpu
from jax.sharding import PartitionSpec as P


MESH = pl.DeviceIdType.MESH
ANY = pl.ANY
H = 16
epsilon = 1e-05


def work(us):
    return pl.CostEstimate(flops=int(us * 6e8), bytes_accessed=0, transcendentals=0)


def greet(peers):
    barrier = pltpu.get_barrier_semaphore()
    for peer in peers:
        pl.semaphore_signal(barrier, inc=1, device_id={"seq": peer}, device_id_type=MESH)
    pl.semaphore_wait(barrier, len(peers))


def push(src, dst, send, recv, peer):
    return pltpu.make_async_remote_copy(
        src_ref=src, dst_ref=dst, send_sem=send, recv_sem=recv,
        device_id={"seq": peer}, device_id_type=MESH)


def gather_kernel(n, pieces, by_index, own, out, send_sem, recv_sem, copy_sem):
    pair = 2
    lines = n // pair
    me = lax.axis_index("seq")
    a, b = me // pair, me % pair
    column = [((a + k) % lines) * pair + b for k in range(1, lines)]
    across = a * pair + (1 - b)
    greet(column + [across])
    rows = own.shape[0] // pieces
    if by_index:
        here = [((a + lines - k) % lines) * pair + b for k in range(lines)]
        there = [((a + lines - k) % lines) * pair + 1 - b for k in range(lines)]
        sent = [me] * lines
        relayed = here
    else:
        here, there = list(range(lines)), list(range(lines, n))
        sent = here
        relayed = there
    local = pltpu.make_async_copy(own, out.at[here[0]], copy_sem)
    local.start()

    def piece(p):
        return pl.ds(p * rows, rows)

    sends = []
    for p in range(pieces):
        for k in range(lines):
            peer = across if k == 0 else column[k - 1]
            place = relayed[0] if k == 0 else sent[k]
            copy = push(own.at[piece(p)], out.at[place, piece(p)], send_sem.at[k, p], recv_sem.at[k, p], peer)
            copy.start()
            sends.append(copy)
    relays = []
    for p in range(pieces):
        for k in range(1, lines):
            push(own.at[piece(p)], out.at[here[k], piece(p)], send_sem.at[k, p], recv_sem.at[k, p], across).wait_recv()
            slot = lines + k - 1
            copy = push(
                out.at[here[k], piece(p)], out.at[relayed[k], piece(p)], send_sem.at[slot, p], recv_sem.at[slot, p], across
            )
            copy.start()
            relays.append(copy)
    for p in range(pieces):
        push(own.at[piece(p)], out.at[there[0], piece(p)], send_sem.at[0, p], recv_sem.at[0, p], across).wait_recv()
    for copy in relays:
        copy.wait_recv()
    for copy in sends + relays:
        copy.wait_send()
    local.wait()


def gather_rows(x, n, pieces, by_index, collective_id):
    slots = n // 2 + n // 2 - 1
    return pl.pallas_call(
        functools.partial(gather_kernel, n, pieces, by_index),
        out_shape=jax.ShapeDtypeStruct((n,) + x.shape, x.dtype),
        in_specs=[pl.BlockSpec(memory_space=pltpu.VMEM)],
        out_specs=pl.BlockSpec(memory_space=ANY),
        scratch_shapes=[
            pltpu.SemaphoreType.DMA((slots, pieces)),
            pltpu.SemaphoreType.DMA((slots, pieces)),
            pltpu.SemaphoreType.DMA,
        ],
        compiler_params=pltpu.CompilerParams(collective_id=collective_id, has_side_effects=True),
        cost_estimate=work(105),
        name="gather_rows",
    )(x)


def reduce_kernel(n, pieces, by_index, part, out, mine, got, sums, landed, send_sem, recv_sem, load_sem):
    pair = 2
    lines = n // pair
    me = lax.axis_index("seq")
    a, b = me // pair, me % pair
    column = [((a + lines - k) % lines) * pair + b for k in range(1, lines)]
    across = a * pair + (1 - b)
    greet(column + [across])
    rows = out.shape[0] // pieces
    order = list(range(1, lines)) + [0]
    if by_index:
        here = [((a + lines - k) % lines) * pair + b for k in range(lines)]
        there = [((a + lines - k) % lines) * pair + 1 - b for k in range(lines)]
    else:
        here, there = list(range(lines)), list(range(lines, n))

    def piece(p):
        return pl.ds(p * rows, rows)

    firsts, loads = {}, {}
    for k in order:
        for p in range(pieces):
            copy = push(part.at[there[k], piece(p)], got.at[k, piece(p)],
                        send_sem.at[k, p], recv_sem.at[k, p], across)
            copy.start()
            firsts[k, p] = copy
            load = pltpu.make_async_copy(part.at[here[k], piece(p)], mine.at[k, piece(p)], load_sem.at[k, p])
            load.start()
            loads[k, p] = load
    seconds = {}
    for k in order:
        for p in range(pieces):
            firsts[k, p].wait_recv()
            loads[k, p].wait()
            total = mine[k, piece(p)].astype(jnp.float32) + got[k, piece(p)].astype(jnp.float32)
            if k:
                sums[k - 1, piece(p)] = total.astype(jnp.bfloat16)
                slot = lines + k - 1
                copy = push(sums.at[k - 1, piece(p)], landed.at[k - 1, piece(p)],
                            send_sem.at[slot, p], recv_sem.at[slot, p], column[k - 1])
                copy.start()
                seconds[k, p] = copy
            else:
                for j in range(1, lines):
                    seconds[j, p].wait_recv()
                    total += landed[j - 1, piece(p)].astype(jnp.float32)
                out[piece(p), :] = total
    for copy in list(firsts.values()) + list(seconds.values()):
        copy.wait_send()


def reduce_rows(part, n, pieces, by_index, collective_id):
    _, rows, width = part.shape
    lines = n // 2
    slots = lines + lines - 1
    return pl.pallas_call(
        functools.partial(reduce_kernel, n, pieces, by_index),
        out_shape=jax.ShapeDtypeStruct((rows, width), jnp.float32),
        in_specs=[pl.BlockSpec(memory_space=ANY)],
        out_specs=pl.BlockSpec(memory_space=pltpu.VMEM),
        scratch_shapes=[
            pltpu.VMEM((lines, rows, width), jnp.bfloat16),
            pltpu.VMEM((lines, rows, width), jnp.bfloat16),
            pltpu.VMEM((lines - 1, rows, width), jnp.bfloat16),
            pltpu.VMEM((lines - 1, rows, width), jnp.bfloat16),
            pltpu.SemaphoreType.DMA((slots, pieces)),
            pltpu.SemaphoreType.DMA((slots, pieces)),
            pltpu.SemaphoreType.DMA((lines, pieces)),
        ],
        compiler_params=pltpu.CompilerParams(collective_id=collective_id, has_side_effects=True),
        cost_estimate=work(98),
        name="reduce_rows",
    )(part)


def reduce_terms_kernel(
    n, pieces, tile, part, x, first, second, out, first_term, second_term,
    mine, got, sums, landed, x_buf, g_buf, o_buf, send_sem, recv_sem, load_sem, x_sem, g_sem, o_sem
):
    pair = 2
    lines = n // pair
    me = lax.axis_index("seq")
    a, b = me // pair, me % pair
    across = a * pair + (1 - b)
    greet([((a + lines - k) % lines) * pair + b for k in range(1, lines)] + [across])
    rows = out.shape[0] // pieces
    experts, _, width = x.shape
    tiles = width // tile
    jobs = experts * tiles
    terms = (first_term, second_term)

    def piece(p):
        return pl.ds(pl.multiple_of(p * rows, rows), rows)

    def first_copy(k, p):
        return push(part.at[lines + k, piece(p)], got.at[k, piece(p)], send_sem.at[k, p], recv_sem.at[k, p], across)

    def load(k, p):
        return pltpu.make_async_copy(part.at[k, piece(p)], mine.at[k, piece(p)], load_sem.at[k, p])

    def second_copy(k, p):
        peer = ((a + lines - k) % lines) * pair + b
        slot = lines + k - 1
        return push(sums.at[k - 1, piece(p)], landed.at[k - 1, piece(p)], send_sem.at[slot, p], recv_sem.at[slot, p], peer)

    def x_copy(j):
        cols = pl.ds(pl.multiple_of(j % tiles * tile, tile), tile)
        return pltpu.make_async_copy(x.at[j // tiles, :, cols], x_buf.at[j % 2], x_sem.at[j % 2])

    def g_copies(e):
        return [
            pltpu.make_async_copy(g.at[e], g_buf.at[e % 2, i], g_sem.at[e % 2, i]) for i, g in enumerate((first, second))
        ]

    def o_copies(j):
        place = pl.ds(pl.multiple_of(j % tiles * tile, tile), tile)
        return [
            pltpu.make_async_copy(o_buf.at[j % 2, i], o.at[j // tiles, place, :], o_sem.at[j % 2, i])
            for i, o in enumerate(terms)
        ]

    for k in list(range(1, lines)) + [0]:
        for p in range(pieces):
            first_copy(k, p).start()
            load(k, p).start()
    x_copy(0).start()
    for copy in g_copies(0):
        copy.start()

    def add(k, p):
        first_copy(k, p).wait_recv()
        load(k, p).wait()
        return mine[k, piece(p)].astype(jnp.float32) + got[k, piece(p)].astype(jnp.float32)

    def step(s):
        k, p = 1 + s // pieces, s % pieces
        sums[k - 1, piece(p)] = add(k, p).astype(jnp.bfloat16)
        second_copy(k, p).start()

    def job(j):
        @pl.when(j + 1 < jobs)
        def _():
            x_copy(j + 1).start()

        @pl.when(j % tiles == 0)
        def _():
            for copy in g_copies(j // tiles):
                copy.wait()

            @pl.when(j // tiles + 1 < experts)
            def _():
                for copy in g_copies(j // tiles + 1):
                    copy.start()

        @pl.when(j >= 2)
        def _():
            for copy in o_copies(j - 2):
                copy.wait()

        x_copy(j).wait()
        for i in range(2):
            o_buf[j % 2, i] = down_rows(x_buf[j % 2], g_buf[j // tiles % 2, i]).astype(jnp.bfloat16)
        for copy in o_copies(j):
            copy.start()

    steps = (lines - 1) * pieces
    per = steps * 2 // jobs

    def both(t, _):
        for i in range(per):
            step(t * per + i)
            if i == 0:
                job(2 * t)
            if i == per - 1:
                job(2 * t + 1)
        return 0

    lax.fori_loop(0, jobs // 2, both, 0)
    for copy in o_copies(jobs - 2) + o_copies(jobs - 1):
        copy.wait()

    def finish(p, _):
        total = add(0, p)
        for k in range(1, lines):
            second_copy(k, p).wait_recv()
            total += landed[k - 1, piece(p)].astype(jnp.float32)
        out[piece(p), :] = total
        return 0

    lax.fori_loop(0, pieces, finish, 0)
    for p in range(pieces):
        for k in range(lines):
            first_copy(k, p).wait_send()
        for k in range(1, lines):
            second_copy(k, p).wait_send()


def reduce_terms(part, x, first, second, n, pieces, tile, collective_id):
    _, rows, width = part.shape
    experts, tokens, _ = x.shape
    hidden = first.shape[2]
    lines = n // 2
    slots = lines + lines - 1
    hbm = pl.BlockSpec(memory_space=ANY)
    term = jax.ShapeDtypeStruct((experts, width, hidden), jnp.bfloat16)
    return pl.pallas_call(
        functools.partial(reduce_terms_kernel, n, pieces, tile),
        out_shape=(jax.ShapeDtypeStruct((rows, width), jnp.float32), term, term),
        in_specs=[hbm] * 4,
        out_specs=[pl.BlockSpec(memory_space=pltpu.VMEM), hbm, hbm],
        scratch_shapes=[
            pltpu.VMEM((lines, rows, width), jnp.bfloat16),
            pltpu.VMEM((lines, rows, width), jnp.bfloat16),
            pltpu.VMEM((lines - 1, rows, width), jnp.bfloat16),
            pltpu.VMEM((lines - 1, rows, width), jnp.bfloat16),
            pltpu.VMEM((2, tokens, tile), jnp.bfloat16),
            pltpu.VMEM((2, 2, tokens, hidden), jnp.bfloat16),
            pltpu.VMEM((2, 2, tile, hidden), jnp.bfloat16),
            pltpu.SemaphoreType.DMA((slots, pieces)),
            pltpu.SemaphoreType.DMA((slots, pieces)),
            pltpu.SemaphoreType.DMA((lines, pieces)),
            pltpu.SemaphoreType.DMA((2,)),
            pltpu.SemaphoreType.DMA((2, 2)),
            pltpu.SemaphoreType.DMA((2, 2)),
        ],
        compiler_params=pltpu.CompilerParams(
            collective_id=collective_id, has_side_effects=True, vmem_limit_bytes=50 << 20
        ),
        cost_estimate=work(105),
        name="reduce_terms",
    )(part, x, first, second)


def gains_kernel(n, groups, sent, own, out, taken, summed, landed, send_sem, recv_sem, side_send, side_recv):
    me, group = lax.axis_index("seq"), lax.axis_index("fsdp")
    barrier = pltpu.get_barrier_semaphore()
    peers = [(me + k) % n for k in range(1, n)]
    mates = [(group + k) % groups for k in range(1, groups)]
    for peer in peers:
        pl.semaphore_signal(barrier, inc=1, device_id={"seq": peer}, device_id_type=MESH)
    for mate in mates:
        pl.semaphore_signal(barrier, inc=1, device_id={"fsdp": mate}, device_id_type=MESH)
    pl.semaphore_wait(barrier, n - 1 + groups - 1)
    copies = []
    for k in range(1, n):
        copy = push(sent.at[peers[k - 1]], taken.at[k - 1], send_sem.at[k - 1], recv_sem.at[k - 1], peers[k - 1])
        copy.start()
        copies.append(copy)
    total = sent[me] + own[...]
    for k in range(1, n):
        copies[k - 1].wait_recv()
        total = total + taken[k - 1]
    summed[...] = total
    sides = []
    for k in range(1, groups):
        side = pltpu.make_async_remote_copy(
            src_ref=summed, dst_ref=landed.at[k - 1], send_sem=side_send.at[k - 1], recv_sem=side_recv.at[k - 1],
            device_id={"fsdp": mates[k - 1]}, device_id_type=MESH)
        side.start()
        sides.append(side)
    for k in range(1, groups):
        sides[k - 1].wait_recv()
        total = total + landed[k - 1]
    out[...] = total
    for copy in copies + sides:
        copy.wait_send()


def sum_gains(sent, own, n, groups, collective_id):
    shape = own.shape
    return pl.pallas_call(
        functools.partial(gains_kernel, n, groups),
        out_shape=jax.ShapeDtypeStruct(shape, own.dtype),
        in_specs=[pl.BlockSpec(memory_space=pltpu.VMEM)] * 2,
        out_specs=pl.BlockSpec(memory_space=pltpu.VMEM),
        scratch_shapes=[
            pltpu.VMEM((n - 1,) + shape, own.dtype),
            pltpu.VMEM(shape, own.dtype),
            pltpu.VMEM((groups - 1,) + shape, own.dtype),
            pltpu.SemaphoreType.DMA((n - 1,)),
            pltpu.SemaphoreType.DMA((n - 1,)),
            pltpu.SemaphoreType.DMA((groups - 1,)),
            pltpu.SemaphoreType.DMA((groups - 1,)),
        ],
        compiler_params=pltpu.CompilerParams(collective_id=collective_id, has_side_effects=True),
        cost_estimate=work(10),
        name="sum_gains",
    )(sent, own)


def widen_kernel(x_ref, o_ref):
    for e in range(x_ref.shape[0]):
        o_ref[:, e, :] = x_ref[e].astype(jnp.float32)


def widen(x):
    experts, rows, columns = x.shape
    step = min(128, rows)
    return pl.pallas_call(
        widen_kernel,
        grid=(rows // step,),
        out_shape=jax.ShapeDtypeStruct((rows, experts, columns), jnp.float32),
        in_specs=[pl.BlockSpec((experts, step, columns), lambda i: (0, i, 0))],
        out_specs=pl.BlockSpec((step, experts, columns), lambda i: (i, 0, 0)),
        cost_estimate=work(5),
        name="widen",
    )(x)


def masked(block):
    keys = lax.broadcasted_iota(jnp.int32, (block, block), 0)
    rows = lax.broadcasted_iota(jnp.int32, (block, block), 1)
    return keys <= rows


def across_lanes(a, b):
    return lax.dot_general(a, b, (((1,), (1,)), ((), ())), preferred_element_type=jnp.float32)


def down_rows(a, b):
    return lax.dot_general(a, b, (((0,), (0,)), ((), ())), preferred_element_type=jnp.float32)


LOG2E = 1.4426950408889634


def attend_kernel(block, scale, q_ref, k_ref, v_ref, o_ref, lse_ref, s_ref, acc_ref):
    length, _ = q_ref.shape

    def rows(i):
        return pl.ds(pl.multiple_of(i * block, block), block)

    def one_block(i, _):
        q = q_ref[rows(i), :]
        diag = across_lanes(k_ref[rows(i), :], q) * (scale * LOG2E)
        diag = jnp.where(masked(block), diag, -1e30)
        s_ref[rows(i), :] = diag
        peak = jnp.max(diag, axis=0, keepdims=True)

        def score(j, peak):
            s = across_lanes(k_ref[rows(j), :], q) * (scale * LOG2E)
            s_ref[rows(j), :] = s
            return jnp.maximum(peak, jnp.max(s, axis=0, keepdims=True))

        peak = lax.fori_loop(0, i, score, peak)
        acc_ref[...] = jnp.zeros_like(acc_ref)

        def weigh(j, total):
            p = jnp.exp2(s_ref[rows(j), :] - peak)
            acc_ref[...] += down_rows(v_ref[rows(j), :], p.astype(jnp.bfloat16))
            return total + jnp.sum(p, axis=0, keepdims=True)

        total = lax.fori_loop(0, i + 1, weigh, jnp.zeros_like(peak))
        o_ref[rows(i), :] = (acc_ref[...] / total).T.astype(o_ref.dtype)
        lse_ref[0, :, rows(i)] = peak + jnp.log2(total)
        return 0

    lax.fori_loop(0, length // block, one_block, 0)


def attend(q, k, v, heads, block, scale):
    length, width = q.shape
    dim = width // heads
    spec = pl.BlockSpec((length, dim), lambda h: (0, h))
    return pl.pallas_call(
        functools.partial(attend_kernel, block, scale),
        grid=(heads,),
        out_shape=(
            jax.ShapeDtypeStruct(q.shape, q.dtype),
            jax.ShapeDtypeStruct((heads, 1, length), jnp.float32),
        ),
        in_specs=[spec] * 3,
        out_specs=[spec, pl.BlockSpec((1, 1, length), lambda h: (h, 0, 0))],
        scratch_shapes=[
            pltpu.VMEM((length, block), jnp.float32),
            pltpu.VMEM((dim, block), jnp.float32),
        ],
        cost_estimate=work(25),
        name="attend",
    )(q, k, v)


def attend_back_kernel(
    block, scale, q_ref, k_ref, v_ref, g_ref, o_ref, lse_ref, dq_ref, dk_ref, dv_ref, dk_acc, dv_acc, dq_acc
):
    length, dim = q_ref.shape
    dk_acc[...] = jnp.zeros_like(dk_acc)
    dv_acc[...] = jnp.zeros_like(dv_acc)

    def rows(i):
        return pl.ds(pl.multiple_of(i * block, block), block)

    def one_block(i, _):
        q, g = q_ref[rows(i), :], g_ref[rows(i), :]
        lse = lse_ref[0, :, rows(i)]
        products = g.astype(jnp.float32) * o_ref[rows(i), :].astype(jnp.float32)
        shift = lax.dot_general(
            jnp.ones((8, dim), jnp.float32), products, (((1,), (1,)), ((), ())),
            precision=lax.Precision.HIGHEST, preferred_element_type=jnp.float32,
        )[:1]

        def pair(j, keep):
            k, v = k_ref[rows(j), :], v_ref[rows(j), :]
            p = jnp.exp2(across_lanes(k, q) * (scale * LOG2E) - lse)
            if keep is not None:
                p = jnp.where(keep, p, 0.0)
            ds = (p * (across_lanes(v, g) - shift) * scale).astype(jnp.bfloat16)
            dv_acc[rows(j), :] += jnp.dot(p.astype(jnp.bfloat16), g, preferred_element_type=jnp.float32)
            dk_acc[rows(j), :] += jnp.dot(ds, q, preferred_element_type=jnp.float32)
            dq_acc[...] += down_rows(k, ds)

        dq_acc[...] = jnp.zeros_like(dq_acc)
        pair(i, masked(block))

        def body(j, _):
            pair(j, None)
            return 0

        lax.fori_loop(0, i, body, 0)
        dq_ref[rows(i), :] = dq_acc[...].T.astype(dq_ref.dtype)
        return 0

    lax.fori_loop(0, length // block, one_block, 0)
    dk_ref[...] = dk_acc[...].astype(dk_ref.dtype)
    dv_ref[...] = dv_acc[...].astype(dv_ref.dtype)


def attend_back(q, k, v, g, o, lse, heads, block, scale):
    length, width = q.shape
    dim = width // heads
    spec = pl.BlockSpec((length, dim), lambda h: (0, h))
    return pl.pallas_call(
        functools.partial(attend_back_kernel, block, scale),
        grid=(heads,),
        out_shape=(jax.ShapeDtypeStruct(q.shape, q.dtype),) * 3,
        in_specs=[spec] * 5 + [pl.BlockSpec((1, 1, length), lambda h: (h, 0, 0))],
        out_specs=[spec] * 3,
        scratch_shapes=[
            pltpu.VMEM((length, dim), jnp.float32),
            pltpu.VMEM((length, dim), jnp.float32),
            pltpu.VMEM((dim, block), jnp.float32),
        ],
        cost_estimate=work(60),
        name="attend_back",
    )(q, k, v, g, o, lse)


def project_kernel(
    n, groups, pieces, own, w_query, w_key, w_value, gain_own,
    normed, proj, squares, w_ref, gains, held, send_sem, recv_sem, side_send, side_recv, copy_sem
):
    pair = 2
    lines = n // pair
    me, group = lax.axis_index("seq"), lax.axis_index("fsdp")
    a, b = me // pair, me % pair
    column = [((a + k) % lines) * pair + b for k in range(1, lines)]
    back = [((a + lines - k) % lines) * pair + b for k in range(1, lines)]
    across = a * pair + (1 - b)
    mates = [(group + k) % groups for k in range(1, groups)]
    barrier = pltpu.get_barrier_semaphore()
    for peer in column + [across]:
        pl.semaphore_signal(barrier, inc=1, device_id={"seq": peer}, device_id_type=MESH)
    for mate in mates:
        pl.semaphore_signal(barrier, inc=1, device_id={"fsdp": mate}, device_id_type=MESH)
    pl.semaphore_wait(barrier, lines + groups - 1)
    rows, _ = own.shape
    step = rows // pieces
    span = w_ref.shape[1] // 3
    shard = w_query.shape[0]

    def piece(p):
        return pl.ds(p * step, step)

    sends = []
    for p in range(pieces):
        for k in range(lines):
            peer = across if k == 0 else column[k - 1]
            copy = push(own.at[piece(p)], held.at[me, piece(p)], send_sem.at[k, p], recv_sem.at[k, p], peer)
            copy.start()
            sends.append(copy)

    shard_rows = pl.ds(pl.multiple_of(group * shard, shard), shard)
    mine = pl.ds(pl.multiple_of(me * span, span), span)
    blocks = [
        (w.at[:, mine], w_ref.at[shard_rows, part * span : (part + 1) * span])
        for part, w in enumerate((w_query, w_key, w_value))
    ]
    blocks.append((gain_own, gains.at[:, shard_rows]))
    locals_, sides = [], []
    for i, (src, dst) in enumerate(blocks):
        for k in range(1, groups):
            side = pltpu.make_async_remote_copy(
                src_ref=src, dst_ref=dst, send_sem=side_send.at[i, k - 1], recv_sem=side_recv.at[i, k - 1],
                device_id={"fsdp": mates[k - 1]}, device_id_type=MESH)
            side.start()
            sides.append(side)
        local = pltpu.make_async_copy(src, dst, copy_sem.at[i])
        local.start()
        locals_.append(local)

    def project(src, chunk):
        x = chunk[...].astype(jnp.float32)
        factor = lax.rsqrt(jnp.mean(x * x, axis=-1, keepdims=True) + epsilon)
        place = pl.ds(pl.multiple_of(src * rows, rows), rows)
        normed[place, :] = (x * factor * gains[0:1, :]).astype(jnp.bfloat16)
        for part in range(3):
            cols = slice(part * span, (part + 1) * span)
            out = jnp.dot(normed[place, :], w_ref[:, cols], preferred_element_type=jnp.float32)
            proj[place, cols] = out
            if part < 2:
                sums = lax.dot_general(
                    jnp.ones((8, span), jnp.float32), out * out, (((1,), (1,)), ((), ())),
                    precision=lax.Precision.HIGHEST, preferred_element_type=jnp.float32,
                )
                squares[pl.ds(part * n + src, 1), :] = sums[:1]

    relays = []
    for p in range(pieces):
        for k in range(1, lines):
            src = back[k - 1]
            push(own.at[piece(p)], held.at[src, piece(p)], send_sem.at[k, p], recv_sem.at[k, p], across).wait_recv()
            slot = lines + k - 1
            copy = push(held.at[src, piece(p)], held.at[src, piece(p)], send_sem.at[slot, p], recv_sem.at[slot, p], across)
            copy.start()
            relays.append(copy)
    for copy in locals_:
        copy.wait()
    for side in sides:
        side.wait_recv()
    project(me, own)
    for p in range(pieces):
        push(own.at[piece(p)], held.at[across, piece(p)], send_sem.at[0, p], recv_sem.at[0, p], across).wait_recv()
    project(across, held.at[across])
    for k in range(1, lines):
        project(back[k - 1], held.at[back[k - 1]])
    for k in range(1, lines):
        for p in range(pieces):
            relays[p * (lines - 1) + k - 1].wait_recv()
        src = ((a + lines - k) % lines) * pair + 1 - b
        project(src, held.at[src])
    for copy in sends + relays + sides:
        copy.wait_send()


def project_rows(x, w_query, w_key, w_value, gains, n, groups, pieces, collective_id):
    rows, width = x.shape
    span = w_query.shape[1] // n
    slots = n // 2 + n // 2 - 1
    vmem = pl.BlockSpec(memory_space=pltpu.VMEM)
    hbm = pl.BlockSpec(memory_space=ANY)
    return pl.pallas_call(
        functools.partial(project_kernel, n, groups, pieces),
        out_shape=(
            jax.ShapeDtypeStruct((n * rows, width), jnp.bfloat16),
            jax.ShapeDtypeStruct((n * rows, 3 * span), jnp.float32),
            jax.ShapeDtypeStruct((2 * n, rows), jnp.float32),
            jax.ShapeDtypeStruct((width, 3 * span), jnp.bfloat16),
            jax.ShapeDtypeStruct((8, width), jnp.float32),
        ),
        in_specs=[vmem, hbm, hbm, hbm, vmem],
        out_specs=[vmem] * 5,
        scratch_shapes=[
            pltpu.VMEM((n, rows, width), jnp.bfloat16),
            pltpu.SemaphoreType.DMA((slots, pieces)),
            pltpu.SemaphoreType.DMA((slots, pieces)),
            pltpu.SemaphoreType.DMA((4, groups - 1)),
            pltpu.SemaphoreType.DMA((4, groups - 1)),
            pltpu.SemaphoreType.DMA((4,)),
        ],
        compiler_params=pltpu.CompilerParams(
            collective_id=collective_id, has_side_effects=True, vmem_limit_bytes=50 << 20
        ),
        cost_estimate=work(110),
        name="project_rows",
    )(x, w_query, w_key, w_value, gains)


def as_columns(row, lanes):
    return jnp.broadcast_to(row, (lanes, row.shape[1])).T


def turn_tables(c, near_cos, near_sin, far_cos, far_sin):
    far_c, far_s = far_cos[pl.ds(c, 1), :], far_sin[pl.ds(c, 1), :]
    cosine = near_cos[...] * far_c - near_sin[...] * far_s
    sine = near_sin[...] * far_c + near_cos[...] * far_s
    first = lax.broadcasted_iota(jnp.int32, sine.shape, 1) < sine.shape[1] // 2
    return cosine, jnp.where(first, -sine, sine)


def add_over_seq(n, own, landed, send_sem, recv_sem, peers):
    copies = []
    for k in range(1, n):
        copy = push(own, landed.at[k - 1], send_sem.at[k - 1], recv_sem.at[k - 1], peers[k - 1])
        copy.start()
        copies.append(copy)
    return copies


def rotate_kernel(
    n, full, squares, sent, proj, gains, near_cos, near_sin, far_cos, far_sin,
    queries, keys, values, factors, taken, landed, send_sem, recv_sem, copy_sem
):
    me = lax.axis_index("seq")
    peers = [(me + k) % n for k in range(1, n)]
    greet(peers)
    local = pltpu.make_async_copy(sent.at[me], taken.at[me], copy_sem)
    local.start()
    copies = add_over_seq(n, squares, landed, send_sem.at[0], recv_sem.at[0], peers)
    swaps = []
    for k in range(1, n):
        swap = push(sent.at[peers[k - 1]], taken.at[me], send_sem.at[1, k - 1], recv_sem.at[1, k - 1], peers[k - 1])
        swap.start()
        swaps.append(swap)
    span = queries.shape[1]
    rows = squares.shape[1]
    lanes = near_cos.shape[1]
    total = squares[...]
    for k in range(1, n):
        copies[k - 1].wait_recv()
        total = total + landed[k - 1]
    factors[...] = lax.rsqrt(total / full + epsilon)

    def chunk(c, _):
        place = pl.ds(pl.multiple_of(c * rows, rows), rows)
        cosine, sine = turn_tables(c, near_cos, near_sin, far_cos, far_sin)
        for part, out in ((0, queries), (1, keys)):
            factor = as_columns(factors[pl.ds(part * n + c, 1), :], lanes)
            for h in range(span // lanes):
                cols = slice(part * span + h * lanes, part * span + (h + 1) * lanes)
                x = proj[place, cols] * factor * gains[part : part + 1, h * lanes : (h + 1) * lanes]
                turned = x * cosine + pltpu.roll(x, lanes // 2, 1) * sine
                out[place, h * lanes : (h + 1) * lanes] = turned.astype(jnp.bfloat16)
        values[place, :] = proj[place, 2 * span :].astype(jnp.bfloat16)
        return 0

    lax.fori_loop(0, n, chunk, 0)
    for copy in copies:
        copy.wait_send()
    for swap in swaps:
        swap.wait()
    local.wait()


def rotate_rows(squares, sent, proj, gains, tables, n, full, collective_id):
    length, outs = proj.shape
    span = outs // 3
    vmem = pl.BlockSpec(memory_space=pltpu.VMEM)
    heads = jax.ShapeDtypeStruct((length, span), jnp.bfloat16)
    return pl.pallas_call(
        functools.partial(rotate_kernel, n, full),
        out_shape=(
            heads, heads, heads,
            jax.ShapeDtypeStruct(squares.shape, jnp.float32),
            jax.ShapeDtypeStruct(sent.shape, sent.dtype),
        ),
        in_specs=[vmem] * 8,
        out_specs=[vmem] * 5,
        scratch_shapes=[
            pltpu.VMEM((n - 1,) + squares.shape, jnp.float32),
            pltpu.SemaphoreType.DMA((2, n - 1)),
            pltpu.SemaphoreType.DMA((2, n - 1)),
            pltpu.SemaphoreType.DMA,
        ],
        compiler_params=pltpu.CompilerParams(
            collective_id=collective_id, has_side_effects=True, vmem_limit_bytes=40 << 20
        ),
        cost_estimate=work(15),
        name="rotate_rows",
    )(squares, sent, proj, gains, *tables)


def heads_back_kernel(
    n, full, dq, dk, dv, proj, factors, gains, near_cos, near_sin, far_cos, far_sin,
    grads, gain_grads, sums, landed, send_sem, recv_sem
):
    me = lax.axis_index("seq")
    peers = [(me + k) % n for k in range(1, n)]
    greet(peers)
    span = dq.shape[1]
    rows = sums.shape[1]
    lanes = near_cos.shape[1]
    count = span // lanes

    def parts(c, part, h, grad):
        place = pl.ds(pl.multiple_of(c * rows, rows), rows)
        cosine, sine = turn_tables(c, near_cos, near_sin, far_cos, far_sin)
        g = grad[place, h * lanes : (h + 1) * lanes].astype(jnp.float32)
        up = g * cosine + pltpu.roll(g * sine, lanes // 2, 1)
        factor = as_columns(factors[pl.ds(part * n + c, 1), :], lanes)
        cols = slice(part * span + h * lanes, part * span + (h + 1) * lanes)
        normal = proj[place, cols] * factor
        weighted = up * gains[part : part + 1, h * lanes : (h + 1) * lanes]
        return place, cols, up, factor, normal, weighted

    def first(c, _):
        for part, grad in ((0, dq), (1, dk)):
            products = 0.0
            for h in range(count):
                _, _, _, _, normal, weighted = parts(c, part, h, grad)
                products = products + weighted * normal
            total = lax.dot_general(
                jnp.ones((8, lanes), jnp.float32), products, (((1,), (1,)), ((), ())),
                precision=lax.Precision.HIGHEST, preferred_element_type=jnp.float32,
            )
            sums[pl.ds(part * n + c, 1), :] = total[:1]
        return 0

    lax.fori_loop(0, n, first, 0)
    copies = add_over_seq(n, sums, landed, send_sem, recv_sem, peers)
    gain_grads[...] = jnp.zeros_like(gain_grads)

    def gain_sum(c, _):
        for part, grad in ((0, dq), (1, dk)):
            for h in range(count):
                _, _, up, _, normal, _ = parts(c, part, h, grad)
                cell = (slice(part + 2, part + 3), slice(h * lanes, (h + 1) * lanes))
                gain_grads[cell] += jnp.sum(up * normal, axis=0, keepdims=True)
        place = pl.ds(pl.multiple_of(c * rows, rows), rows)
        grads[place, 2 * span :] = dv[place, :]
        return 0

    lax.fori_loop(0, n, gain_sum, 0)
    total = sums[...]
    for k in range(1, n):
        copies[k - 1].wait_recv()
        total = total + landed[k - 1]
    landed[0] = total / full

    def last(c, _):
        for part, grad in ((0, dq), (1, dk)):
            mean = as_columns(landed[0, pl.ds(part * n + c, 1), :], lanes)
            for h in range(count):
                place, cols, _, factor, normal, weighted = parts(c, part, h, grad)
                grads[place, cols] = (factor * (weighted - normal * mean)).astype(jnp.bfloat16)
        return 0

    lax.fori_loop(0, n, last, 0)
    for copy in copies:
        copy.wait_send()


def heads_back(dq, dk, dv, proj, factors, gains, tables, n, full, collective_id):
    length, span = dq.shape
    vmem = pl.BlockSpec(memory_space=pltpu.VMEM)
    return pl.pallas_call(
        functools.partial(heads_back_kernel, n, full),
        out_shape=(
            jax.ShapeDtypeStruct((length, 3 * span), jnp.bfloat16),
            jax.ShapeDtypeStruct((8, span), jnp.float32),
        ),
        in_specs=[vmem] * 10,
        out_specs=[vmem] * 2,
        scratch_shapes=[
            pltpu.VMEM(factors.shape, jnp.float32),
            pltpu.VMEM((n - 1,) + factors.shape, jnp.float32),
            pltpu.SemaphoreType.DMA((n - 1,)),
            pltpu.SemaphoreType.DMA((n - 1,)),
        ],
        compiler_params=pltpu.CompilerParams(
            collective_id=collective_id, has_side_effects=True, vmem_limit_bytes=40 << 20
        ),
        cost_estimate=work(20),
        name="heads_back",
    )(dq, dk, dv, proj, factors, gains, *tables)


def turn_parts(rows, n, dim):
    half = dim // 2
    frequency = jnp.power(10000.0, -2.0 * jnp.arange(half, dtype=jnp.float32) / dim)
    frequency = jnp.concatenate([frequency, frequency])[None]
    near = jnp.arange(rows, dtype=jnp.float32)[:, None] * frequency
    far = (rows * jnp.arange(n)).astype(jnp.float32)[:, None] * frequency
    return jnp.cos(near), jnp.sin(near), jnp.cos(far), jnp.sin(far)


def inverse_norm(values):
    return lax.rsqrt(jnp.mean(values * values, axis=-1, keepdims=True) + epsilon)


def norm_backward(values, factor, gain, upstream):
    normal = values * factor
    weighted = upstream * gain
    gain_term = jnp.sum(upstream * normal, axis=0)
    back = factor * (weighted - normal * jnp.mean(weighted * normal, axis=-1, keepdims=True))
    return (back, gain_term)


def across_pairs(lines, pair):
    return [(a * pair + b, a * pair + 1 - b) for a in range(lines) for b in range(pair)]


def along_lines(lines, pair, k):
    return [(a * pair + b, (a + k) % lines * pair + b) for a in range(lines) for b in range(pair)]


def by_place(v, n):
    lines = n // 2
    me = lax.axis_index("seq")
    a, b = me // 2, me % 2
    column = [((a + lines - k) % lines) * 2 for k in range(lines)]
    order = jnp.stack([c + b for c in column] + [c + 1 - b for c in column])
    return v[order]


def gather_column(x, n):
    lines = n // 2
    return [lax.ppermute(x, "seq", along_lines(lines, 2, k)) for k in range(1, lines)]


def gather_across(column, n):
    return [lax.ppermute(c, "seq", across_pairs(n // 2, 2)) for c in column]


def reduce_column(v, k, n):
    return lax.ppermute(v, "seq", along_lines(n // 2, 2, n // 2 - k))


def local(
    tokens, routes, route_weights, cotangent, attn_gain, query_gain, key_gain, ffn_gain,
    w_query, w_key, w_value, w_out, w_gate, w_up, w_down,
):
    n = lax.axis_size("seq")
    groups = lax.axis_size("fsdp")
    me = lax.axis_index("seq")
    width = tokens.shape[-1]
    own_tokens = tokens.reshape(-1, width)
    rows = own_tokens.shape[0]
    length = rows * n
    picks = routes.shape[-1]
    local_experts = w_gate.shape[1]
    experts = local_experts * n
    capacity = 3 * rows * picks // (2 * experts)
    head_dim = width // H
    heads = H // n
    span = heads * head_dim
    part = width // (n * groups)
    scale = head_dim ** (-0.5)
    bf, f32 = jnp.bfloat16, jnp.float32
    barrier = lax.optimization_barrier

    own_gains = jnp.stack([attn_gain, query_gain, key_gain, ffn_gain]).astype(f32)
    own_gains = jnp.pad(own_gains, ((0, 4), (0, 0)))
    full_out = lax.all_gather(w_out, "fsdp", axis=0, tiled=True)
    by_expert = lambda w: lax.all_gather(jnp.swapaxes(w, 0, 1), "fsdp", axis=1, tiled=True)
    full_gate = by_expert(w_gate)
    normed, proj, squares, w_heads, gains = project_rows(
        own_tokens, w_query, w_key, w_value, own_gains, n, groups, 8, 0
    )
    w_up, w_down, squares = barrier((w_up, w_down, squares))
    full_up, full_down = by_expert(w_up), by_expert(w_down)
    gain_attn, gain_ffn = gains[0], gains[3]
    head_gains = lax.dynamic_slice(gains, (1, me * span), (2, span))

    expert_ids = jnp.arange(experts, dtype=jnp.int32)
    named = routes.reshape(rows, picks)[None] == expert_ids[:, None, None]
    mixing = route_weights.reshape(rows, picks)[None]
    sent = jnp.sum(jnp.where(named, mixing, 0.0), axis=-1).reshape(n, local_experts, rows)
    tables = turn_parts(rows, n, head_dim)
    queries, keys, values, factors, weights = rotate_rows(
        squares, sent, proj, head_gains, tables, n, width, 1
    )
    block = min(512, length)
    heads_out, log_totals = attend(queries, keys, values, heads, block, scale)
    context = lax.all_to_all(heads_out, "seq", split_axis=0, concat_axis=1, tiled=True)
    inputs = own_tokens.astype(f32)
    mid = inputs + jnp.dot(context, full_out, preferred_element_type=f32)
    norm_two = inverse_norm(mid)
    ffn_in = (mid * norm_two * gain_ffn).astype(bf)

    ffn_all = gather_rows(ffn_in, n, 8, False, 2)
    cot_own, ffn_all = barrier((cotangent.reshape(rows, width), ffn_all))
    half = rows // 2
    cot_halves = [cot_own[:half], cot_own[half:]]
    cot_columns = [gather_column(v, n) for v in cot_halves]
    cot_others = [gather_across([v], n) for v in cot_halves]
    weights = by_place(weights, n)
    taken = weights > 0
    tri = (jnp.arange(rows)[:, None] <= jnp.arange(rows)[None, :]).astype(bf)
    rank = jnp.einsum("cet,tu->ceu", taken.astype(bf), tri, preferred_element_type=f32) - 1.0
    slot_ids = jnp.arange(capacity, dtype=f32)
    hit = (rank[:, :, None, :] == slot_ids[None, None, :, None]) & taken[:, :, None, :]
    place = hit.astype(bf)
    slot_weight = jnp.sum(jnp.where(hit, weights[:, :, None, :], 0.0), axis=-1)
    slot_weight = jnp.swapaxes(slot_weight, 0, 1)[..., None]
    place_rows = lambda v: jnp.einsum("cert,ctd->ecrd", place, v, preferred_element_type=f32)
    unplace = lambda v: jnp.einsum("cert,ecrd->ctd", place, v, preferred_element_type=f32).astype(bf)
    received = place_rows(ffn_all).astype(bf)
    gate = jnp.einsum("ecrd,edf->ecrf", received, full_gate, preferred_element_type=f32)
    received, gate, cot_columns[0] = barrier((received, gate, cot_columns[0]))
    cot_others[0] += gather_across(cot_columns[0], n)
    up_part = jnp.einsum("ecrd,edf->ecrf", received, full_up, preferred_element_type=f32)
    sigmoid_gate = jax.nn.sigmoid(gate)
    activated = gate * sigmoid_gate
    hidden = (activated * up_part).astype(bf)
    expert_out = jnp.einsum("ecrf,edf->ecrd", hidden, full_down, preferred_element_type=f32)
    expert_out = (expert_out * slot_weight).astype(bf)
    expert_out, cot_columns[1], cot_others[0] = barrier((expert_out, cot_columns[1], cot_others[0]))
    cot_others[1] += gather_across(cot_columns[1], n)
    ffn_part = unplace(expert_out)
    ffn_part, cot_others = barrier((ffn_part, cot_others))
    cot_all = jnp.stack(
        [jnp.concatenate(v) for v in zip(*(([h] + c + o) for h, c, o in zip(cot_halves, cot_columns, cot_others)))]
    )
    lines = n // 2
    ffn_got = {k: gather_across([ffn_part[lines + k]], n)[0] for k in list(range(1, lines)) + [0]}
    ffn_sum = lambda k: (ffn_part[k].astype(f32) + ffn_got[k].astype(f32)).astype(bf)

    out_grad = cotangent.reshape(rows, width).astype(f32)
    down_received = (place_rows(cot_all) * slot_weight).astype(bf)
    hidden_grad = jnp.einsum("ecrd,edf->ecrf", down_received, full_down, preferred_element_type=f32)
    slope = sigmoid_gate * (1.0 + gate * (1.0 - sigmoid_gate))
    gate_grad = (hidden_grad * up_part * slope).astype(bf)
    up_grad = (hidden_grad * activated).astype(bf)
    early = list(range(1, lines - 1))
    gate_grad, up_grad, got = barrier((gate_grad, up_grad, [ffn_got[k] for k in early]))
    ffn_got.update(zip(early, got))
    ffn_pieces = [reduce_column(ffn_sum(k), k, n) for k in early]
    rows_gate = jnp.einsum("ecrf,edf->ecrd", gate_grad, full_gate, preferred_element_type=f32)
    rows_gate, ffn_got[lines - 1] = barrier((rows_gate, ffn_got[lines - 1]))
    ffn_pieces.append(reduce_column(ffn_sum(lines - 1), lines - 1, n))
    rows_up = jnp.einsum("ecrf,edf->ecrd", up_grad, full_up, preferred_element_type=f32)
    rows_part = unplace((rows_gate + rows_up).astype(bf))
    rows_part, down_received, hidden = barrier((rows_part, down_received, hidden))
    down_term = jnp.einsum("ecrd,ecrf->edf", down_received, hidden, preferred_element_type=f32)
    scatter = lambda v: lax.psum_scatter(v, "fsdp", scatter_dimension=1, tiled=True)
    rows_part, ffn_pieces, ffn_got[0], down_term = barrier(
        (rows_part, ffn_pieces, ffn_got[0], down_term.astype(bf))
    )
    by_slot = lambda v: v.reshape(local_experts, n * capacity, v.shape[-1])
    ffn_in_grad, gate_term, up_term = reduce_terms(
        rows_part, by_slot(received), by_slot(gate_grad), by_slot(up_grad), n, 8, 512, 4
    )
    scattered = [scatter(down_term)]
    scattered += [scatter(gate_term), scatter(up_term)]
    mid_back, ffn_gain_term = norm_backward(mid, norm_two, gain_ffn, ffn_in_grad)
    mid_grad = out_grad + mid_back
    branch_grad = mid_grad.astype(bf)

    branch_all = gather_rows(branch_grad, n, 8, True, 5).reshape(length, width)
    out_rows = lax.dynamic_slice_in_dim(full_out, me * span, span, 0)
    heads_grad = jnp.einsum("te,de->td", branch_all, out_rows, preferred_element_type=f32).astype(bf)
    out_term = jnp.einsum("td,te->de", heads_out, branch_all, preferred_element_type=f32).astype(bf)
    query_back, key_back, value_back = attend_back(
        queries, keys, values, heads_grad, heads_out, log_totals, heads, block, scale
    )
    proj_grad, gain_terms = heads_back(
        query_back, key_back, value_back, proj, factors, head_gains, tables, n, width, 6
    )
    normed_part = jnp.einsum("te,de->td", proj_grad, w_heads, preferred_element_type=f32).astype(bf)
    head_term = jnp.einsum("td,te->de", normed, proj_grad, preferred_element_type=f32).astype(bf)
    head_term = head_term.reshape(n, groups, part, 3 * span).swapaxes(0, 1)
    normed_part, out_term, head_term = barrier((normed_part, out_term, head_term))
    block_out = mid + sum(piece.astype(f32) for piece in [ffn_part[0], ffn_got[0]] + ffn_pieces)
    normed_grad = reduce_rows(normed_part.reshape(n, rows, width), n, 8, True, 7)
    out_term, head_term, (down_sum, gate_sum, up_sum), normed_grad = barrier(
        (out_term, head_term, scattered, normed_grad)
    )
    out_sum = lax.psum_scatter(out_term, "fsdp", scatter_dimension=0, tiled=True).astype(f32)
    gate_sum, up_sum, down_sum = widen(gate_sum), widen(up_sum), widen(down_sum)
    input_back, attn_gain_term = norm_backward(inputs, inverse_norm(inputs), gain_attn, normed_grad)
    tokens_grad = mid_grad + input_back
    head_term = lax.psum_scatter(head_term, "fsdp", scatter_dimension=0, tiled=True)
    head_term = head_term.reshape(n, part, 3, span)
    head_term = lax.all_to_all(head_term, "seq", split_axis=0, concat_axis=0, tiled=True)
    head_sums = [
        head_term[:, :, i].swapaxes(0, 1).reshape(part, width).astype(f32) for i in range(3)
    ]
    by_span = lambda v: v.reshape(n, 1, span)
    sent_gains = jnp.concatenate([by_span(attn_gain_term), by_span(ffn_gain_term)], axis=1)
    sent_gains = jnp.pad(sent_gains, ((0, 0), (0, 6), (0, 0)))
    gain_sums = sum_gains(sent_gains, gain_terms, n, groups, 8)
    gain_sums = lax.dynamic_slice_in_dim(gain_sums, lax.axis_index("fsdp") * part, part, 1)
    return (
        block_out.astype(bf).reshape(tokens.shape),
        tokens_grad.reshape(tokens.shape),
        gain_sums[0],
        gain_sums[2],
        gain_sums[3],
        gain_sums[1],
        head_sums[0],
        head_sums[1],
        head_sums[2],
        out_sum,
        gate_sum,
        up_sum,
        down_sum,
    )


def solution(mesh):
    rows3 = P("fsdp", "seq", None)
    both = P(("seq", "fsdp"))
    both2 = P(("seq", "fsdp"), None)
    placed = (rows3,) * 4 + (P("fsdp"),) * 4 + (P("fsdp", None),) * 4 + (rows3,) * 3
    return jax.shard_map(
        local,
        mesh=mesh,
        in_specs=placed,
        out_specs=(rows3,) * 2 + (both,) * 4 + (both2,) * 4 + (rows3,) * 3,
        check_vma=False,
    )
```

```python
import functools
import jax
import jax.numpy as jnp
from jax import lax
from jax.experimental import pallas as pl
from jax.experimental.pallas import tpu as pltpu
from jax.sharding import PartitionSpec as P


MESH = pl.DeviceIdType.MESH
ANY = pl.ANY
H = 16
epsilon = 1e-05


def work(us):
    return pl.CostEstimate(flops=int(us * 6e8), bytes_accessed=0, transcendentals=0)


def greet(peers):
    barrier = pltpu.get_barrier_semaphore()
    for peer in peers:
        pl.semaphore_signal(barrier, inc=1, device_id={"seq": peer}, device_id_type=MESH)
    pl.semaphore_wait(barrier, len(peers))


def push(src, dst, send, recv, peer):
    return pltpu.make_async_remote_copy(
        src_ref=src, dst_ref=dst, send_sem=send, recv_sem=recv,
        device_id={"seq": peer}, device_id_type=MESH)


def gather_kernel(n, pieces, by_index, own, out, send_sem, recv_sem, copy_sem):
    pair = 2
    lines = n // pair
    me = lax.axis_index("seq")
    a, b = me // pair, me % pair
    column = [((a + k) % lines) * pair + b for k in range(1, lines)]
    across = a * pair + (1 - b)
    greet(column + [across])
    rows = own.shape[0] // pieces
    if by_index:
        here = [((a + lines - k) % lines) * pair + b for k in range(lines)]
        there = [((a + lines - k) % lines) * pair + 1 - b for k in range(lines)]
        sent = [me] * lines
        relayed = here
    else:
        here, there = list(range(lines)), list(range(lines, n))
        sent = here
        relayed = there
    local = pltpu.make_async_copy(own, out.at[here[0]], copy_sem)
    local.start()

    def piece(p):
        return pl.ds(p * rows, rows)

    sends = []
    for p in range(pieces):
        for k in range(lines):
            peer = across if k == 0 else column[k - 1]
            place = relayed[0] if k == 0 else sent[k]
            copy = push(own.at[piece(p)], out.at[place, piece(p)], send_sem.at[k, p], recv_sem.at[k, p], peer)
            copy.start()
            sends.append(copy)
    relays = []
    for p in range(pieces):
        for k in range(1, lines):
            push(own.at[piece(p)], out.at[here[k], piece(p)], send_sem.at[k, p], recv_sem.at[k, p], across).wait_recv()
            slot = lines + k - 1
            copy = push(
                out.at[here[k], piece(p)], out.at[relayed[k], piece(p)], send_sem.at[slot, p], recv_sem.at[slot, p], across
            )
            copy.start()
            relays.append(copy)
    for p in range(pieces):
        push(own.at[piece(p)], out.at[there[0], piece(p)], send_sem.at[0, p], recv_sem.at[0, p], across).wait_recv()
    for copy in relays:
        copy.wait_recv()
    for copy in sends + relays:
        copy.wait_send()
    local.wait()


def gather_rows(x, n, pieces, by_index, collective_id):
    slots = n // 2 + n // 2 - 1
    return pl.pallas_call(
        functools.partial(gather_kernel, n, pieces, by_index),
        out_shape=jax.ShapeDtypeStruct((n,) + x.shape, x.dtype),
        in_specs=[pl.BlockSpec(memory_space=pltpu.VMEM)],
        out_specs=pl.BlockSpec(memory_space=ANY),
        scratch_shapes=[
            pltpu.SemaphoreType.DMA((slots, pieces)),
            pltpu.SemaphoreType.DMA((slots, pieces)),
            pltpu.SemaphoreType.DMA,
        ],
        compiler_params=pltpu.CompilerParams(collective_id=collective_id, has_side_effects=True),
        cost_estimate=work(105),
        name="gather_rows",
    )(x)


def reduce_terms_kernel(
    n, pieces, tile, part, x, first, second, out, first_term, second_term,
    mine, got, sums, landed, x_buf, g_buf, o_buf, send_sem, recv_sem, load_sem, x_sem, g_sem, o_sem
):
    pair = 2
    lines = n // pair
    me = lax.axis_index("seq")
    a, b = me // pair, me % pair
    across = a * pair + (1 - b)
    greet([((a + lines - k) % lines) * pair + b for k in range(1, lines)] + [across])
    rows = out.shape[0] // pieces
    experts, _, width = x.shape
    tiles = width // tile
    jobs = experts * tiles
    terms = (first_term, second_term)

    def piece(p):
        return pl.ds(pl.multiple_of(p * rows, rows), rows)

    def first_copy(k, p):
        return push(part.at[lines + k, piece(p)], got.at[k, piece(p)], send_sem.at[k, p], recv_sem.at[k, p], across)

    def load(k, p):
        return pltpu.make_async_copy(part.at[k, piece(p)], mine.at[k, piece(p)], load_sem.at[k, p])

    def second_copy(k, p):
        peer = ((a + lines - k) % lines) * pair + b
        slot = lines + k - 1
        return push(sums.at[k - 1, piece(p)], landed.at[k - 1, piece(p)], send_sem.at[slot, p], recv_sem.at[slot, p], peer)

    def x_copy(j):
        cols = pl.ds(pl.multiple_of(j % tiles * tile, tile), tile)
        return pltpu.make_async_copy(x.at[j // tiles, :, cols], x_buf.at[j % 2], x_sem.at[j % 2])

    def g_copies(e):
        return [
            pltpu.make_async_copy(g.at[e], g_buf.at[e % 2, i], g_sem.at[e % 2, i]) for i, g in enumerate((first, second))
        ]

    def o_copies(j):
        place = pl.ds(pl.multiple_of(j % tiles * tile, tile), tile)
        return [
            pltpu.make_async_copy(o_buf.at[j % 2, i], o.at[j // tiles, place, :], o_sem.at[j % 2, i])
            for i, o in enumerate(terms)
        ]

    for k in list(range(1, lines)) + [0]:
        for p in range(pieces):
            first_copy(k, p).start()
            load(k, p).start()
    x_copy(0).start()
    for copy in g_copies(0):
        copy.start()

    def add(k, p):
        first_copy(k, p).wait_recv()
        load(k, p).wait()
        return mine[k, piece(p)].astype(jnp.float32) + got[k, piece(p)].astype(jnp.float32)

    def step(s):
        k, p = 1 + s // pieces, s % pieces
        sums[k - 1, piece(p)] = add(k, p).astype(jnp.bfloat16)
        second_copy(k, p).start()

    def job(j):
        @pl.when(j + 1 < jobs)
        def _():
            x_copy(j + 1).start()

        @pl.when(j % tiles == 0)
        def _():
            for copy in g_copies(j // tiles):
                copy.wait()

            @pl.when(j // tiles + 1 < experts)
            def _():
                for copy in g_copies(j // tiles + 1):
                    copy.start()

        @pl.when(j >= 2)
        def _():
            for copy in o_copies(j - 2):
                copy.wait()

        x_copy(j).wait()
        for i in range(2):
            o_buf[j % 2, i] = down_rows(x_buf[j % 2], g_buf[j // tiles % 2, i]).astype(jnp.bfloat16)
        for copy in o_copies(j):
            copy.start()

    steps = (lines - 1) * pieces
    per = steps * 2 // jobs

    def both(t, _):
        for i in range(per):
            step(t * per + i)
            if i == 0:
                job(2 * t)
            if i == per - 1:
                job(2 * t + 1)
        return 0

    lax.fori_loop(0, jobs // 2, both, 0)
    for copy in o_copies(jobs - 2) + o_copies(jobs - 1):
        copy.wait()

    def finish(p, _):
        total = add(0, p)
        for k in range(1, lines):
            second_copy(k, p).wait_recv()
            total += landed[k - 1, piece(p)].astype(jnp.float32)
        out[piece(p), :] = total
        return 0

    lax.fori_loop(0, pieces, finish, 0)
    for p in range(pieces):
        for k in range(lines):
            first_copy(k, p).wait_send()
        for k in range(1, lines):
            second_copy(k, p).wait_send()


def reduce_terms(part, x, first, second, n, pieces, tile, collective_id):
    _, rows, width = part.shape
    experts, tokens, _ = x.shape
    hidden = first.shape[2]
    lines = n // 2
    slots = lines + lines - 1
    hbm = pl.BlockSpec(memory_space=ANY)
    term = jax.ShapeDtypeStruct((experts, width, hidden), jnp.bfloat16)
    return pl.pallas_call(
        functools.partial(reduce_terms_kernel, n, pieces, tile),
        out_shape=(jax.ShapeDtypeStruct((rows, width), jnp.float32), term, term),
        in_specs=[hbm] * 4,
        out_specs=[pl.BlockSpec(memory_space=pltpu.VMEM), hbm, hbm],
        scratch_shapes=[
            pltpu.VMEM((lines, rows, width), jnp.bfloat16),
            pltpu.VMEM((lines, rows, width), jnp.bfloat16),
            pltpu.VMEM((lines - 1, rows, width), jnp.bfloat16),
            pltpu.VMEM((lines - 1, rows, width), jnp.bfloat16),
            pltpu.VMEM((2, tokens, tile), jnp.bfloat16),
            pltpu.VMEM((2, 2, tokens, hidden), jnp.bfloat16),
            pltpu.VMEM((2, 2, tile, hidden), jnp.bfloat16),
            pltpu.SemaphoreType.DMA((slots, pieces)),
            pltpu.SemaphoreType.DMA((slots, pieces)),
            pltpu.SemaphoreType.DMA((lines, pieces)),
            pltpu.SemaphoreType.DMA((2,)),
            pltpu.SemaphoreType.DMA((2, 2)),
            pltpu.SemaphoreType.DMA((2, 2)),
        ],
        compiler_params=pltpu.CompilerParams(
            collective_id=collective_id, has_side_effects=True, vmem_limit_bytes=50 << 20
        ),
        cost_estimate=work(105),
        name="reduce_terms",
    )(part, x, first, second)


def reduce_sides_kernel(
    n, groups, pieces, block, part, head, wide, narrow_a, narrow_b,
    out, q_out, k_out, v_out, o_out, wide_a, wide_b,
    mine, got, sums, landed, head_own, head_land, wide_own, wide_land, head_sum, head_got, x_buf, o_buf,
    send_sem, recv_sem, load_sem, side_send, side_recv, side_load, swap_send, swap_recv, x_sem, o_sem
):
    pair = 2
    lines = n // pair
    me, group = lax.axis_index("seq"), lax.axis_index("fsdp")
    a, b = me // pair, me % pair
    across = a * pair + (1 - b)
    peers = [(me + k) % n for k in range(1, n)]
    mates = [(group + k) % groups for k in range(1, groups)]
    barrier = pltpu.get_barrier_semaphore()
    for peer in peers:
        pl.semaphore_signal(barrier, inc=1, device_id={"seq": peer}, device_id_type=MESH)
    for mate in mates:
        pl.semaphore_signal(barrier, inc=1, device_id={"fsdp": mate}, device_id_type=MESH)
    pl.semaphore_wait(barrier, n - 1 + groups - 1)
    rows = out.shape[0] // pieces
    experts, shard, _ = narrow_a.shape
    blocks = shard // block

    def piece(p):
        return pl.ds(pl.multiple_of(p * rows, rows), rows)

    def first_copy(k, p):
        there = ((a + lines - k) % lines) * pair + 1 - b
        return push(part.at[there, piece(p)], got.at[k, piece(p)], send_sem.at[k, p], recv_sem.at[k, p], across)

    def load(k, p):
        here = ((a + lines - k) % lines) * pair + b
        return pltpu.make_async_copy(part.at[here, piece(p)], mine.at[k, piece(p)], load_sem.at[k, p])

    def second_copy(k, p):
        peer = ((a + lines - k) % lines) * pair + b
        slot = lines + k - 1
        return push(sums.at[k - 1, piece(p)], landed.at[k - 1, piece(p)], send_sem.at[slot, p], recv_sem.at[slot, p], peer)

    def side_copy(i, k):
        src, dst = ((head, head_land), (wide, wide_land))[i]
        return pltpu.make_async_remote_copy(
            src_ref=src.at[mates[k - 1]], dst_ref=dst.at[k - 1],
            send_sem=side_send.at[i, k - 1], recv_sem=side_recv.at[i, k - 1],
            device_id={"fsdp": mates[k - 1]}, device_id_type=MESH)

    def job_refs(j, i):
        place = pl.ds(pl.multiple_of(j * block, block), block)
        return (narrow_a, narrow_b)[i].at[:, place, :], (wide_a, wide_b)[i].at[place]

    def x_copy(j, i):
        return pltpu.make_async_copy(job_refs(j, i)[0], x_buf.at[j % 2, i], x_sem.at[j % 2, i])

    def o_copy(j, i):
        return pltpu.make_async_copy(o_buf.at[j % 2, i], job_refs(j, i)[1], o_sem.at[j % 2, i])

    for k in list(range(1, lines)) + [0]:
        for p in range(pieces):
            first_copy(k, p).start()
            load(k, p).start()
    own_copies = [
        pltpu.make_async_copy(head.at[group], head_own, side_load.at[0]),
        pltpu.make_async_copy(wide.at[group], wide_own, side_load.at[1]),
    ]
    for copy in own_copies:
        copy.start()
    for i in range(2):
        for k in range(1, groups):
            side_copy(i, k).start()
        x_copy(0, i).start()

    def add(k, p):
        first_copy(k, p).wait_recv()
        load(k, p).wait()
        return mine[k, piece(p)].astype(jnp.float32) + got[k, piece(p)].astype(jnp.float32)

    def step(s):
        k, p = 1 + s // pieces, s % pieces
        sums[k - 1, piece(p)] = add(k, p).astype(jnp.bfloat16)
        second_copy(k, p).start()

    def job(j, i):
        @pl.when(j + 1 < blocks)
        def _():
            x_copy(j + 1, i).start()

        @pl.when(j >= 2)
        def _():
            o_copy(j - 2, i).wait()

        x_copy(j, i).wait()
        for e in range(experts):
            o_buf[j % 2, i, :, e, :] = x_buf[j % 2, i, e].astype(jnp.float32)
        o_copy(j, i).start()

    per = (lines - 1) * pieces // blocks

    def both(t, _):
        for i in range(per):
            step(t * per + i)
            if i == 0:
                job(t, 0)
            if i == per - 1:
                job(t, 1)
        return 0

    lax.fori_loop(0, blocks, both, 0)
    for i in range(2):
        for j in range(max(0, blocks - 2), blocks):
            o_copy(j, i).wait()

    for copy in own_copies:
        copy.wait()
    total, side = head_own[...].astype(jnp.float32), wide_own[...].astype(jnp.float32)
    for k in range(1, groups):
        side_copy(0, k).wait_recv()
        side_copy(1, k).wait_recv()
        total = total + head_land[k - 1].astype(jnp.float32)
        side = side + wide_land[k - 1].astype(jnp.float32)
    o_out[...] = side
    head_sum[...] = total.astype(jnp.bfloat16)
    count = o_out.shape[0]

    def swap(k):
        place = pl.ds(pl.multiple_of(peers[k - 1] * count, count), count)
        return push(head_sum.at[place], head_got.at[me], swap_send.at[k - 1], swap_recv.at[k - 1], peers[k - 1])

    for k in range(1, n):
        swap(k).start()
    head_got[me] = head_sum[pl.ds(pl.multiple_of(me * count, count), count), :]

    def finish(p, _):
        total = add(0, p)
        for k in range(1, lines):
            second_copy(k, p).wait_recv()
            total += landed[k - 1, piece(p)].astype(jnp.float32)
        out[piece(p), :] = total
        return 0

    lax.fori_loop(0, pieces, finish, 0)
    for k in range(1, n):
        swap(k).wait_recv()
    span = head.shape[2] // 3
    for s in range(n):
        for i, o in enumerate((q_out, k_out, v_out)):
            o[:, s * span : (s + 1) * span] = head_got[s, :, i * span : (i + 1) * span].astype(jnp.float32)
    for p in range(pieces):
        for k in range(lines):
            first_copy(k, p).wait_send()
        for k in range(1, lines):
            second_copy(k, p).wait_send()
    for i in range(2):
        for k in range(1, groups):
            side_copy(i, k).wait_send()
    for k in range(1, n):
        swap(k).wait_send()


def reduce_sides(part, head, wide, narrow_a, narrow_b, n, groups, pieces, collective_id):
    _, rows, width = part.shape
    _, blocks, outs = head.shape
    count = blocks // n
    experts, shard, hidden = narrow_a.shape
    block = min(64, shard)
    lines = n // 2
    slots = lines + lines - 1
    hbm = pl.BlockSpec(memory_space=ANY)
    vmem = pl.BlockSpec(memory_space=pltpu.VMEM)
    f32, bf = jnp.float32, jnp.bfloat16
    grad = jax.ShapeDtypeStruct((count, n * outs // 3), f32)
    widened = jax.ShapeDtypeStruct((shard, experts, hidden), f32)
    return pl.pallas_call(
        functools.partial(reduce_sides_kernel, n, groups, pieces, block),
        out_shape=(
            jax.ShapeDtypeStruct((rows, width), f32),
            grad, grad, grad,
            jax.ShapeDtypeStruct((count, wide.shape[2]), f32),
            widened, widened,
        ),
        in_specs=[hbm] * 5,
        out_specs=[vmem] * 5 + [hbm] * 2,
        scratch_shapes=[
            pltpu.VMEM((lines, rows, width), bf),
            pltpu.VMEM((lines, rows, width), bf),
            pltpu.VMEM((lines - 1, rows, width), bf),
            pltpu.VMEM((lines - 1, rows, width), bf),
            pltpu.VMEM((blocks, outs), bf),
            pltpu.VMEM((groups - 1, blocks, outs), bf),
            pltpu.VMEM((count, wide.shape[2]), bf),
            pltpu.VMEM((groups - 1, count, wide.shape[2]), bf),
            pltpu.VMEM((blocks, outs), bf),
            pltpu.VMEM((n, count, outs), bf),
            pltpu.VMEM((2, 2, experts, block, hidden), bf),
            pltpu.VMEM((2, 2, block, experts, hidden), f32),
            pltpu.SemaphoreType.DMA((slots, pieces)),
            pltpu.SemaphoreType.DMA((slots, pieces)),
            pltpu.SemaphoreType.DMA((lines, pieces)),
            pltpu.SemaphoreType.DMA((2, groups - 1)),
            pltpu.SemaphoreType.DMA((2, groups - 1)),
            pltpu.SemaphoreType.DMA((2,)),
            pltpu.SemaphoreType.DMA((n - 1,)),
            pltpu.SemaphoreType.DMA((n - 1,)),
            pltpu.SemaphoreType.DMA((2, 2)),
            pltpu.SemaphoreType.DMA((2, 2)),
        ],
        compiler_params=pltpu.CompilerParams(
            collective_id=collective_id, has_side_effects=True, vmem_limit_bytes=50 << 20
        ),
        cost_estimate=work(105),
        name="reduce_sides",
    )(part, head, wide, narrow_a, narrow_b)


def gains_kernel(n, groups, sent, own, out, taken, summed, landed, send_sem, recv_sem, side_send, side_recv):
    me, group = lax.axis_index("seq"), lax.axis_index("fsdp")
    barrier = pltpu.get_barrier_semaphore()
    peers = [(me + k) % n for k in range(1, n)]
    mates = [(group + k) % groups for k in range(1, groups)]
    for peer in peers:
        pl.semaphore_signal(barrier, inc=1, device_id={"seq": peer}, device_id_type=MESH)
    for mate in mates:
        pl.semaphore_signal(barrier, inc=1, device_id={"fsdp": mate}, device_id_type=MESH)
    pl.semaphore_wait(barrier, n - 1 + groups - 1)
    copies = []
    for k in range(1, n):
        copy = push(sent.at[peers[k - 1]], taken.at[k - 1], send_sem.at[k - 1], recv_sem.at[k - 1], peers[k - 1])
        copy.start()
        copies.append(copy)
    total = sent[me] + own[...]
    for k in range(1, n):
        copies[k - 1].wait_recv()
        total = total + taken[k - 1]
    summed[...] = total
    sides = []
    for k in range(1, groups):
        side = pltpu.make_async_remote_copy(
            src_ref=summed, dst_ref=landed.at[k - 1], send_sem=side_send.at[k - 1], recv_sem=side_recv.at[k - 1],
            device_id={"fsdp": mates[k - 1]}, device_id_type=MESH)
        side.start()
        sides.append(side)
    for k in range(1, groups):
        sides[k - 1].wait_recv()
        total = total + landed[k - 1]
    out[...] = total
    for copy in copies + sides:
        copy.wait_send()


def sum_gains(sent, own, n, groups, collective_id):
    shape = own.shape
    return pl.pallas_call(
        functools.partial(gains_kernel, n, groups),
        out_shape=jax.ShapeDtypeStruct(shape, own.dtype),
        in_specs=[pl.BlockSpec(memory_space=pltpu.VMEM)] * 2,
        out_specs=pl.BlockSpec(memory_space=pltpu.VMEM),
        scratch_shapes=[
            pltpu.VMEM((n - 1,) + shape, own.dtype),
            pltpu.VMEM(shape, own.dtype),
            pltpu.VMEM((groups - 1,) + shape, own.dtype),
            pltpu.SemaphoreType.DMA((n - 1,)),
            pltpu.SemaphoreType.DMA((n - 1,)),
            pltpu.SemaphoreType.DMA((groups - 1,)),
            pltpu.SemaphoreType.DMA((groups - 1,)),
        ],
        compiler_params=pltpu.CompilerParams(collective_id=collective_id, has_side_effects=True),
        cost_estimate=work(10),
        name="sum_gains",
    )(sent, own)


def widen_kernel(x_ref, o_ref):
    for e in range(x_ref.shape[0]):
        o_ref[:, e, :] = x_ref[e].astype(jnp.float32)


def widen(x):
    experts, rows, columns = x.shape
    step = min(128, rows)
    return pl.pallas_call(
        widen_kernel,
        grid=(rows // step,),
        out_shape=jax.ShapeDtypeStruct((rows, experts, columns), jnp.float32),
        in_specs=[pl.BlockSpec((experts, step, columns), lambda i: (0, i, 0))],
        out_specs=pl.BlockSpec((step, experts, columns), lambda i: (i, 0, 0)),
        cost_estimate=work(5),
        name="widen",
    )(x)


def masked(block):
    keys = lax.broadcasted_iota(jnp.int32, (block, block), 0)
    rows = lax.broadcasted_iota(jnp.int32, (block, block), 1)
    return keys <= rows


def across_lanes(a, b):
    return lax.dot_general(a, b, (((1,), (1,)), ((), ())), preferred_element_type=jnp.float32)


def down_rows(a, b):
    return lax.dot_general(a, b, (((0,), (0,)), ((), ())), preferred_element_type=jnp.float32)


LOG2E = 1.4426950408889634


def attend_kernel(block, scale, q_ref, k_ref, v_ref, o_ref, lse_ref, s_ref, acc_ref):
    length, _ = q_ref.shape

    def rows(i):
        return pl.ds(pl.multiple_of(i * block, block), block)

    def one_block(i, _):
        q = q_ref[rows(i), :]
        diag = across_lanes(k_ref[rows(i), :], q) * (scale * LOG2E)
        diag = jnp.where(masked(block), diag, -1e30)
        s_ref[rows(i), :] = diag
        peak = jnp.max(diag, axis=0, keepdims=True)

        def score(j, peak):
            s = across_lanes(k_ref[rows(j), :], q) * (scale * LOG2E)
            s_ref[rows(j), :] = s
            return jnp.maximum(peak, jnp.max(s, axis=0, keepdims=True))

        peak = lax.fori_loop(0, i, score, peak)
        acc_ref[...] = jnp.zeros_like(acc_ref)

        def weigh(j, total):
            p = jnp.exp2(s_ref[rows(j), :] - peak)
            acc_ref[...] += down_rows(v_ref[rows(j), :], p.astype(jnp.bfloat16))
            return total + jnp.sum(p, axis=0, keepdims=True)

        total = lax.fori_loop(0, i + 1, weigh, jnp.zeros_like(peak))
        o_ref[rows(i), :] = (acc_ref[...] / total).T.astype(o_ref.dtype)
        lse_ref[0, :, rows(i)] = peak + jnp.log2(total)
        return 0

    lax.fori_loop(0, length // block, one_block, 0)


def attend(q, k, v, heads, block, scale):
    length, width = q.shape
    dim = width // heads
    spec = pl.BlockSpec((length, dim), lambda h: (0, h))
    return pl.pallas_call(
        functools.partial(attend_kernel, block, scale),
        grid=(heads,),
        out_shape=(
            jax.ShapeDtypeStruct(q.shape, q.dtype),
            jax.ShapeDtypeStruct((heads, 1, length), jnp.float32),
        ),
        in_specs=[spec] * 3,
        out_specs=[spec, pl.BlockSpec((1, 1, length), lambda h: (h, 0, 0))],
        scratch_shapes=[
            pltpu.VMEM((length, block), jnp.float32),
            pltpu.VMEM((dim, block), jnp.float32),
        ],
        cost_estimate=work(25),
        name="attend",
    )(q, k, v)


def attend_back_kernel(
    block, scale, q_ref, k_ref, v_ref, g_ref, o_ref, lse_ref, dq_ref, dk_ref, dv_ref, dk_acc, dv_acc, dq_acc
):
    length, dim = q_ref.shape
    dk_acc[...] = jnp.zeros_like(dk_acc)
    dv_acc[...] = jnp.zeros_like(dv_acc)

    def rows(i):
        return pl.ds(pl.multiple_of(i * block, block), block)

    def one_block(i, _):
        q, g = q_ref[rows(i), :], g_ref[rows(i), :]
        lse = lse_ref[0, :, rows(i)]
        products = g.astype(jnp.float32) * o_ref[rows(i), :].astype(jnp.float32)
        shift = lax.dot_general(
            jnp.ones((8, dim), jnp.float32), products, (((1,), (1,)), ((), ())),
            precision=lax.Precision.HIGHEST, preferred_element_type=jnp.float32,
        )[:1]

        def pair(j, keep):
            k, v = k_ref[rows(j), :], v_ref[rows(j), :]
            p = jnp.exp2(across_lanes(k, q) * (scale * LOG2E) - lse)
            if keep is not None:
                p = jnp.where(keep, p, 0.0)
            ds = (p * (across_lanes(v, g) - shift) * scale).astype(jnp.bfloat16)
            dv_acc[rows(j), :] += jnp.dot(p.astype(jnp.bfloat16), g, preferred_element_type=jnp.float32)
            dk_acc[rows(j), :] += jnp.dot(ds, q, preferred_element_type=jnp.float32)
            dq_acc[...] += down_rows(k, ds)

        dq_acc[...] = jnp.zeros_like(dq_acc)
        pair(i, masked(block))

        def body(j, _):
            pair(j, None)
            return 0

        lax.fori_loop(0, i, body, 0)
        dq_ref[rows(i), :] = dq_acc[...].T.astype(dq_ref.dtype)
        return 0

    lax.fori_loop(0, length // block, one_block, 0)
    dk_ref[...] = dk_acc[...].astype(dk_ref.dtype)
    dv_ref[...] = dv_acc[...].astype(dv_ref.dtype)


def attend_back(q, k, v, g, o, lse, heads, block, scale):
    length, width = q.shape
    dim = width // heads
    spec = pl.BlockSpec((length, dim), lambda h: (0, h))
    return pl.pallas_call(
        functools.partial(attend_back_kernel, block, scale),
        grid=(heads,),
        out_shape=(jax.ShapeDtypeStruct(q.shape, q.dtype),) * 3,
        in_specs=[spec] * 5 + [pl.BlockSpec((1, 1, length), lambda h: (h, 0, 0))],
        out_specs=[spec] * 3,
        scratch_shapes=[
            pltpu.VMEM((length, dim), jnp.float32),
            pltpu.VMEM((length, dim), jnp.float32),
            pltpu.VMEM((dim, block), jnp.float32),
        ],
        cost_estimate=work(60),
        name="attend_back",
    )(q, k, v, g, o, lse)


def project_kernel(
    n, groups, pieces, own, w_query, w_key, w_value, gain_own,
    normed, proj, squares, w_ref, gains, held, send_sem, recv_sem, side_send, side_recv, copy_sem
):
    pair = 2
    lines = n // pair
    me, group = lax.axis_index("seq"), lax.axis_index("fsdp")
    a, b = me // pair, me % pair
    column = [((a + k) % lines) * pair + b for k in range(1, lines)]
    back = [((a + lines - k) % lines) * pair + b for k in range(1, lines)]
    across = a * pair + (1 - b)
    mates = [(group + k) % groups for k in range(1, groups)]
    barrier = pltpu.get_barrier_semaphore()
    for peer in column + [across]:
        pl.semaphore_signal(barrier, inc=1, device_id={"seq": peer}, device_id_type=MESH)
    for mate in mates:
        pl.semaphore_signal(barrier, inc=1, device_id={"fsdp": mate}, device_id_type=MESH)
    pl.semaphore_wait(barrier, lines + groups - 1)
    rows, _ = own.shape
    step = rows // pieces
    span = w_ref.shape[1] // 3
    shard = w_query.shape[0]

    def piece(p):
        return pl.ds(p * step, step)

    sends = []
    for p in range(pieces):
        for k in range(lines):
            peer = across if k == 0 else column[k - 1]
            copy = push(own.at[piece(p)], held.at[me, piece(p)], send_sem.at[k, p], recv_sem.at[k, p], peer)
            copy.start()
            sends.append(copy)

    shard_rows = pl.ds(pl.multiple_of(group * shard, shard), shard)
    mine = pl.ds(pl.multiple_of(me * span, span), span)
    blocks = [
        (w.at[:, mine], w_ref.at[shard_rows, part * span : (part + 1) * span])
        for part, w in enumerate((w_query, w_key, w_value))
    ]
    blocks.append((gain_own, gains.at[:, shard_rows]))
    locals_, sides = [], []

    def side_copy(i, src, dst, slot, mate):
        return pltpu.make_async_remote_copy(
            src_ref=src, dst_ref=dst, send_sem=side_send.at[i, slot], recv_sem=side_recv.at[i, slot],
            device_id={"fsdp": mate}, device_id_type=MESH)

    def side_block(i, g):
        place = pl.ds(pl.multiple_of(g * shard, shard), shard)
        return gains.at[:, place] if i == 3 else w_ref.at[place, i * span : (i + 1) * span]

    chips = groups // 2
    partner = group // 2 * 2 + 1 - group % 2
    alike = [(group + 2 * k) % groups for k in range(1, chips)]
    behind = [(group + groups - 2 * k) % groups for k in range(1, chips)]
    for i, (src, dst) in enumerate(blocks):
        for k in range(chips):
            side = side_copy(i, src, dst, k, partner if k == 0 else alike[k - 1])
            side.start()
            sides.append(side)
        local = pltpu.make_async_copy(src, dst, copy_sem.at[i])
        local.start()
        locals_.append(local)
    for k in range(1, chips):
        for i in range(4):
            block = side_block(i, behind[k - 1])
            side_copy(i, block, block, k, partner).wait_recv()
            side = side_copy(i, block, block, chips + k - 1, partner)
            side.start()
            sides.append(side)

    def project(src, chunk):
        x = chunk[...].astype(jnp.float32)
        factor = lax.rsqrt(jnp.mean(x * x, axis=-1, keepdims=True) + epsilon)
        place = pl.ds(pl.multiple_of(src * rows, rows), rows)
        normed[place, :] = (x * factor * gains[0:1, :]).astype(jnp.bfloat16)
        for part in range(3):
            cols = slice(part * span, (part + 1) * span)
            out = jnp.dot(normed[place, :], w_ref[:, cols], preferred_element_type=jnp.float32)
            proj[place, cols] = out
            if part < 2:
                sums = lax.dot_general(
                    jnp.ones((8, span), jnp.float32), out * out, (((1,), (1,)), ((), ())),
                    precision=lax.Precision.HIGHEST, preferred_element_type=jnp.float32,
                )
                squares[pl.ds(part * n + src, 1), :] = sums[:1]

    relays = []
    for p in range(pieces):
        for k in range(1, lines):
            src = back[k - 1]
            push(own.at[piece(p)], held.at[src, piece(p)], send_sem.at[k, p], recv_sem.at[k, p], across).wait_recv()
            slot = lines + k - 1
            copy = push(held.at[src, piece(p)], held.at[src, piece(p)], send_sem.at[slot, p], recv_sem.at[slot, p], across)
            copy.start()
            relays.append(copy)
    for copy in locals_:
        copy.wait()
    for i in range(4):
        for k in [0] + list(range(chips, 2 * chips - 1)):
            side_copy(i, blocks[i][0], blocks[i][1], k, partner).wait_recv()
    project(me, own)
    for p in range(pieces):
        push(own.at[piece(p)], held.at[across, piece(p)], send_sem.at[0, p], recv_sem.at[0, p], across).wait_recv()
    project(across, held.at[across])
    for k in range(1, lines):
        project(back[k - 1], held.at[back[k - 1]])
    for k in range(1, lines):
        for p in range(pieces):
            relays[p * (lines - 1) + k - 1].wait_recv()
        src = ((a + lines - k) % lines) * pair + 1 - b
        project(src, held.at[src])
    for copy in sends + relays + sides:
        copy.wait_send()


def project_rows(x, w_query, w_key, w_value, gains, n, groups, pieces, collective_id):
    rows, width = x.shape
    span = w_query.shape[1] // n
    slots = n // 2 + n // 2 - 1
    vmem = pl.BlockSpec(memory_space=pltpu.VMEM)
    hbm = pl.BlockSpec(memory_space=ANY)
    return pl.pallas_call(
        functools.partial(project_kernel, n, groups, pieces),
        out_shape=(
            jax.ShapeDtypeStruct((n * rows, width), jnp.bfloat16),
            jax.ShapeDtypeStruct((n * rows, 3 * span), jnp.float32),
            jax.ShapeDtypeStruct((2 * n, rows), jnp.float32),
            jax.ShapeDtypeStruct((width, 3 * span), jnp.bfloat16),
            jax.ShapeDtypeStruct((8, width), jnp.float32),
        ),
        in_specs=[vmem, hbm, hbm, hbm, vmem],
        out_specs=[vmem] * 5,
        scratch_shapes=[
            pltpu.VMEM((n, rows, width), jnp.bfloat16),
            pltpu.SemaphoreType.DMA((slots, pieces)),
            pltpu.SemaphoreType.DMA((slots, pieces)),
            pltpu.SemaphoreType.DMA((4, groups - 1)),
            pltpu.SemaphoreType.DMA((4, groups - 1)),
            pltpu.SemaphoreType.DMA((4,)),
        ],
        compiler_params=pltpu.CompilerParams(
            collective_id=collective_id, has_side_effects=True, vmem_limit_bytes=50 << 20
        ),
        cost_estimate=work(110),
        name="project_rows",
    )(x, w_query, w_key, w_value, gains)


def as_columns(row, lanes):
    return jnp.broadcast_to(row, (lanes, row.shape[1])).T


def turn_tables(c, near_cos, near_sin, far_cos, far_sin):
    far_c, far_s = far_cos[pl.ds(c, 1), :], far_sin[pl.ds(c, 1), :]
    cosine = near_cos[...] * far_c - near_sin[...] * far_s
    sine = near_sin[...] * far_c + near_cos[...] * far_s
    first = lax.broadcasted_iota(jnp.int32, sine.shape, 1) < sine.shape[1] // 2
    return cosine, jnp.where(first, -sine, sine)


def add_over_seq(n, own, landed, send_sem, recv_sem, peers):
    copies = []
    for k in range(1, n):
        copy = push(own, landed.at[k - 1], send_sem.at[k - 1], recv_sem.at[k - 1], peers[k - 1])
        copy.start()
        copies.append(copy)
    return copies


def rotate_kernel(
    n, full, squares, sent, proj, gains, near_cos, near_sin, far_cos, far_sin,
    queries, keys, values, factors, taken, landed, send_sem, recv_sem, copy_sem
):
    me = lax.axis_index("seq")
    peers = [(me + k) % n for k in range(1, n)]
    greet(peers)
    local = pltpu.make_async_copy(sent.at[me], taken.at[me], copy_sem)
    local.start()
    copies = add_over_seq(n, squares, landed, send_sem.at[0], recv_sem.at[0], peers)
    swaps = []
    for k in range(1, n):
        swap = push(sent.at[peers[k - 1]], taken.at[me], send_sem.at[1, k - 1], recv_sem.at[1, k - 1], peers[k - 1])
        swap.start()
        swaps.append(swap)
    span = queries.shape[1]
    rows = squares.shape[1]
    lanes = near_cos.shape[1]
    total = squares[...]
    for k in range(1, n):
        copies[k - 1].wait_recv()
        total = total + landed[k - 1]
    factors[...] = lax.rsqrt(total / full + epsilon)

    def chunk(c, _):
        place = pl.ds(pl.multiple_of(c * rows, rows), rows)
        cosine, sine = turn_tables(c, near_cos, near_sin, far_cos, far_sin)
        for part, out in ((0, queries), (1, keys)):
            factor = as_columns(factors[pl.ds(part * n + c, 1), :], lanes)
            for h in range(span // lanes):
                cols = slice(part * span + h * lanes, part * span + (h + 1) * lanes)
                x = proj[place, cols] * factor * gains[part : part + 1, h * lanes : (h + 1) * lanes]
                turned = x * cosine + pltpu.roll(x, lanes // 2, 1) * sine
                out[place, h * lanes : (h + 1) * lanes] = turned.astype(jnp.bfloat16)
        values[place, :] = proj[place, 2 * span :].astype(jnp.bfloat16)
        return 0

    lax.fori_loop(0, n, chunk, 0)
    for copy in copies:
        copy.wait_send()
    for swap in swaps:
        swap.wait()
    local.wait()


def rotate_rows(squares, sent, proj, gains, tables, n, full, collective_id):
    length, outs = proj.shape
    span = outs // 3
    vmem = pl.BlockSpec(memory_space=pltpu.VMEM)
    heads = jax.ShapeDtypeStruct((length, span), jnp.bfloat16)
    return pl.pallas_call(
        functools.partial(rotate_kernel, n, full),
        out_shape=(
            heads, heads, heads,
            jax.ShapeDtypeStruct(squares.shape, jnp.float32),
            jax.ShapeDtypeStruct(sent.shape, sent.dtype),
        ),
        in_specs=[vmem] * 8,
        out_specs=[vmem] * 5,
        scratch_shapes=[
            pltpu.VMEM((n - 1,) + squares.shape, jnp.float32),
            pltpu.SemaphoreType.DMA((2, n - 1)),
            pltpu.SemaphoreType.DMA((2, n - 1)),
            pltpu.SemaphoreType.DMA,
        ],
        compiler_params=pltpu.CompilerParams(
            collective_id=collective_id, has_side_effects=True, vmem_limit_bytes=40 << 20
        ),
        cost_estimate=work(15),
        name="rotate_rows",
    )(squares, sent, proj, gains, *tables)


def heads_back_kernel(
    n, full, dq, dk, dv, proj, factors, gains, near_cos, near_sin, far_cos, far_sin,
    grads, gain_grads, sums, landed, send_sem, recv_sem
):
    me = lax.axis_index("seq")
    peers = [(me + k) % n for k in range(1, n)]
    greet(peers)
    span = dq.shape[1]
    rows = sums.shape[1]
    lanes = near_cos.shape[1]
    count = span // lanes

    def parts(c, part, h, grad):
        place = pl.ds(pl.multiple_of(c * rows, rows), rows)
        cosine, sine = turn_tables(c, near_cos, near_sin, far_cos, far_sin)
        g = grad[place, h * lanes : (h + 1) * lanes].astype(jnp.float32)
        up = g * cosine + pltpu.roll(g * sine, lanes // 2, 1)
        factor = as_columns(factors[pl.ds(part * n + c, 1), :], lanes)
        cols = slice(part * span + h * lanes, part * span + (h + 1) * lanes)
        normal = proj[place, cols] * factor
        weighted = up * gains[part : part + 1, h * lanes : (h + 1) * lanes]
        return place, cols, up, factor, normal, weighted

    def first(c, _):
        for part, grad in ((0, dq), (1, dk)):
            products = 0.0
            for h in range(count):
                _, _, _, _, normal, weighted = parts(c, part, h, grad)
                products = products + weighted * normal
            total = lax.dot_general(
                jnp.ones((8, lanes), jnp.float32), products, (((1,), (1,)), ((), ())),
                precision=lax.Precision.HIGHEST, preferred_element_type=jnp.float32,
            )
            sums[pl.ds(part * n + c, 1), :] = total[:1]
        return 0

    lax.fori_loop(0, n, first, 0)
    copies = add_over_seq(n, sums, landed, send_sem, recv_sem, peers)
    gain_grads[...] = jnp.zeros_like(gain_grads)

    def gain_sum(c, _):
        for part, grad in ((0, dq), (1, dk)):
            for h in range(count):
                _, _, up, _, normal, _ = parts(c, part, h, grad)
                cell = (slice(part + 2, part + 3), slice(h * lanes, (h + 1) * lanes))
                gain_grads[cell] += jnp.sum(up * normal, axis=0, keepdims=True)
        place = pl.ds(pl.multiple_of(c * rows, rows), rows)
        grads[place, 2 * span :] = dv[place, :]
        return 0

    lax.fori_loop(0, n, gain_sum, 0)
    total = sums[...]
    for k in range(1, n):
        copies[k - 1].wait_recv()
        total = total + landed[k - 1]
    landed[0] = total / full

    def last(c, _):
        for part, grad in ((0, dq), (1, dk)):
            mean = as_columns(landed[0, pl.ds(part * n + c, 1), :], lanes)
            for h in range(count):
                place, cols, _, factor, normal, weighted = parts(c, part, h, grad)
                grads[place, cols] = (factor * (weighted - normal * mean)).astype(jnp.bfloat16)
        return 0

    lax.fori_loop(0, n, last, 0)
    for copy in copies:
        copy.wait_send()


def heads_back(dq, dk, dv, proj, factors, gains, tables, n, full, collective_id):
    length, span = dq.shape
    vmem = pl.BlockSpec(memory_space=pltpu.VMEM)
    return pl.pallas_call(
        functools.partial(heads_back_kernel, n, full),
        out_shape=(
            jax.ShapeDtypeStruct((length, 3 * span), jnp.bfloat16),
            jax.ShapeDtypeStruct((8, span), jnp.float32),
        ),
        in_specs=[vmem] * 10,
        out_specs=[vmem] * 2,
        scratch_shapes=[
            pltpu.VMEM(factors.shape, jnp.float32),
            pltpu.VMEM((n - 1,) + factors.shape, jnp.float32),
            pltpu.SemaphoreType.DMA((n - 1,)),
            pltpu.SemaphoreType.DMA((n - 1,)),
        ],
        compiler_params=pltpu.CompilerParams(
            collective_id=collective_id, has_side_effects=True, vmem_limit_bytes=40 << 20
        ),
        cost_estimate=work(20),
        name="heads_back",
    )(dq, dk, dv, proj, factors, gains, *tables)


def turn_parts(rows, n, dim):
    half = dim // 2
    frequency = jnp.power(10000.0, -2.0 * jnp.arange(half, dtype=jnp.float32) / dim)
    frequency = jnp.concatenate([frequency, frequency])[None]
    near = jnp.arange(rows, dtype=jnp.float32)[:, None] * frequency
    far = (rows * jnp.arange(n)).astype(jnp.float32)[:, None] * frequency
    return jnp.cos(near), jnp.sin(near), jnp.cos(far), jnp.sin(far)


def inverse_norm(values):
    return lax.rsqrt(jnp.mean(values * values, axis=-1, keepdims=True) + epsilon)


def norm_backward(values, factor, gain, upstream):
    normal = values * factor
    weighted = upstream * gain
    gain_term = jnp.sum(upstream * normal, axis=0)
    back = factor * (weighted - normal * jnp.mean(weighted * normal, axis=-1, keepdims=True))
    return (back, gain_term)


def across_pairs(lines, pair):
    return [(a * pair + b, a * pair + 1 - b) for a in range(lines) for b in range(pair)]


def along_lines(lines, pair, k):
    return [(a * pair + b, (a + k) % lines * pair + b) for a in range(lines) for b in range(pair)]


def by_place(v, n):
    lines = n // 2
    me = lax.axis_index("seq")
    a, b = me // 2, me % 2
    column = [((a + lines - k) % lines) * 2 for k in range(lines)]
    order = jnp.stack([c + b for c in column] + [c + 1 - b for c in column])
    return v[order]


def gather_column(x, n):
    lines = n // 2
    return [lax.ppermute(x, "seq", along_lines(lines, 2, k)) for k in range(1, lines)]


def gather_across(column, n):
    return [lax.ppermute(c, "seq", across_pairs(n // 2, 2)) for c in column]


def reduce_column(v, k, n):
    return lax.ppermute(v, "seq", along_lines(n // 2, 2, n // 2 - k))


def local(
    tokens, routes, route_weights, cotangent, attn_gain, query_gain, key_gain, ffn_gain,
    w_query, w_key, w_value, w_out, w_gate, w_up, w_down,
):
    n = lax.axis_size("seq")
    groups = lax.axis_size("fsdp")
    me = lax.axis_index("seq")
    width = tokens.shape[-1]
    own_tokens = tokens.reshape(-1, width)
    rows = own_tokens.shape[0]
    length = rows * n
    picks = routes.shape[-1]
    local_experts = w_gate.shape[1]
    experts = local_experts * n
    capacity = 3 * rows * picks // (2 * experts)
    head_dim = width // H
    heads = H // n
    span = heads * head_dim
    part = width // (n * groups)
    scale = head_dim ** (-0.5)
    bf, f32 = jnp.bfloat16, jnp.float32
    barrier = lax.optimization_barrier

    own_gains = jnp.stack([attn_gain, query_gain, key_gain, ffn_gain]).astype(f32)
    own_gains = jnp.pad(own_gains, ((0, 4), (0, 0)))
    full_out = lax.all_gather(w_out, "fsdp", axis=0, tiled=True)
    by_expert = lambda w: lax.all_gather(jnp.swapaxes(w, 0, 1), "fsdp", axis=1, tiled=True)
    full_gate = by_expert(w_gate)
    normed, proj, squares, w_heads, gains = project_rows(
        own_tokens, w_query, w_key, w_value, own_gains, n, groups, 8, 0
    )
    w_up, w_down, squares = barrier((w_up, w_down, squares))
    full_up, full_down = by_expert(w_up), by_expert(w_down)
    gain_attn, gain_ffn = gains[0], gains[3]
    head_gains = lax.dynamic_slice(gains, (1, me * span), (2, span))

    expert_ids = jnp.arange(experts, dtype=jnp.int32)
    named = routes.reshape(rows, picks)[None] == expert_ids[:, None, None]
    mixing = route_weights.reshape(rows, picks)[None]
    sent = jnp.sum(jnp.where(named, mixing, 0.0), axis=-1).reshape(n, local_experts, rows)
    tables = turn_parts(rows, n, head_dim)
    queries, keys, values, factors, weights = rotate_rows(
        squares, sent, proj, head_gains, tables, n, width, 1
    )
    block = min(512, length)
    heads_out, log_totals = attend(queries, keys, values, heads, block, scale)
    context = lax.all_to_all(heads_out, "seq", split_axis=0, concat_axis=1, tiled=True)
    inputs = own_tokens.astype(f32)
    mid = inputs + jnp.dot(context, full_out, preferred_element_type=f32)
    norm_two = inverse_norm(mid)
    ffn_in = (mid * norm_two * gain_ffn).astype(bf)

    ffn_all = gather_rows(ffn_in, n, 8, False, 2)
    cot_own, ffn_all = barrier((cotangent.reshape(rows, width), ffn_all))
    half = rows // 2
    cot_halves = [cot_own[:half], cot_own[half:]]
    cot_columns = [gather_column(cot_halves[0], n)]
    cot_columns.append(gather_column(cot_halves[1], n))
    cot_others = [gather_across([v], n) for v in cot_halves]
    weights = by_place(weights, n)
    taken = weights > 0
    tri = (jnp.arange(rows)[:, None] <= jnp.arange(rows)[None, :]).astype(bf)
    rank = jnp.einsum("cet,tu->ceu", taken.astype(bf), tri, preferred_element_type=f32) - 1.0
    slot_ids = jnp.arange(capacity, dtype=f32)
    hit = (rank[:, :, None, :] == slot_ids[None, None, :, None]) & taken[:, :, None, :]
    place = hit.astype(bf)
    slot_weight = jnp.sum(jnp.where(hit, weights[:, :, None, :], 0.0), axis=-1)
    slot_weight = jnp.swapaxes(slot_weight, 0, 1)[..., None]
    place_rows = lambda v: jnp.einsum("cert,ctd->ecrd", place, v, preferred_element_type=f32)
    unplace = lambda v: jnp.einsum("cert,ecrd->ctd", place, v, preferred_element_type=f32).astype(bf)
    received = place_rows(ffn_all).astype(bf)
    gate = jnp.einsum("ecrd,edf->ecrf", received, full_gate, preferred_element_type=f32)
    cot_others[0] += gather_across(cot_columns[0], n)
    cot_others[1] += gather_across(cot_columns[1], n)
    up_part = jnp.einsum("ecrd,edf->ecrf", received, full_up, preferred_element_type=f32)
    sigmoid_gate = jax.nn.sigmoid(gate)
    activated = gate * sigmoid_gate
    hidden = (activated * up_part).astype(bf)
    expert_out = jnp.einsum("ecrf,edf->ecrd", hidden, full_down, preferred_element_type=f32)
    expert_out = (expert_out * slot_weight).astype(bf)
    ffn_part = unplace(expert_out)
    ffn_part, cot_others = barrier((ffn_part, cot_others))
    cot_all = jnp.stack(
        [jnp.concatenate(v) for v in zip(*(([h] + c + o) for h, c, o in zip(cot_halves, cot_columns, cot_others)))]
    )
    lines = n // 2
    ffn_got = {k: gather_across([ffn_part[lines + k]], n)[0] for k in list(range(1, lines)) + [0]}
    ffn_keep = [barrier(ffn_part[k]) for k in range(lines)]
    ffn_sum = lambda k: (ffn_keep[k].astype(f32) + ffn_got[k].astype(f32)).astype(bf)

    out_grad = cotangent.reshape(rows, width).astype(f32)
    down_received = (place_rows(cot_all) * slot_weight).astype(bf)
    hidden_grad = jnp.einsum("ecrd,edf->ecrf", down_received, full_down, preferred_element_type=f32)
    slope = sigmoid_gate * (1.0 + gate * (1.0 - sigmoid_gate))
    gate_grad = (hidden_grad * up_part * slope).astype(bf)
    up_grad = (hidden_grad * activated).astype(bf)
    early = list(range(1, lines - 1))
    gate_grad, up_grad, got = barrier((gate_grad, up_grad, [ffn_got[k] for k in early]))
    ffn_got.update(zip(early, got))
    ffn_pieces = [reduce_column(ffn_sum(k), k, n) for k in early]
    rows_gate = jnp.einsum("ecrf,edf->ecrd", gate_grad, full_gate, preferred_element_type=f32)
    rows_gate, ffn_got[lines - 1] = barrier((rows_gate, ffn_got[lines - 1]))
    ffn_pieces.append(reduce_column(ffn_sum(lines - 1), lines - 1, n))
    rows_up = jnp.einsum("ecrf,edf->ecrd", up_grad, full_up, preferred_element_type=f32)
    rows_part = unplace((rows_gate + rows_up).astype(bf))
    down_term = jnp.einsum("ecrd,ecrf->edf", down_received, hidden, preferred_element_type=f32)
    scatter = lambda v: lax.psum_scatter(v, "fsdp", scatter_dimension=1, tiled=True)
    rows_part, ffn_pieces, ffn_got[0], down_term = barrier(
        (rows_part, ffn_pieces, ffn_got[0], down_term.astype(bf))
    )
    by_slot = lambda v: v.reshape(local_experts, n * capacity, v.shape[-1])
    ffn_in_grad, gate_term, up_term = reduce_terms(
        rows_part, by_slot(received), by_slot(gate_grad), by_slot(up_grad), n, 8, 512, 4
    )
    scattered = [scatter(down_term)]
    scattered += [scatter(gate_term), scatter(up_term)]
    mid_back, ffn_gain_term = norm_backward(mid, norm_two, gain_ffn, ffn_in_grad)
    mid_grad = out_grad + mid_back
    branch_grad = mid_grad.astype(bf)

    branch_all = gather_rows(branch_grad, n, 8, True, 5).reshape(length, width)
    out_rows = lax.dynamic_slice_in_dim(full_out, me * span, span, 0)
    heads_grad = jnp.einsum("te,de->td", branch_all, out_rows, preferred_element_type=f32).astype(bf)
    out_term = jnp.einsum("td,te->de", heads_out, branch_all, preferred_element_type=f32).astype(bf)
    query_back, key_back, value_back = attend_back(
        queries, keys, values, heads_grad, heads_out, log_totals, heads, block, scale
    )
    proj_grad, gain_terms = heads_back(
        query_back, key_back, value_back, proj, factors, head_gains, tables, n, width, 6
    )
    normed_part = jnp.einsum("te,de->td", proj_grad, w_heads, preferred_element_type=f32).astype(bf)
    head_term = jnp.einsum("td,te->de", normed, proj_grad, preferred_element_type=f32).astype(bf)
    head_term = head_term.reshape(n, groups, part, 3 * span).swapaxes(0, 1)
    block_out = mid + sum(piece.astype(f32) for piece in [ffn_keep[0], ffn_got[0]] + ffn_pieces)
    down_sum, gate_sum, up_sum = scattered
    normed_grad, *head_sums, out_sum, down_sum, gate_sum = reduce_sides(
        normed_part.reshape(n, rows, width),
        head_term.reshape(groups, n * part, 3 * span),
        out_term.reshape(groups, part, width),
        down_sum, gate_sum, n, groups, 8, 7,
    )
    up_sum, normed_grad = barrier((up_sum, normed_grad))
    up_sum = widen(up_sum)
    input_back, attn_gain_term = norm_backward(inputs, inverse_norm(inputs), gain_attn, normed_grad)
    tokens_grad = mid_grad + input_back
    by_span = lambda v: v.reshape(n, 1, span)
    sent_gains = jnp.concatenate([by_span(attn_gain_term), by_span(ffn_gain_term)], axis=1)
    sent_gains = jnp.pad(sent_gains, ((0, 0), (0, 6), (0, 0)))
    gain_sums = sum_gains(sent_gains, gain_terms, n, groups, 8)
    gain_sums = lax.dynamic_slice_in_dim(gain_sums, lax.axis_index("fsdp") * part, part, 1)
    return (
        block_out.astype(bf).reshape(tokens.shape),
        tokens_grad.reshape(tokens.shape),
        gain_sums[0],
        gain_sums[2],
        gain_sums[3],
        gain_sums[1],
        head_sums[0],
        head_sums[1],
        head_sums[2],
        out_sum,
        gate_sum,
        up_sum,
        down_sum,
    )


def solution(mesh):
    rows3 = P("fsdp", "seq", None)
    both = P(("seq", "fsdp"))
    both2 = P(("seq", "fsdp"), None)
    placed = (rows3,) * 4 + (P("fsdp"),) * 4 + (P("fsdp", None),) * 4 + (rows3,) * 3
    return jax.shard_map(
        local,
        mesh=mesh,
        in_specs=placed,
        out_specs=(rows3,) * 2 + (both,) * 4 + (both2,) * 4 + (rows3,) * 3,
        check_vma=False,
    )
```

```python
import functools
import jax
import jax.numpy as jnp
from jax import lax
from jax.experimental import pallas as pl
from jax.experimental.pallas import tpu as pltpu
from jax.sharding import PartitionSpec as P


MESH = pl.DeviceIdType.MESH
ANY = pl.ANY
H = 16
epsilon = 1e-05


def work(us):
    return pl.CostEstimate(flops=int(us * 6e8), bytes_accessed=0, transcendentals=0)


def greet(peers):
    barrier = pltpu.get_barrier_semaphore()
    for peer in peers:
        pl.semaphore_signal(barrier, inc=1, device_id={"seq": peer}, device_id_type=MESH)
    pl.semaphore_wait(barrier, len(peers))


def push(src, dst, send, recv, peer):
    return pltpu.make_async_remote_copy(
        src_ref=src, dst_ref=dst, send_sem=send, recv_sem=recv,
        device_id={"seq": peer}, device_id_type=MESH)


def gather_kernel(n, pieces, by_index, own, out, send_sem, recv_sem, copy_sem):
    pair = 2
    lines = n // pair
    me = lax.axis_index("seq")
    a, b = me // pair, me % pair
    column = [((a + k) % lines) * pair + b for k in range(1, lines)]
    across = a * pair + (1 - b)
    greet(column + [across])
    rows = own.shape[0] // pieces
    if by_index:
        here = [((a + lines - k) % lines) * pair + b for k in range(lines)]
        there = [((a + lines - k) % lines) * pair + 1 - b for k in range(lines)]
        sent = [me] * lines
        relayed = here
    else:
        here, there = list(range(lines)), list(range(lines, n))
        sent = here
        relayed = there
    local = pltpu.make_async_copy(own, out.at[here[0]], copy_sem)
    local.start()

    def piece(p):
        return pl.ds(p * rows, rows)

    sends = []
    for p in range(pieces):
        for k in range(lines):
            peer = across if k == 0 else column[k - 1]
            place = relayed[0] if k == 0 else sent[k]
            copy = push(own.at[piece(p)], out.at[place, piece(p)], send_sem.at[k, p], recv_sem.at[k, p], peer)
            copy.start()
            sends.append(copy)
    relays = []
    for p in range(pieces):
        for k in range(1, lines):
            push(own.at[piece(p)], out.at[here[k], piece(p)], send_sem.at[k, p], recv_sem.at[k, p], across).wait_recv()
            slot = lines + k - 1
            copy = push(
                out.at[here[k], piece(p)], out.at[relayed[k], piece(p)], send_sem.at[slot, p], recv_sem.at[slot, p], across
            )
            copy.start()
            relays.append(copy)
    for p in range(pieces):
        push(own.at[piece(p)], out.at[there[0], piece(p)], send_sem.at[0, p], recv_sem.at[0, p], across).wait_recv()
    for copy in relays:
        copy.wait_recv()
    for copy in sends + relays:
        copy.wait_send()
    local.wait()


def gather_rows(x, n, pieces, by_index, collective_id):
    slots = n // 2 + n // 2 - 1
    return pl.pallas_call(
        functools.partial(gather_kernel, n, pieces, by_index),
        out_shape=jax.ShapeDtypeStruct((n,) + x.shape, x.dtype),
        in_specs=[pl.BlockSpec(memory_space=pltpu.VMEM)],
        out_specs=pl.BlockSpec(memory_space=ANY),
        scratch_shapes=[
            pltpu.SemaphoreType.DMA((slots, pieces)),
            pltpu.SemaphoreType.DMA((slots, pieces)),
            pltpu.SemaphoreType.DMA,
        ],
        compiler_params=pltpu.CompilerParams(collective_id=collective_id, has_side_effects=True),
        cost_estimate=work(105),
        name="gather_rows",
    )(x)


def reduce_terms_kernel(
    n, pieces, tile, part, x, first, second, out, first_term, second_term,
    mine, got, sums, landed, x_buf, g_buf, o_buf, send_sem, recv_sem, load_sem, x_sem, g_sem, o_sem
):
    pair = 2
    lines = n // pair
    me = lax.axis_index("seq")
    a, b = me // pair, me % pair
    across = a * pair + (1 - b)
    greet([((a + lines - k) % lines) * pair + b for k in range(1, lines)] + [across])
    rows = out.shape[0] // pieces
    experts, _, width = x.shape
    tiles = width // tile
    jobs = experts * tiles
    terms = (first_term, second_term)

    def piece(p):
        return pl.ds(pl.multiple_of(p * rows, rows), rows)

    def first_copy(k, p):
        return push(part.at[lines + k, piece(p)], got.at[k, piece(p)], send_sem.at[k, p], recv_sem.at[k, p], across)

    def load(k, p):
        return pltpu.make_async_copy(part.at[k, piece(p)], mine.at[k, piece(p)], load_sem.at[k, p])

    def second_copy(k, p):
        peer = ((a + lines - k) % lines) * pair + b
        slot = lines + k - 1
        return push(sums.at[k - 1, piece(p)], landed.at[k - 1, piece(p)], send_sem.at[slot, p], recv_sem.at[slot, p], peer)

    def x_copy(j):
        cols = pl.ds(pl.multiple_of(j % tiles * tile, tile), tile)
        return pltpu.make_async_copy(x.at[j // tiles, :, cols], x_buf.at[j % 2], x_sem.at[j % 2])

    def g_copies(e):
        return [
            pltpu.make_async_copy(g.at[e], g_buf.at[e % 2, i], g_sem.at[e % 2, i]) for i, g in enumerate((first, second))
        ]

    def o_copies(j):
        place = pl.ds(pl.multiple_of(j % tiles * tile, tile), tile)
        return [
            pltpu.make_async_copy(o_buf.at[j % 2, i], o.at[j // tiles, place, :], o_sem.at[j % 2, i])
            for i, o in enumerate(terms)
        ]

    for k in list(range(1, lines)) + [0]:
        for p in range(pieces):
            first_copy(k, p).start()
            load(k, p).start()
    x_copy(0).start()
    for copy in g_copies(0):
        copy.start()

    def add(k, p):
        first_copy(k, p).wait_recv()
        load(k, p).wait()
        return mine[k, piece(p)].astype(jnp.float32) + got[k, piece(p)].astype(jnp.float32)

    def step(s):
        k, p = 1 + s // pieces, s % pieces
        sums[k - 1, piece(p)] = add(k, p).astype(jnp.bfloat16)
        second_copy(k, p).start()

    def job(j):
        @pl.when(j + 1 < jobs)
        def _():
            x_copy(j + 1).start()

        @pl.when(j % tiles == 0)
        def _():
            for copy in g_copies(j // tiles):
                copy.wait()

            @pl.when(j // tiles + 1 < experts)
            def _():
                for copy in g_copies(j // tiles + 1):
                    copy.start()

        @pl.when(j >= 2)
        def _():
            for copy in o_copies(j - 2):
                copy.wait()

        x_copy(j).wait()
        for i in range(2):
            o_buf[j % 2, i] = down_rows(x_buf[j % 2], g_buf[j // tiles % 2, i]).astype(jnp.bfloat16)
        for copy in o_copies(j):
            copy.start()

    steps = (lines - 1) * pieces
    per = steps * 2 // jobs

    def both(t, _):
        for i in range(per):
            step(t * per + i)
            if i == 0:
                job(2 * t)
            if i == per - 1:
                job(2 * t + 1)
        return 0

    lax.fori_loop(0, jobs // 2, both, 0)
    for copy in o_copies(jobs - 2) + o_copies(jobs - 1):
        copy.wait()

    def finish(p, _):
        total = add(0, p)
        for k in range(1, lines):
            second_copy(k, p).wait_recv()
            total += landed[k - 1, piece(p)].astype(jnp.float32)
        out[piece(p), :] = total
        return 0

    lax.fori_loop(0, pieces, finish, 0)
    for p in range(pieces):
        for k in range(lines):
            first_copy(k, p).wait_send()
        for k in range(1, lines):
            second_copy(k, p).wait_send()


def reduce_terms(part, x, first, second, n, pieces, tile, collective_id):
    _, rows, width = part.shape
    experts, tokens, _ = x.shape
    hidden = first.shape[2]
    lines = n // 2
    slots = lines + lines - 1
    hbm = pl.BlockSpec(memory_space=ANY)
    term = jax.ShapeDtypeStruct((experts, width, hidden), jnp.bfloat16)
    return pl.pallas_call(
        functools.partial(reduce_terms_kernel, n, pieces, tile),
        out_shape=(jax.ShapeDtypeStruct((rows, width), jnp.float32), term, term),
        in_specs=[hbm] * 4,
        out_specs=[pl.BlockSpec(memory_space=pltpu.VMEM), hbm, hbm],
        scratch_shapes=[
            pltpu.VMEM((lines, rows, width), jnp.bfloat16),
            pltpu.VMEM((lines, rows, width), jnp.bfloat16),
            pltpu.VMEM((lines - 1, rows, width), jnp.bfloat16),
            pltpu.VMEM((lines - 1, rows, width), jnp.bfloat16),
            pltpu.VMEM((2, tokens, tile), jnp.bfloat16),
            pltpu.VMEM((2, 2, tokens, hidden), jnp.bfloat16),
            pltpu.VMEM((2, 2, tile, hidden), jnp.bfloat16),
            pltpu.SemaphoreType.DMA((slots, pieces)),
            pltpu.SemaphoreType.DMA((slots, pieces)),
            pltpu.SemaphoreType.DMA((lines, pieces)),
            pltpu.SemaphoreType.DMA((2,)),
            pltpu.SemaphoreType.DMA((2, 2)),
            pltpu.SemaphoreType.DMA((2, 2)),
        ],
        compiler_params=pltpu.CompilerParams(
            collective_id=collective_id, has_side_effects=True, vmem_limit_bytes=50 << 20
        ),
        cost_estimate=work(105),
        name="reduce_terms",
    )(part, x, first, second)


def reduce_sides_kernel(
    n, groups, pieces, part, head, wide, out, q_out, k_out, v_out, o_out,
    mine, got, sums, landed, head_own, head_land, wide_own, wide_land, head_sum, head_got,
    send_sem, recv_sem, load_sem, side_send, side_recv, side_load, swap_send, swap_recv
):
    pair = 2
    lines = n // pair
    me, group = lax.axis_index("seq"), lax.axis_index("fsdp")
    a, b = me // pair, me % pair
    across = a * pair + (1 - b)
    peers = [(me + k) % n for k in range(1, n)]
    mates = [(group + k) % groups for k in range(1, groups)]
    barrier = pltpu.get_barrier_semaphore()
    for peer in peers:
        pl.semaphore_signal(barrier, inc=1, device_id={"seq": peer}, device_id_type=MESH)
    for mate in mates:
        pl.semaphore_signal(barrier, inc=1, device_id={"fsdp": mate}, device_id_type=MESH)
    pl.semaphore_wait(barrier, n - 1 + groups - 1)
    rows = out.shape[0] // pieces

    def piece(p):
        return pl.ds(pl.multiple_of(p * rows, rows), rows)

    def first_copy(k, p):
        there = ((a + lines - k) % lines) * pair + 1 - b
        return push(part.at[there, piece(p)], got.at[k, piece(p)], send_sem.at[k, p], recv_sem.at[k, p], across)

    def load(k, p):
        here = ((a + lines - k) % lines) * pair + b
        return pltpu.make_async_copy(part.at[here, piece(p)], mine.at[k, piece(p)], load_sem.at[k, p])

    def second_copy(k, p):
        peer = ((a + lines - k) % lines) * pair + b
        slot = lines + k - 1
        return push(sums.at[k - 1, piece(p)], landed.at[k - 1, piece(p)], send_sem.at[slot, p], recv_sem.at[slot, p], peer)

    def side_copy(i, k):
        src, dst = ((head, head_land), (wide, wide_land))[i]
        return pltpu.make_async_remote_copy(
            src_ref=src.at[mates[k - 1]], dst_ref=dst.at[k - 1],
            send_sem=side_send.at[i, k - 1], recv_sem=side_recv.at[i, k - 1],
            device_id={"fsdp": mates[k - 1]}, device_id_type=MESH)

    for k in list(range(1, lines)) + [0]:
        for p in range(pieces):
            first_copy(k, p).start()
            load(k, p).start()
    own_copies = [
        pltpu.make_async_copy(head.at[group], head_own, side_load.at[0]),
        pltpu.make_async_copy(wide.at[group], wide_own, side_load.at[1]),
    ]
    for copy in own_copies:
        copy.start()
    for i in range(2):
        for k in range(1, groups):
            side_copy(i, k).start()

    def add(k, p):
        first_copy(k, p).wait_recv()
        load(k, p).wait()
        return mine[k, piece(p)].astype(jnp.float32) + got[k, piece(p)].astype(jnp.float32)

    def step(s, _):
        k, p = 1 + s // pieces, s % pieces
        sums[k - 1, piece(p)] = add(k, p).astype(jnp.bfloat16)
        second_copy(k, p).start()
        return 0

    lax.fori_loop(0, (lines - 1) * pieces, step, 0)

    for copy in own_copies:
        copy.wait()
    total, side = head_own[...].astype(jnp.float32), wide_own[...].astype(jnp.float32)
    for k in range(1, groups):
        side_copy(0, k).wait_recv()
        side_copy(1, k).wait_recv()
        total = total + head_land[k - 1].astype(jnp.float32)
        side = side + wide_land[k - 1].astype(jnp.float32)
    o_out[...] = side
    head_sum[...] = total.astype(jnp.bfloat16)
    count = o_out.shape[0]

    def swap(k):
        place = pl.ds(pl.multiple_of(peers[k - 1] * count, count), count)
        return push(head_sum.at[place], head_got.at[me], swap_send.at[k - 1], swap_recv.at[k - 1], peers[k - 1])

    for k in range(1, n):
        swap(k).start()
    head_got[me] = head_sum[pl.ds(pl.multiple_of(me * count, count), count), :]

    def finish(p, _):
        total = add(0, p)
        for k in range(1, lines):
            second_copy(k, p).wait_recv()
            total += landed[k - 1, piece(p)].astype(jnp.float32)
        out[piece(p), :] = total
        return 0

    lax.fori_loop(0, pieces, finish, 0)
    for k in range(1, n):
        swap(k).wait_recv()
    span = head.shape[2] // 3
    for s in range(n):
        for i, o in enumerate((q_out, k_out, v_out)):
            o[:, s * span : (s + 1) * span] = head_got[s, :, i * span : (i + 1) * span].astype(jnp.float32)
    for p in range(pieces):
        for k in range(lines):
            first_copy(k, p).wait_send()
        for k in range(1, lines):
            second_copy(k, p).wait_send()
    for i in range(2):
        for k in range(1, groups):
            side_copy(i, k).wait_send()
    for k in range(1, n):
        swap(k).wait_send()


def reduce_sides(part, head, wide, n, groups, pieces, collective_id):
    _, rows, width = part.shape
    _, blocks, outs = head.shape
    count = blocks // n
    lines = n // 2
    slots = lines + lines - 1
    hbm = pl.BlockSpec(memory_space=ANY)
    vmem = pl.BlockSpec(memory_space=pltpu.VMEM)
    f32, bf = jnp.float32, jnp.bfloat16
    grad = jax.ShapeDtypeStruct((count, n * outs // 3), f32)
    return pl.pallas_call(
        functools.partial(reduce_sides_kernel, n, groups, pieces),
        out_shape=(
            jax.ShapeDtypeStruct((rows, width), f32),
            grad, grad, grad,
            jax.ShapeDtypeStruct((count, wide.shape[2]), f32),
        ),
        in_specs=[hbm] * 3,
        out_specs=[vmem] * 5,
        scratch_shapes=[
            pltpu.VMEM((lines, rows, width), bf),
            pltpu.VMEM((lines, rows, width), bf),
            pltpu.VMEM((lines - 1, rows, width), bf),
            pltpu.VMEM((lines - 1, rows, width), bf),
            pltpu.VMEM((blocks, outs), bf),
            pltpu.VMEM((groups - 1, blocks, outs), bf),
            pltpu.VMEM((count, wide.shape[2]), bf),
            pltpu.VMEM((groups - 1, count, wide.shape[2]), bf),
            pltpu.VMEM((blocks, outs), bf),
            pltpu.VMEM((n, count, outs), bf),
            pltpu.SemaphoreType.DMA((slots, pieces)),
            pltpu.SemaphoreType.DMA((slots, pieces)),
            pltpu.SemaphoreType.DMA((lines, pieces)),
            pltpu.SemaphoreType.DMA((2, groups - 1)),
            pltpu.SemaphoreType.DMA((2, groups - 1)),
            pltpu.SemaphoreType.DMA((2,)),
            pltpu.SemaphoreType.DMA((n - 1,)),
            pltpu.SemaphoreType.DMA((n - 1,)),
        ],
        compiler_params=pltpu.CompilerParams(
            collective_id=collective_id, has_side_effects=True, vmem_limit_bytes=50 << 20
        ),
        cost_estimate=work(105),
        name="reduce_sides",
    )(part, head, wide)


def gains_kernel(n, groups, sent, own, out, taken, summed, landed, send_sem, recv_sem, side_send, side_recv):
    me, group = lax.axis_index("seq"), lax.axis_index("fsdp")
    barrier = pltpu.get_barrier_semaphore()
    peers = [(me + k) % n for k in range(1, n)]
    mates = [(group + k) % groups for k in range(1, groups)]
    for peer in peers:
        pl.semaphore_signal(barrier, inc=1, device_id={"seq": peer}, device_id_type=MESH)
    for mate in mates:
        pl.semaphore_signal(barrier, inc=1, device_id={"fsdp": mate}, device_id_type=MESH)
    pl.semaphore_wait(barrier, n - 1 + groups - 1)
    copies = []
    for k in range(1, n):
        copy = push(sent.at[peers[k - 1]], taken.at[k - 1], send_sem.at[k - 1], recv_sem.at[k - 1], peers[k - 1])
        copy.start()
        copies.append(copy)
    total = sent[me] + own[...]
    for k in range(1, n):
        copies[k - 1].wait_recv()
        total = total + taken[k - 1]
    summed[...] = total
    sides = []
    for k in range(1, groups):
        side = pltpu.make_async_remote_copy(
            src_ref=summed, dst_ref=landed.at[k - 1], send_sem=side_send.at[k - 1], recv_sem=side_recv.at[k - 1],
            device_id={"fsdp": mates[k - 1]}, device_id_type=MESH)
        side.start()
        sides.append(side)
    for k in range(1, groups):
        sides[k - 1].wait_recv()
        total = total + landed[k - 1]
    out[...] = total
    for copy in copies + sides:
        copy.wait_send()


def sum_gains(sent, own, n, groups, collective_id):
    shape = own.shape
    return pl.pallas_call(
        functools.partial(gains_kernel, n, groups),
        out_shape=jax.ShapeDtypeStruct(shape, own.dtype),
        in_specs=[pl.BlockSpec(memory_space=pltpu.VMEM)] * 2,
        out_specs=pl.BlockSpec(memory_space=pltpu.VMEM),
        scratch_shapes=[
            pltpu.VMEM((n - 1,) + shape, own.dtype),
            pltpu.VMEM(shape, own.dtype),
            pltpu.VMEM((groups - 1,) + shape, own.dtype),
            pltpu.SemaphoreType.DMA((n - 1,)),
            pltpu.SemaphoreType.DMA((n - 1,)),
            pltpu.SemaphoreType.DMA((groups - 1,)),
            pltpu.SemaphoreType.DMA((groups - 1,)),
        ],
        compiler_params=pltpu.CompilerParams(collective_id=collective_id, has_side_effects=True),
        cost_estimate=work(10),
        name="sum_gains",
    )(sent, own)


def slots_of(w, experts, capacity):
    tokens = w.shape[1]
    taken = w > 0
    before = lax.broadcasted_iota(jnp.int32, (tokens, tokens), 0) <= lax.broadcasted_iota(jnp.int32, (tokens, tokens), 1)
    rank = jnp.dot(
        taken.astype(jnp.float32).astype(jnp.bfloat16), before.astype(jnp.float32).astype(jnp.bfloat16),
        preferred_element_type=jnp.float32,
    )
    rank = jnp.where(taken, rank - 1.0, -1.0)
    slot = lax.broadcasted_iota(jnp.int32, (capacity, tokens), 0).astype(jnp.float32)
    hits, weights = [], []
    for e in range(experts):
        hit = slot == rank[e : e + 1, :]
        hits.append(hit.astype(jnp.float32).astype(jnp.bfloat16))
        weights.append(jnp.sum(jnp.where(hit, w[e : e + 1, :], 0.0), axis=1, keepdims=True))
    return jnp.concatenate(hits, axis=0), weights


def place_kernel(experts, w_ref, x_ref, o_ref, s_ref):
    capacity = o_ref.shape[1]
    hits, weights = slots_of(w_ref[0], experts, capacity)
    out = jnp.dot(hits, x_ref[0], preferred_element_type=jnp.float32)
    for e in range(experts):
        o_ref[e] = out[e * capacity : (e + 1) * capacity].astype(jnp.bfloat16)
        s_ref[e] = weights[e]


def place(weights, x, experts, capacity):
    n, tokens, width = x.shape
    return pl.pallas_call(
        functools.partial(place_kernel, experts),
        grid=(n,),
        out_shape=(
            jax.ShapeDtypeStruct((experts, n * capacity, width), x.dtype),
            jax.ShapeDtypeStruct((experts, n * capacity, 1), jnp.float32),
        ),
        in_specs=[
            pl.BlockSpec((1, 8, tokens), lambda c: (c, 0, 0)),
            pl.BlockSpec((1, tokens, width), lambda c: (c, 0, 0)),
        ],
        out_specs=[
            pl.BlockSpec((experts, capacity, width), lambda c: (0, c, 0)),
            pl.BlockSpec((experts, capacity, 1), lambda c: (0, c, 0)),
        ],
        cost_estimate=work(10),
        name="place",
    )(weights, x)


def place_weighted_kernel(experts, w_ref, *refs):
    pieces, o_ref, x_buf = refs[:-2], refs[-2], refs[-1]
    capacity = o_ref.shape[1]
    half = pieces[0].shape[0]
    for k in range(len(pieces) // 2):

        @pl.when(pl.program_id(0) == k)
        def _():
            x_buf[:half] = pieces[2 * k][...]
            x_buf[half:] = pieces[2 * k + 1][...]

    hits, weights = slots_of(w_ref[0], experts, capacity)
    out = jnp.dot(hits, x_buf[...], preferred_element_type=jnp.float32)
    for e in range(experts):
        o_ref[e] = (out[e * capacity : (e + 1) * capacity] * weights[e]).astype(jnp.bfloat16)


def place_weighted(weights, pieces, experts, capacity):
    n, _, tokens = weights.shape
    half, width = pieces[0].shape
    return pl.pallas_call(
        functools.partial(place_weighted_kernel, experts),
        grid=(n,),
        out_shape=jax.ShapeDtypeStruct((experts, n * capacity, width), pieces[0].dtype),
        in_specs=[pl.BlockSpec((1, 8, tokens), lambda c: (c, 0, 0))]
        + [pl.BlockSpec((half, width), lambda c: (0, 0), pipeline_mode=pl.Buffered(1))] * len(pieces),
        out_specs=pl.BlockSpec((experts, capacity, width), lambda c: (0, c, 0)),
        scratch_shapes=[pltpu.VMEM((2 * half, width), pieces[0].dtype)],
        cost_estimate=work(12),
        name="place_weighted",
    )(weights, *pieces)


def unplace_kernel(experts, w_ref, y_ref, o_ref):
    capacity, width = y_ref.shape[1:]
    hits, _ = slots_of(w_ref[0], experts, capacity)
    o_ref[0] = down_rows(hits, y_ref[...].reshape(experts * capacity, width)).astype(o_ref.dtype)


def unplace(weights, y, capacity):
    n, _, tokens = weights.shape
    experts, _, width = y.shape
    return pl.pallas_call(
        functools.partial(unplace_kernel, experts),
        grid=(n,),
        out_shape=jax.ShapeDtypeStruct((n, tokens, width), y.dtype),
        in_specs=[
            pl.BlockSpec((1, 8, tokens), lambda c: (c, 0, 0)),
            pl.BlockSpec((experts, capacity, width), lambda c: (0, c, 0)),
        ],
        out_specs=pl.BlockSpec((1, tokens, width), lambda c: (c, 0, 0)),
        cost_estimate=work(10),
        name="unplace",
    )(weights, y)


def widen_kernel(x_ref, o_ref):
    for e in range(x_ref.shape[0]):
        o_ref[:, e, :] = x_ref[e].astype(jnp.float32)


def widen(x):
    experts, rows, columns = x.shape
    step = min(128, rows)
    return pl.pallas_call(
        widen_kernel,
        grid=(rows // step,),
        out_shape=jax.ShapeDtypeStruct((rows, experts, columns), jnp.float32),
        in_specs=[pl.BlockSpec((experts, step, columns), lambda i: (0, i, 0))],
        out_specs=pl.BlockSpec((step, experts, columns), lambda i: (i, 0, 0)),
        cost_estimate=work(5),
        name="widen",
    )(x)


def masked(block):
    keys = lax.broadcasted_iota(jnp.int32, (block, block), 0)
    rows = lax.broadcasted_iota(jnp.int32, (block, block), 1)
    return keys <= rows


def across_lanes(a, b):
    return lax.dot_general(a, b, (((1,), (1,)), ((), ())), preferred_element_type=jnp.float32)


def down_rows(a, b):
    return lax.dot_general(a, b, (((0,), (0,)), ((), ())), preferred_element_type=jnp.float32)


LOG2E = 1.4426950408889634


def attend_kernel(block, scale, q_ref, k_ref, v_ref, o_ref, lse_ref, s_ref, acc_ref):
    length, _ = q_ref.shape

    def rows(i):
        return pl.ds(pl.multiple_of(i * block, block), block)

    def one_block(i, _):
        q = q_ref[rows(i), :]
        diag = across_lanes(k_ref[rows(i), :], q) * (scale * LOG2E)
        diag = jnp.where(masked(block), diag, -1e30)
        s_ref[rows(i), :] = diag
        peak = jnp.max(diag, axis=0, keepdims=True)

        def score(j, peak):
            s = across_lanes(k_ref[rows(j), :], q) * (scale * LOG2E)
            s_ref[rows(j), :] = s
            return jnp.maximum(peak, jnp.max(s, axis=0, keepdims=True))

        peak = lax.fori_loop(0, i, score, peak)
        acc_ref[...] = jnp.zeros_like(acc_ref)

        def weigh(j, total):
            p = jnp.exp2(s_ref[rows(j), :] - peak)
            acc_ref[...] += down_rows(v_ref[rows(j), :], p.astype(jnp.bfloat16))
            return total + jnp.sum(p, axis=0, keepdims=True)

        total = lax.fori_loop(0, i + 1, weigh, jnp.zeros_like(peak))
        o_ref[rows(i), :] = (acc_ref[...] / total).T.astype(o_ref.dtype)
        lse_ref[0, :, rows(i)] = peak + jnp.log2(total)
        return 0

    lax.fori_loop(0, length // block, one_block, 0)


def attend(q, k, v, heads, block, scale):
    length, width = q.shape
    dim = width // heads
    spec = pl.BlockSpec((length, dim), lambda h: (0, h))
    return pl.pallas_call(
        functools.partial(attend_kernel, block, scale),
        grid=(heads,),
        out_shape=(
            jax.ShapeDtypeStruct(q.shape, q.dtype),
            jax.ShapeDtypeStruct((heads, 1, length), jnp.float32),
        ),
        in_specs=[spec] * 3,
        out_specs=[spec, pl.BlockSpec((1, 1, length), lambda h: (h, 0, 0))],
        scratch_shapes=[
            pltpu.VMEM((length, block), jnp.float32),
            pltpu.VMEM((dim, block), jnp.float32),
        ],
        cost_estimate=work(25),
        name="attend",
    )(q, k, v)


def attend_back_kernel(
    block, scale, q_ref, k_ref, v_ref, g_ref, o_ref, lse_ref, dq_ref, dk_ref, dv_ref, dk_acc, dv_acc, dq_acc
):
    length, dim = q_ref.shape
    dk_acc[...] = jnp.zeros_like(dk_acc)
    dv_acc[...] = jnp.zeros_like(dv_acc)

    def rows(i):
        return pl.ds(pl.multiple_of(i * block, block), block)

    def one_block(i, _):
        q, g = q_ref[rows(i), :], g_ref[rows(i), :]
        lse = lse_ref[0, :, rows(i)]
        products = g.astype(jnp.float32) * o_ref[rows(i), :].astype(jnp.float32)
        shift = lax.dot_general(
            jnp.ones((8, dim), jnp.float32), products, (((1,), (1,)), ((), ())),
            precision=lax.Precision.HIGHEST, preferred_element_type=jnp.float32,
        )[:1]

        def pair(j, keep):
            k, v = k_ref[rows(j), :], v_ref[rows(j), :]
            p = jnp.exp2(across_lanes(k, q) * (scale * LOG2E) - lse)
            if keep is not None:
                p = jnp.where(keep, p, 0.0)
            ds = (p * (across_lanes(v, g) - shift) * scale).astype(jnp.bfloat16)
            dv_acc[rows(j), :] += jnp.dot(p.astype(jnp.bfloat16), g, preferred_element_type=jnp.float32)
            dk_acc[rows(j), :] += jnp.dot(ds, q, preferred_element_type=jnp.float32)
            dq_acc[...] += down_rows(k, ds)

        dq_acc[...] = jnp.zeros_like(dq_acc)
        pair(i, masked(block))

        def body(j, _):
            pair(j, None)
            return 0

        lax.fori_loop(0, i, body, 0)
        dq_ref[rows(i), :] = dq_acc[...].T.astype(dq_ref.dtype)
        return 0

    lax.fori_loop(0, length // block, one_block, 0)
    dk_ref[...] = dk_acc[...].astype(dk_ref.dtype)
    dv_ref[...] = dv_acc[...].astype(dv_ref.dtype)


def attend_back(q, k, v, g, o, lse, heads, block, scale):
    length, width = q.shape
    dim = width // heads
    spec = pl.BlockSpec((length, dim), lambda h: (0, h))
    return pl.pallas_call(
        functools.partial(attend_back_kernel, block, scale),
        grid=(heads,),
        out_shape=(jax.ShapeDtypeStruct(q.shape, q.dtype),) * 3,
        in_specs=[spec] * 5 + [pl.BlockSpec((1, 1, length), lambda h: (h, 0, 0))],
        out_specs=[spec] * 3,
        scratch_shapes=[
            pltpu.VMEM((length, dim), jnp.float32),
            pltpu.VMEM((length, dim), jnp.float32),
            pltpu.VMEM((dim, block), jnp.float32),
        ],
        cost_estimate=work(60),
        name="attend_back",
    )(q, k, v, g, o, lse)


def project_kernel(
    n, groups, pieces, own, w_query, w_key, w_value, gain_own,
    normed, proj, squares, w_ref, gains, held, send_sem, recv_sem, side_send, side_recv, copy_sem
):
    pair = 2
    lines = n // pair
    me, group = lax.axis_index("seq"), lax.axis_index("fsdp")
    a, b = me // pair, me % pair
    column = [((a + k) % lines) * pair + b for k in range(1, lines)]
    back = [((a + lines - k) % lines) * pair + b for k in range(1, lines)]
    across = a * pair + (1 - b)
    mates = [(group + k) % groups for k in range(1, groups)]
    barrier = pltpu.get_barrier_semaphore()
    for peer in column + [across]:
        pl.semaphore_signal(barrier, inc=1, device_id={"seq": peer}, device_id_type=MESH)
    for mate in mates:
        pl.semaphore_signal(barrier, inc=1, device_id={"fsdp": mate}, device_id_type=MESH)
    pl.semaphore_wait(barrier, lines + groups - 1)
    rows, _ = own.shape
    step = rows // pieces
    span = w_ref.shape[1] // 3
    shard = w_query.shape[0]

    def piece(p):
        return pl.ds(p * step, step)

    sends = []
    for p in range(pieces):
        for k in range(lines):
            peer = across if k == 0 else column[k - 1]
            copy = push(own.at[piece(p)], held.at[me, piece(p)], send_sem.at[k, p], recv_sem.at[k, p], peer)
            copy.start()
            sends.append(copy)

    shard_rows = pl.ds(pl.multiple_of(group * shard, shard), shard)
    mine = pl.ds(pl.multiple_of(me * span, span), span)
    blocks = [
        (w.at[:, mine], w_ref.at[shard_rows, part * span : (part + 1) * span])
        for part, w in enumerate((w_query, w_key, w_value))
    ]
    blocks.append((gain_own, gains.at[:, shard_rows]))
    locals_, sides = [], []

    def side_copy(i, src, dst, slot, mate):
        return pltpu.make_async_remote_copy(
            src_ref=src, dst_ref=dst, send_sem=side_send.at[i, slot], recv_sem=side_recv.at[i, slot],
            device_id={"fsdp": mate}, device_id_type=MESH)

    def side_block(i, g):
        place = pl.ds(pl.multiple_of(g * shard, shard), shard)
        return gains.at[:, place] if i == 3 else w_ref.at[place, i * span : (i + 1) * span]

    chips = groups // 2
    partner = group // 2 * 2 + 1 - group % 2
    alike = [(group + 2 * k) % groups for k in range(1, chips)]
    behind = [(group + groups - 2 * k) % groups for k in range(1, chips)]
    for i, (src, dst) in enumerate(blocks):
        for k in range(chips):
            side = side_copy(i, src, dst, k, partner if k == 0 else alike[k - 1])
            side.start()
            sides.append(side)
        local = pltpu.make_async_copy(src, dst, copy_sem.at[i])
        local.start()
        locals_.append(local)
    for k in range(1, chips):
        for i in range(4):
            block = side_block(i, behind[k - 1])
            side_copy(i, block, block, k, partner).wait_recv()
            side = side_copy(i, block, block, chips + k - 1, partner)
            side.start()
            sides.append(side)

    def project(src, chunk):
        x = chunk[...].astype(jnp.float32)
        factor = lax.rsqrt(jnp.mean(x * x, axis=-1, keepdims=True) + epsilon)
        place = pl.ds(pl.multiple_of(src * rows, rows), rows)
        normed[place, :] = (x * factor * gains[0:1, :]).astype(jnp.bfloat16)
        for part in range(3):
            cols = slice(part * span, (part + 1) * span)
            out = jnp.dot(normed[place, :], w_ref[:, cols], preferred_element_type=jnp.float32)
            proj[place, cols] = out
            if part < 2:
                sums = lax.dot_general(
                    jnp.ones((8, span), jnp.float32), out * out, (((1,), (1,)), ((), ())),
                    precision=lax.Precision.HIGHEST, preferred_element_type=jnp.float32,
                )
                squares[pl.ds(part * n + src, 1), :] = sums[:1]

    relays = []
    for p in range(pieces):
        for k in range(1, lines):
            src = back[k - 1]
            push(own.at[piece(p)], held.at[src, piece(p)], send_sem.at[k, p], recv_sem.at[k, p], across).wait_recv()
            slot = lines + k - 1
            copy = push(held.at[src, piece(p)], held.at[src, piece(p)], send_sem.at[slot, p], recv_sem.at[slot, p], across)
            copy.start()
            relays.append(copy)
    for copy in locals_:
        copy.wait()
    for i in range(4):
        for k in [0] + list(range(chips, 2 * chips - 1)):
            side_copy(i, blocks[i][0], blocks[i][1], k, partner).wait_recv()
    project(me, own)
    for p in range(pieces):
        push(own.at[piece(p)], held.at[across, piece(p)], send_sem.at[0, p], recv_sem.at[0, p], across).wait_recv()
    project(across, held.at[across])
    for k in range(1, lines):
        project(back[k - 1], held.at[back[k - 1]])
    for k in range(1, lines):
        for p in range(pieces):
            relays[p * (lines - 1) + k - 1].wait_recv()
        src = ((a + lines - k) % lines) * pair + 1 - b
        project(src, held.at[src])
    for copy in sends + relays + sides:
        copy.wait_send()


def project_rows(x, w_query, w_key, w_value, gains, n, groups, pieces, collective_id):
    rows, width = x.shape
    span = w_query.shape[1] // n
    slots = n // 2 + n // 2 - 1
    vmem = pl.BlockSpec(memory_space=pltpu.VMEM)
    hbm = pl.BlockSpec(memory_space=ANY)
    return pl.pallas_call(
        functools.partial(project_kernel, n, groups, pieces),
        out_shape=(
            jax.ShapeDtypeStruct((n * rows, width), jnp.bfloat16),
            jax.ShapeDtypeStruct((n * rows, 3 * span), jnp.float32),
            jax.ShapeDtypeStruct((2 * n, rows), jnp.float32),
            jax.ShapeDtypeStruct((width, 3 * span), jnp.bfloat16),
            jax.ShapeDtypeStruct((8, width), jnp.float32),
        ),
        in_specs=[vmem, hbm, hbm, hbm, vmem],
        out_specs=[vmem] * 5,
        scratch_shapes=[
            pltpu.VMEM((n, rows, width), jnp.bfloat16),
            pltpu.SemaphoreType.DMA((slots, pieces)),
            pltpu.SemaphoreType.DMA((slots, pieces)),
            pltpu.SemaphoreType.DMA((4, groups - 1)),
            pltpu.SemaphoreType.DMA((4, groups - 1)),
            pltpu.SemaphoreType.DMA((4,)),
        ],
        compiler_params=pltpu.CompilerParams(
            collective_id=collective_id, has_side_effects=True, vmem_limit_bytes=50 << 20
        ),
        cost_estimate=work(110),
        name="project_rows",
    )(x, w_query, w_key, w_value, gains)


def as_columns(row, lanes):
    return jnp.broadcast_to(row, (lanes, row.shape[1])).T


def turn_tables(c, near_cos, near_sin, far_cos, far_sin):
    far_c, far_s = far_cos[pl.ds(c, 1), :], far_sin[pl.ds(c, 1), :]
    cosine = near_cos[...] * far_c - near_sin[...] * far_s
    sine = near_sin[...] * far_c + near_cos[...] * far_s
    first = lax.broadcasted_iota(jnp.int32, sine.shape, 1) < sine.shape[1] // 2
    return cosine, jnp.where(first, -sine, sine)


def add_over_seq(n, own, landed, send_sem, recv_sem, peers):
    copies = []
    for k in range(1, n):
        copy = push(own, landed.at[k - 1], send_sem.at[k - 1], recv_sem.at[k - 1], peers[k - 1])
        copy.start()
        copies.append(copy)
    return copies


def rotate_kernel(
    n, full, squares, sent, proj, gains, near_cos, near_sin, far_cos, far_sin,
    queries, keys, values, factors, taken, landed, send_sem, recv_sem, copy_sem
):
    me = lax.axis_index("seq")
    peers = [(me + k) % n for k in range(1, n)]
    greet(peers)
    local = pltpu.make_async_copy(sent.at[me], taken.at[me], copy_sem)
    local.start()
    copies = add_over_seq(n, squares, landed, send_sem.at[0], recv_sem.at[0], peers)
    swaps = []
    for k in range(1, n):
        swap = push(sent.at[peers[k - 1]], taken.at[me], send_sem.at[1, k - 1], recv_sem.at[1, k - 1], peers[k - 1])
        swap.start()
        swaps.append(swap)
    span = queries.shape[1]
    rows = squares.shape[1]
    lanes = near_cos.shape[1]
    total = squares[...]
    for k in range(1, n):
        copies[k - 1].wait_recv()
        total = total + landed[k - 1]
    factors[...] = lax.rsqrt(total / full + epsilon)

    def chunk(c, _):
        place = pl.ds(pl.multiple_of(c * rows, rows), rows)
        cosine, sine = turn_tables(c, near_cos, near_sin, far_cos, far_sin)
        for part, out in ((0, queries), (1, keys)):
            factor = as_columns(factors[pl.ds(part * n + c, 1), :], lanes)
            for h in range(span // lanes):
                cols = slice(part * span + h * lanes, part * span + (h + 1) * lanes)
                x = proj[place, cols] * factor * gains[part : part + 1, h * lanes : (h + 1) * lanes]
                turned = x * cosine + pltpu.roll(x, lanes // 2, 1) * sine
                out[place, h * lanes : (h + 1) * lanes] = turned.astype(jnp.bfloat16)
        values[place, :] = proj[place, 2 * span :].astype(jnp.bfloat16)
        return 0

    lax.fori_loop(0, n, chunk, 0)
    for copy in copies:
        copy.wait_send()
    for swap in swaps:
        swap.wait()
    local.wait()


def rotate_rows(squares, sent, proj, gains, tables, n, full, collective_id):
    length, outs = proj.shape
    span = outs // 3
    vmem = pl.BlockSpec(memory_space=pltpu.VMEM)
    heads = jax.ShapeDtypeStruct((length, span), jnp.bfloat16)
    return pl.pallas_call(
        functools.partial(rotate_kernel, n, full),
        out_shape=(
            heads, heads, heads,
            jax.ShapeDtypeStruct(squares.shape, jnp.float32),
            jax.ShapeDtypeStruct(sent.shape, sent.dtype),
        ),
        in_specs=[vmem] * 8,
        out_specs=[vmem] * 5,
        scratch_shapes=[
            pltpu.VMEM((n - 1,) + squares.shape, jnp.float32),
            pltpu.SemaphoreType.DMA((2, n - 1)),
            pltpu.SemaphoreType.DMA((2, n - 1)),
            pltpu.SemaphoreType.DMA,
        ],
        compiler_params=pltpu.CompilerParams(
            collective_id=collective_id, has_side_effects=True, vmem_limit_bytes=40 << 20
        ),
        cost_estimate=work(15),
        name="rotate_rows",
    )(squares, sent, proj, gains, *tables)


def heads_back_kernel(
    n, full, dq, dk, dv, proj, factors, gains, near_cos, near_sin, far_cos, far_sin,
    grads, gain_grads, sums, landed, send_sem, recv_sem
):
    me = lax.axis_index("seq")
    peers = [(me + k) % n for k in range(1, n)]
    greet(peers)
    span = dq.shape[1]
    rows = sums.shape[1]
    lanes = near_cos.shape[1]
    count = span // lanes

    def parts(c, part, h, grad):
        place = pl.ds(pl.multiple_of(c * rows, rows), rows)
        cosine, sine = turn_tables(c, near_cos, near_sin, far_cos, far_sin)
        g = grad[place, h * lanes : (h + 1) * lanes].astype(jnp.float32)
        up = g * cosine + pltpu.roll(g * sine, lanes // 2, 1)
        factor = as_columns(factors[pl.ds(part * n + c, 1), :], lanes)
        cols = slice(part * span + h * lanes, part * span + (h + 1) * lanes)
        normal = proj[place, cols] * factor
        weighted = up * gains[part : part + 1, h * lanes : (h + 1) * lanes]
        return place, cols, up, factor, normal, weighted

    def first(c, _):
        for part, grad in ((0, dq), (1, dk)):
            products = 0.0
            for h in range(count):
                _, _, _, _, normal, weighted = parts(c, part, h, grad)
                products = products + weighted * normal
            total = lax.dot_general(
                jnp.ones((8, lanes), jnp.float32), products, (((1,), (1,)), ((), ())),
                precision=lax.Precision.HIGHEST, preferred_element_type=jnp.float32,
            )
            sums[pl.ds(part * n + c, 1), :] = total[:1]
        return 0

    lax.fori_loop(0, n, first, 0)
    copies = add_over_seq(n, sums, landed, send_sem, recv_sem, peers)
    gain_grads[...] = jnp.zeros_like(gain_grads)

    def gain_sum(c, _):
        for part, grad in ((0, dq), (1, dk)):
            for h in range(count):
                _, _, up, _, normal, _ = parts(c, part, h, grad)
                cell = (slice(part + 2, part + 3), slice(h * lanes, (h + 1) * lanes))
                gain_grads[cell] += jnp.sum(up * normal, axis=0, keepdims=True)
        place = pl.ds(pl.multiple_of(c * rows, rows), rows)
        grads[place, 2 * span :] = dv[place, :]
        return 0

    lax.fori_loop(0, n, gain_sum, 0)
    total = sums[...]
    for k in range(1, n):
        copies[k - 1].wait_recv()
        total = total + landed[k - 1]
    landed[0] = total / full

    def last(c, _):
        for part, grad in ((0, dq), (1, dk)):
            mean = as_columns(landed[0, pl.ds(part * n + c, 1), :], lanes)
            for h in range(count):
                place, cols, _, factor, normal, weighted = parts(c, part, h, grad)
                grads[place, cols] = (factor * (weighted - normal * mean)).astype(jnp.bfloat16)
        return 0

    lax.fori_loop(0, n, last, 0)
    for copy in copies:
        copy.wait_send()


def heads_back(dq, dk, dv, proj, factors, gains, tables, n, full, collective_id):
    length, span = dq.shape
    vmem = pl.BlockSpec(memory_space=pltpu.VMEM)
    return pl.pallas_call(
        functools.partial(heads_back_kernel, n, full),
        out_shape=(
            jax.ShapeDtypeStruct((length, 3 * span), jnp.bfloat16),
            jax.ShapeDtypeStruct((8, span), jnp.float32),
        ),
        in_specs=[vmem] * 10,
        out_specs=[vmem] * 2,
        scratch_shapes=[
            pltpu.VMEM(factors.shape, jnp.float32),
            pltpu.VMEM((n - 1,) + factors.shape, jnp.float32),
            pltpu.SemaphoreType.DMA((n - 1,)),
            pltpu.SemaphoreType.DMA((n - 1,)),
        ],
        compiler_params=pltpu.CompilerParams(
            collective_id=collective_id, has_side_effects=True, vmem_limit_bytes=40 << 20
        ),
        cost_estimate=work(20),
        name="heads_back",
    )(dq, dk, dv, proj, factors, gains, *tables)


def turn_parts(rows, n, dim):
    half = dim // 2
    frequency = jnp.power(10000.0, -2.0 * jnp.arange(half, dtype=jnp.float32) / dim)
    frequency = jnp.concatenate([frequency, frequency])[None]
    near = jnp.arange(rows, dtype=jnp.float32)[:, None] * frequency
    far = (rows * jnp.arange(n)).astype(jnp.float32)[:, None] * frequency
    return jnp.cos(near), jnp.sin(near), jnp.cos(far), jnp.sin(far)


def inverse_norm(values):
    return lax.rsqrt(jnp.mean(values * values, axis=-1, keepdims=True) + epsilon)


def norm_backward(values, factor, gain, upstream):
    normal = values * factor
    weighted = upstream * gain
    gain_term = jnp.sum(upstream * normal, axis=0)
    back = factor * (weighted - normal * jnp.mean(weighted * normal, axis=-1, keepdims=True))
    return (back, gain_term)


def across_pairs(lines, pair):
    return [(a * pair + b, a * pair + 1 - b) for a in range(lines) for b in range(pair)]


def along_lines(lines, pair, k):
    return [(a * pair + b, (a + k) % lines * pair + b) for a in range(lines) for b in range(pair)]


def by_place(v, n):
    lines = n // 2
    me = lax.axis_index("seq")
    a, b = me // 2, me % 2
    column = [((a + lines - k) % lines) * 2 for k in range(lines)]
    order = jnp.stack([c + b for c in column] + [c + 1 - b for c in column])
    return v[order]


def gather_column(x, n):
    lines = n // 2
    return [lax.ppermute(x, "seq", along_lines(lines, 2, k)) for k in range(1, lines)]


def gather_across(column, n):
    return [lax.ppermute(c, "seq", across_pairs(n // 2, 2)) for c in column]


def reduce_column(v, k, n):
    return lax.ppermute(v, "seq", along_lines(n // 2, 2, n // 2 - k))


def local(
    tokens, routes, route_weights, cotangent, attn_gain, query_gain, key_gain, ffn_gain,
    w_query, w_key, w_value, w_out, w_gate, w_up, w_down,
):
    n = lax.axis_size("seq")
    groups = lax.axis_size("fsdp")
    me = lax.axis_index("seq")
    width = tokens.shape[-1]
    own_tokens = tokens.reshape(-1, width)
    rows = own_tokens.shape[0]
    length = rows * n
    picks = routes.shape[-1]
    local_experts = w_gate.shape[1]
    experts = local_experts * n
    capacity = 3 * rows * picks // (2 * experts)
    head_dim = width // H
    heads = H // n
    span = heads * head_dim
    part = width // (n * groups)
    scale = head_dim ** (-0.5)
    bf, f32 = jnp.bfloat16, jnp.float32
    barrier = lax.optimization_barrier

    own_gains = jnp.stack([attn_gain, query_gain, key_gain, ffn_gain]).astype(f32)
    own_gains = jnp.pad(own_gains, ((0, 4), (0, 0)))
    full_out = lax.all_gather(w_out, "fsdp", axis=0, tiled=True)
    by_expert = lambda w: lax.all_gather(jnp.swapaxes(w, 0, 1), "fsdp", axis=1, tiled=True)
    full_gate = by_expert(w_gate)
    normed, proj, squares, w_heads, gains = project_rows(
        own_tokens, w_query, w_key, w_value, own_gains, n, groups, 8, 0
    )
    w_up, w_down, squares = barrier((w_up, w_down, squares))
    full_up, full_down = by_expert(w_up), by_expert(w_down)
    gain_attn, gain_ffn = gains[0], gains[3]
    head_gains = lax.dynamic_slice(gains, (1, me * span), (2, span))

    expert_ids = jnp.arange(experts, dtype=jnp.int32)
    named = routes.reshape(rows, picks)[None] == expert_ids[:, None, None]
    mixing = route_weights.reshape(rows, picks)[None]
    sent = jnp.sum(jnp.where(named, mixing, 0.0), axis=-1).reshape(n, local_experts, rows)
    tables = turn_parts(rows, n, head_dim)
    queries, keys, values, factors, weights = rotate_rows(
        squares, sent, proj, head_gains, tables, n, width, 1
    )
    block = min(512, length)
    heads_out, log_totals = attend(queries, keys, values, heads, block, scale)
    context = lax.all_to_all(heads_out, "seq", split_axis=0, concat_axis=1, tiled=True)
    inputs = own_tokens.astype(f32)
    mid = inputs + jnp.dot(context, full_out, preferred_element_type=f32)
    norm_two = inverse_norm(mid)
    ffn_in = (mid * norm_two * gain_ffn).astype(bf)

    ffn_all = gather_rows(ffn_in, n, 8, False, 2)
    cot_own, ffn_all = barrier((cotangent.reshape(rows, width), ffn_all))
    half = rows // 2
    cot_halves = [cot_own[:half], cot_own[half:]]
    cot_columns = [gather_column(cot_halves[0], n)]
    cot_columns.append(gather_column(cot_halves[1], n))
    cot_others = [gather_across([v], n) for v in cot_halves]
    weights = jnp.pad(by_place(weights, n), ((0, 0), (0, 8 - local_experts), (0, 0)))
    received, slot_weight = place(weights, ffn_all, local_experts, capacity)
    gate = jnp.einsum("erd,edf->erf", received, full_gate, preferred_element_type=f32)
    cot_others[0] += gather_across(cot_columns[0], n)
    cot_others[1] += gather_across(cot_columns[1], n)
    up_part = jnp.einsum("erd,edf->erf", received, full_up, preferred_element_type=f32)
    sigmoid_gate = jax.nn.sigmoid(gate)
    activated = gate * sigmoid_gate
    hidden = (activated * up_part).astype(bf)
    expert_out = jnp.einsum("erf,edf->erd", hidden, full_down, preferred_element_type=f32)
    expert_out = (expert_out * slot_weight).astype(bf)
    ffn_part = unplace(weights, expert_out, capacity)
    ffn_part, cot_others = barrier((ffn_part, cot_others))
    cot_pieces = [
        v for pair in zip(*(([h] + c + o) for h, c, o in zip(cot_halves, cot_columns, cot_others))) for v in pair
    ]
    lines = n // 2
    ffn_got = {k: gather_across([ffn_part[lines + k]], n)[0] for k in list(range(1, lines)) + [0]}
    ffn_keep = [barrier(ffn_part[k]) for k in range(lines)]
    ffn_sum = lambda k: (ffn_keep[k].astype(f32) + ffn_got[k].astype(f32)).astype(bf)

    out_grad = cotangent.reshape(rows, width).astype(f32)
    down_received = place_weighted(weights, cot_pieces, local_experts, capacity)
    hidden_grad = jnp.einsum("erd,edf->erf", down_received, full_down, preferred_element_type=f32)
    slope = sigmoid_gate * (1.0 + gate * (1.0 - sigmoid_gate))
    gate_grad = (hidden_grad * up_part * slope).astype(bf)
    up_grad = (hidden_grad * activated).astype(bf)
    early = list(range(1, lines - 1))
    gate_grad, up_grad, got = barrier((gate_grad, up_grad, [ffn_got[k] for k in early]))
    ffn_got.update(zip(early, got))
    ffn_pieces = [reduce_column(ffn_sum(k), k, n) for k in early]
    rows_gate = jnp.einsum("erf,edf->erd", gate_grad, full_gate, preferred_element_type=f32)
    rows_gate, ffn_got[lines - 1] = barrier((rows_gate, ffn_got[lines - 1]))
    ffn_pieces.append(reduce_column(ffn_sum(lines - 1), lines - 1, n))
    rows_up = jnp.einsum("erf,edf->erd", up_grad, full_up, preferred_element_type=f32)
    rows_grad = (rows_gate + rows_up).astype(bf)
    rows_part = unplace(weights, rows_grad, capacity)
    down_term = jnp.einsum("erd,erf->edf", down_received, hidden, preferred_element_type=f32)
    scatter = lambda v: lax.psum_scatter(v, "fsdp", scatter_dimension=1, tiled=True)
    rows_part, ffn_pieces, ffn_got[0] = barrier((rows_part, ffn_pieces, ffn_got[0]))
    ffn_in_grad, gate_term, up_term = reduce_terms(
        rows_part, received, gate_grad, up_grad, n, 8, 512, 4
    )
    scattered = [scatter(down_term.astype(bf))]
    scattered += [scatter(gate_term), scatter(up_term)]
    mid_back, ffn_gain_term = norm_backward(mid, norm_two, gain_ffn, ffn_in_grad)
    mid_grad = out_grad + mid_back
    branch_grad = mid_grad.astype(bf)

    branch_all = gather_rows(branch_grad, n, 8, True, 5).reshape(length, width)
    out_rows = lax.dynamic_slice_in_dim(full_out, me * span, span, 0)
    heads_grad = jnp.einsum("te,de->td", branch_all, out_rows, preferred_element_type=f32).astype(bf)
    out_term = jnp.einsum("td,te->de", heads_out, branch_all, preferred_element_type=f32).astype(bf)
    query_back, key_back, value_back = attend_back(
        queries, keys, values, heads_grad, heads_out, log_totals, heads, block, scale
    )
    proj_grad, gain_terms = heads_back(
        query_back, key_back, value_back, proj, factors, head_gains, tables, n, width, 6
    )
    normed_part = jnp.einsum("te,de->td", proj_grad, w_heads, preferred_element_type=f32).astype(bf)
    head_term = jnp.einsum("td,te->de", normed, proj_grad, preferred_element_type=f32).astype(bf)
    head_term = head_term.reshape(n, groups, part, 3 * span).swapaxes(0, 1)
    block_out = mid + sum(piece.astype(f32) for piece in [ffn_keep[0], ffn_got[0]] + ffn_pieces)
    normed_grad, *head_sums, out_sum = reduce_sides(
        normed_part.reshape(n, rows, width),
        head_term.reshape(groups, n * part, 3 * span),
        out_term.reshape(groups, part, width),
        n, groups, 8, 7,
    )
    scattered, normed_grad = barrier((scattered, normed_grad))
    down_sum, gate_sum, up_sum = [widen(v) for v in scattered]
    input_back, attn_gain_term = norm_backward(inputs, inverse_norm(inputs), gain_attn, normed_grad)
    tokens_grad = mid_grad + input_back
    by_span = lambda v: v.reshape(n, 1, span)
    sent_gains = jnp.concatenate([by_span(attn_gain_term), by_span(ffn_gain_term)], axis=1)
    sent_gains = jnp.pad(sent_gains, ((0, 0), (0, 6), (0, 0)))
    gain_sums = sum_gains(sent_gains, gain_terms, n, groups, 8)
    gain_sums = lax.dynamic_slice_in_dim(gain_sums, lax.axis_index("fsdp") * part, part, 1)
    return (
        block_out.astype(bf).reshape(tokens.shape),
        tokens_grad.reshape(tokens.shape),
        gain_sums[0],
        gain_sums[2],
        gain_sums[3],
        gain_sums[1],
        head_sums[0],
        head_sums[1],
        head_sums[2],
        out_sum,
        gate_sum,
        up_sum,
        down_sum,
    )


def solution(mesh):
    rows3 = P("fsdp", "seq", None)
    both = P(("seq", "fsdp"))
    both2 = P(("seq", "fsdp"), None)
    placed = (rows3,) * 4 + (P("fsdp"),) * 4 + (P("fsdp", None),) * 4 + (rows3,) * 3
    return jax.shard_map(
        local,
        mesh=mesh,
        in_specs=placed,
        out_specs=(rows3,) * 2 + (both,) * 4 + (both2,) * 4 + (rows3,) * 3,
        check_vma=False,
    )
```

```python
import functools
import jax
import jax.numpy as jnp
from jax import lax
from jax.experimental import pallas as pl
from jax.experimental.pallas import tpu as pltpu
from jax.sharding import PartitionSpec as P


MESH = pl.DeviceIdType.MESH
ANY = pl.ANY
H = 16
epsilon = 1e-05


def work(us):
    return pl.CostEstimate(flops=int(us * 6e8), bytes_accessed=0, transcendentals=0)


def greet(peers):
    barrier = pltpu.get_barrier_semaphore()
    for peer in peers:
        pl.semaphore_signal(barrier, inc=1, device_id={"seq": peer}, device_id_type=MESH)
    pl.semaphore_wait(barrier, len(peers))


def push(src, dst, send, recv, peer):
    return pltpu.make_async_remote_copy(
        src_ref=src, dst_ref=dst, send_sem=send, recv_sem=recv,
        device_id={"seq": peer}, device_id_type=MESH)


def gather_kernel(n, pieces, by_index, own, out, send_sem, recv_sem, copy_sem):
    pair = 2
    lines = n // pair
    me = lax.axis_index("seq")
    a, b = me // pair, me % pair
    column = [((a + k) % lines) * pair + b for k in range(1, lines)]
    across = a * pair + (1 - b)
    greet(column + [across])
    rows = own.shape[0] // pieces
    if by_index:
        here = [((a + lines - k) % lines) * pair + b for k in range(lines)]
        there = [((a + lines - k) % lines) * pair + 1 - b for k in range(lines)]
        sent = [me] * lines
        relayed = here
    else:
        here, there = list(range(lines)), list(range(lines, n))
        sent = here
        relayed = there
    local = pltpu.make_async_copy(own, out.at[here[0]], copy_sem)
    local.start()

    def piece(p):
        return pl.ds(p * rows, rows)

    sends = []
    for p in range(pieces):
        for k in range(lines):
            peer = across if k == 0 else column[k - 1]
            place = relayed[0] if k == 0 else sent[k]
            copy = push(own.at[piece(p)], out.at[place, piece(p)], send_sem.at[k, p], recv_sem.at[k, p], peer)
            copy.start()
            sends.append(copy)
    relays = []
    for p in range(pieces):
        for k in range(1, lines):
            push(own.at[piece(p)], out.at[here[k], piece(p)], send_sem.at[k, p], recv_sem.at[k, p], across).wait_recv()
            slot = lines + k - 1
            copy = push(
                out.at[here[k], piece(p)], out.at[relayed[k], piece(p)], send_sem.at[slot, p], recv_sem.at[slot, p], across
            )
            copy.start()
            relays.append(copy)
    for p in range(pieces):
        push(own.at[piece(p)], out.at[there[0], piece(p)], send_sem.at[0, p], recv_sem.at[0, p], across).wait_recv()
    for copy in relays:
        copy.wait_recv()
    for copy in sends + relays:
        copy.wait_send()
    local.wait()


def gather_rows(x, n, pieces, by_index, collective_id):
    slots = n // 2 + n // 2 - 1
    return pl.pallas_call(
        functools.partial(gather_kernel, n, pieces, by_index),
        out_shape=jax.ShapeDtypeStruct((n,) + x.shape, x.dtype),
        in_specs=[pl.BlockSpec(memory_space=pltpu.VMEM)],
        out_specs=pl.BlockSpec(memory_space=ANY),
        scratch_shapes=[
            pltpu.SemaphoreType.DMA((slots, pieces)),
            pltpu.SemaphoreType.DMA((slots, pieces)),
            pltpu.SemaphoreType.DMA,
        ],
        compiler_params=pltpu.CompilerParams(collective_id=collective_id, has_side_effects=True),
        cost_estimate=work(105),
        name="gather_rows",
    )(x)


def reduce_terms_kernel(
    n, pieces, tile, part, x, first, second, out, first_term, second_term,
    mine, got, sums, landed, x_buf, g_buf, o_buf, send_sem, recv_sem, load_sem, x_sem, g_sem, o_sem
):
    pair = 2
    lines = n // pair
    me = lax.axis_index("seq")
    a, b = me // pair, me % pair
    across = a * pair + (1 - b)
    greet([((a + lines - k) % lines) * pair + b for k in range(1, lines)] + [across])
    rows = out.shape[0] // pieces
    experts, _, width = x.shape
    tiles = width // tile
    jobs = experts * tiles
    terms = (first_term, second_term)

    def piece(p):
        return pl.ds(pl.multiple_of(p * rows, rows), rows)

    def first_copy(k, p):
        return push(part.at[lines + k, piece(p)], got.at[k, piece(p)], send_sem.at[k, p], recv_sem.at[k, p], across)

    def load(k, p):
        return pltpu.make_async_copy(part.at[k, piece(p)], mine.at[k, piece(p)], load_sem.at[k, p])

    def second_copy(k, p):
        peer = ((a + lines - k) % lines) * pair + b
        slot = lines + k - 1
        return push(sums.at[k - 1, piece(p)], landed.at[k - 1, piece(p)], send_sem.at[slot, p], recv_sem.at[slot, p], peer)

    def x_copy(j):
        cols = pl.ds(pl.multiple_of(j % tiles * tile, tile), tile)
        return pltpu.make_async_copy(x.at[j // tiles, :, cols], x_buf.at[j % 2], x_sem.at[j % 2])

    def g_copies(e):
        return [
            pltpu.make_async_copy(g.at[e], g_buf.at[e % 2, i], g_sem.at[e % 2, i]) for i, g in enumerate((first, second))
        ]

    def o_copies(j):
        place = pl.ds(pl.multiple_of(j % tiles * tile, tile), tile)
        return [
            pltpu.make_async_copy(o_buf.at[j % 2, i], o.at[j // tiles, place, :], o_sem.at[j % 2, i])
            for i, o in enumerate(terms)
        ]

    for k in list(range(1, lines)) + [0]:
        for p in range(pieces):
            first_copy(k, p).start()
            load(k, p).start()
    x_copy(0).start()
    for copy in g_copies(0):
        copy.start()

    def add(k, p):
        first_copy(k, p).wait_recv()
        load(k, p).wait()
        return mine[k, piece(p)].astype(jnp.float32) + got[k, piece(p)].astype(jnp.float32)

    def step(s):
        k, p = 1 + s // pieces, s % pieces
        sums[k - 1, piece(p)] = add(k, p).astype(jnp.bfloat16)
        second_copy(k, p).start()

    def job(j):
        @pl.when(j + 1 < jobs)
        def _():
            x_copy(j + 1).start()

        @pl.when(j % tiles == 0)
        def _():
            for copy in g_copies(j // tiles):
                copy.wait()

            @pl.when(j // tiles + 1 < experts)
            def _():
                for copy in g_copies(j // tiles + 1):
                    copy.start()

        @pl.when(j >= 2)
        def _():
            for copy in o_copies(j - 2):
                copy.wait()

        x_copy(j).wait()
        for i in range(2):
            o_buf[j % 2, i] = down_rows(x_buf[j % 2], g_buf[j // tiles % 2, i]).astype(jnp.bfloat16)
        for copy in o_copies(j):
            copy.start()

    steps = (lines - 1) * pieces
    per = steps * 2 // jobs

    def both(t, _):
        for i in range(per):
            step(t * per + i)
            if i == 0:
                job(2 * t)
            if i == per - 1:
                job(2 * t + 1)
        return 0

    lax.fori_loop(0, jobs // 2, both, 0)
    for copy in o_copies(jobs - 2) + o_copies(jobs - 1):
        copy.wait()

    def finish(p, _):
        total = add(0, p)
        for k in range(1, lines):
            second_copy(k, p).wait_recv()
            total += landed[k - 1, piece(p)].astype(jnp.float32)
        out[piece(p), :] = total
        return 0

    lax.fori_loop(0, pieces, finish, 0)
    for p in range(pieces):
        for k in range(lines):
            first_copy(k, p).wait_send()
        for k in range(1, lines):
            second_copy(k, p).wait_send()


def reduce_terms(part, x, first, second, n, pieces, tile, collective_id):
    _, rows, width = part.shape
    experts, tokens, _ = x.shape
    hidden = first.shape[2]
    lines = n // 2
    slots = lines + lines - 1
    hbm = pl.BlockSpec(memory_space=ANY)
    term = jax.ShapeDtypeStruct((experts, width, hidden), jnp.bfloat16)
    return pl.pallas_call(
        functools.partial(reduce_terms_kernel, n, pieces, tile),
        out_shape=(jax.ShapeDtypeStruct((rows, width), jnp.float32), term, term),
        in_specs=[hbm] * 4,
        out_specs=[pl.BlockSpec(memory_space=pltpu.VMEM), hbm, hbm],
        scratch_shapes=[
            pltpu.VMEM((lines, rows, width), jnp.bfloat16),
            pltpu.VMEM((lines, rows, width), jnp.bfloat16),
            pltpu.VMEM((lines - 1, rows, width), jnp.bfloat16),
            pltpu.VMEM((lines - 1, rows, width), jnp.bfloat16),
            pltpu.VMEM((2, tokens, tile), jnp.bfloat16),
            pltpu.VMEM((2, 2, tokens, hidden), jnp.bfloat16),
            pltpu.VMEM((2, 2, tile, hidden), jnp.bfloat16),
            pltpu.SemaphoreType.DMA((slots, pieces)),
            pltpu.SemaphoreType.DMA((slots, pieces)),
            pltpu.SemaphoreType.DMA((lines, pieces)),
            pltpu.SemaphoreType.DMA((2,)),
            pltpu.SemaphoreType.DMA((2, 2)),
            pltpu.SemaphoreType.DMA((2, 2)),
        ],
        compiler_params=pltpu.CompilerParams(
            collective_id=collective_id, has_side_effects=True, vmem_limit_bytes=50 << 20
        ),
        cost_estimate=work(105),
        name="reduce_terms",
    )(part, x, first, second)


def finish_kernel(
    n, groups, pieces, part, head, wide, tokens, mid_grad, gains, gain_term, own_gains,
    tokens_grad, q_out, k_out, v_out, o_out, gain_out,
    mine, got, sums, landed, head_own, head_land, head_pair, head_far, wide_own, wide_land, wide_pair, wide_far,
    head_sum, head_got, gain_acc, gain_send, gain_got, gain_sum, gain_far,
    send_sem, recv_sem, load_sem, near_send, near_recv, near_load, far_send, far_recv,
    swap_send, swap_recv, gain_sends, gain_recvs, side_sends, side_recvs
):
    pair = 2
    lines = n // pair
    chips = groups // 2
    me, group = lax.axis_index("seq"), lax.axis_index("fsdp")
    a, b = me // pair, me % pair
    chip, parity = group // 2, group % 2
    across = a * pair + (1 - b)
    peers = [(me + k) % n for k in range(1, n)]
    mates = [(group + k) % groups for k in range(1, groups)]
    barrier = pltpu.get_barrier_semaphore()
    for peer in peers:
        pl.semaphore_signal(barrier, inc=1, device_id={"seq": peer}, device_id_type=MESH)
    for mate in mates:
        pl.semaphore_signal(barrier, inc=1, device_id={"fsdp": mate}, device_id_type=MESH)
    pl.semaphore_wait(barrier, n - 1 + groups - 1)
    rows = tokens_grad.shape[0] // pieces
    bf, f32 = jnp.bfloat16, jnp.float32

    def piece(p):
        return pl.ds(pl.multiple_of(p * rows, rows), rows)

    def first_copy(k, p):
        there = ((a + lines - k) % lines) * pair + 1 - b
        return push(part.at[there, piece(p)], got.at[k, piece(p)], send_sem.at[k, p], recv_sem.at[k, p], across)

    def load(k, p):
        here = ((a + lines - k) % lines) * pair + b
        return pltpu.make_async_copy(part.at[here, piece(p)], mine.at[k, piece(p)], load_sem.at[k, p])

    def second_copy(k, p):
        peer = ((a + lines - k) % lines) * pair + b
        slot = lines + k - 1
        return push(sums.at[k - 1, piece(p)], landed.at[k - 1, piece(p)], send_sem.at[slot, p], recv_sem.at[slot, p], peer)

    def to_group(src, dst, send, recv, mate):
        return pltpu.make_async_remote_copy(
            src_ref=src, dst_ref=dst, send_sem=send, recv_sem=recv, device_id={"fsdp": mate}, device_id_type=MESH)

    both = ((head, head_own, head_land, head_pair, head_far), (wide, wide_own, wide_land, wide_pair, wide_far))

    def near_copy(i, c):
        src, _, dst, _, _ = both[i]
        return to_group(
            src.at[2 * c + 1 - parity], dst.at[c], near_send.at[i, c], near_recv.at[i, c], 2 * chip + 1 - parity)

    def near_own(i, c):
        return pltpu.make_async_copy(both[i][0].at[2 * c + parity], both[i][1].at[c], near_load.at[i, c])

    def far_copy(i, k):
        dest = (chip + k) % chips
        return to_group(
            both[i][3].at[dest], both[i][4].at[k - 1], far_send.at[i, k - 1], far_recv.at[i, k - 1], 2 * dest + parity)

    for i in range(2):
        for c in range(chips):
            near_copy(i, c).start()
            near_own(i, c).start()
    for k in list(range(1, lines)) + [0]:
        for p in range(pieces):
            first_copy(k, p).start()
            load(k, p).start()
    for i in range(2):
        _, own, land, pairs, _ = both[i]
        for c in range(chips):
            near_own(i, c).wait()
            near_copy(i, c).wait_recv()
            pairs[c] = (own[c].astype(f32) + land[c].astype(f32)).astype(bf)
        for k in range(1, chips):
            far_copy(i, k).start()

    def add(k, p):
        first_copy(k, p).wait_recv()
        load(k, p).wait()
        return mine[k, piece(p)].astype(f32) + got[k, piece(p)].astype(f32)

    def step(s, _):
        k, p = 1 + s // pieces, s % pieces
        sums[k - 1, piece(p)] = add(k, p).astype(bf)
        second_copy(k, p).start()
        return 0

    lax.fori_loop(0, (lines - 1) * pieces, step, 0)

    def joined(i):
        _, own, land, _, far = both[i]
        total = own[chip].astype(f32) + land[chip].astype(f32)
        for k in range(1, chips):
            far_copy(i, k).wait_recv()
            total = total + far[k - 1].astype(f32)
        return total

    head_sum[...] = joined(0).astype(bf)
    o_out[...] = joined(1)
    count = o_out.shape[0]

    def swap(k):
        place = pl.ds(pl.multiple_of(peers[k - 1] * count, count), count)
        return push(head_sum.at[place], head_got.at[me], swap_send.at[k - 1], swap_recv.at[k - 1], peers[k - 1])

    for k in range(1, n):
        swap(k).start()
    head_got[me] = head_sum[pl.ds(pl.multiple_of(me * count, count), count), :]
    gain_acc[...] = jnp.zeros_like(gain_acc)

    def finish(p, _):
        total = add(0, p)
        for k in range(1, lines):
            second_copy(k, p).wait_recv()
            total += landed[k - 1, piece(p)].astype(f32)
        x = tokens[piece(p), :].astype(f32)
        factor = lax.rsqrt(jnp.mean(x * x, axis=-1, keepdims=True) + epsilon)
        normal = x * factor
        gain_acc[...] += jnp.sum(total * normal, axis=0, keepdims=True)
        weighted = total * gains[0:1, :]
        back = factor * (weighted - normal * jnp.mean(weighted * normal, axis=-1, keepdims=True))
        tokens_grad[piece(p), :] = mid_grad[piece(p), :] + back
        return 0

    lax.fori_loop(0, pieces, finish, 0)
    span = own_gains.shape[1]
    gain_send[...] = jnp.zeros_like(gain_send)
    for s in range(n):
        gain_send[s, 0:1, :] = gain_acc[:, s * span : (s + 1) * span]
        gain_send[s, 1:2, :] = gain_term[:, s * span : (s + 1) * span]

    def gain_copy(k):
        return push(
            gain_send.at[peers[k - 1]], gain_got.at[k - 1], gain_sends.at[k - 1], gain_recvs.at[k - 1], peers[k - 1])

    def gain_side(k):
        return to_group(gain_sum, gain_far.at[k - 1], side_sends.at[k - 1], side_recvs.at[k - 1], mates[k - 1])

    for k in range(1, n):
        gain_copy(k).start()
    for k in range(1, n):
        swap(k).wait_recv()
    for s in range(n):
        for i, o in enumerate((q_out, k_out, v_out)):
            o[:, s * span : (s + 1) * span] = head_got[s, :, i * span : (i + 1) * span].astype(f32)
    total = gain_send[me] + own_gains[...]
    for k in range(1, n):
        gain_copy(k).wait_recv()
        total = total + gain_got[k - 1]
    gain_sum[...] = total
    for k in range(1, groups):
        gain_side(k).start()
    for k in range(1, groups):
        gain_side(k).wait_recv()
        total = total + gain_far[k - 1]
    gain_out[...] = total
    for p in range(pieces):
        for k in range(lines):
            first_copy(k, p).wait_send()
        for k in range(1, lines):
            second_copy(k, p).wait_send()
    for i in range(2):
        for c in range(chips):
            near_copy(i, c).wait_send()
        for k in range(1, chips):
            far_copy(i, k).wait_send()
    for k in range(1, n):
        swap(k).wait_send()
        gain_copy(k).wait_send()
    for k in range(1, groups):
        gain_side(k).wait_send()


def finish_rows(part, head, wide, tokens, mid_grad, gains, gain_term, own_gains, n, groups, pieces, collective_id):
    _, rows, width = part.shape
    _, blocks, outs = head.shape
    count = blocks // n
    lines, chips = n // 2, groups // 2
    slots = lines + lines - 1
    hbm = pl.BlockSpec(memory_space=ANY)
    vmem = pl.BlockSpec(memory_space=pltpu.VMEM)
    f32, bf = jnp.float32, jnp.bfloat16
    grad = jax.ShapeDtypeStruct((count, n * outs // 3), f32)
    cell = own_gains.shape
    far = max(1, chips - 1)
    dma = pltpu.SemaphoreType.DMA
    return pl.pallas_call(
        functools.partial(finish_kernel, n, groups, pieces),
        out_shape=(
            jax.ShapeDtypeStruct((rows, width), f32),
            grad, grad, grad,
            jax.ShapeDtypeStruct((count, wide.shape[2]), f32),
            jax.ShapeDtypeStruct(cell, f32),
        ),
        in_specs=[hbm] * 3 + [vmem] * 5,
        out_specs=[vmem] * 6,
        scratch_shapes=[
            pltpu.VMEM((lines, rows, width), bf),
            pltpu.VMEM((lines, rows, width), bf),
            pltpu.VMEM((lines - 1, rows, width), bf),
            pltpu.VMEM((lines - 1, rows, width), bf),
            pltpu.VMEM((chips, blocks, outs), bf),
            pltpu.VMEM((chips, blocks, outs), bf),
            pltpu.VMEM((chips, blocks, outs), bf),
            pltpu.VMEM((far, blocks, outs), bf),
            pltpu.VMEM((chips, count, wide.shape[2]), bf),
            pltpu.VMEM((chips, count, wide.shape[2]), bf),
            pltpu.VMEM((chips, count, wide.shape[2]), bf),
            pltpu.VMEM((far, count, wide.shape[2]), bf),
            pltpu.VMEM((blocks, outs), bf),
            pltpu.VMEM((n, count, outs), bf),
            pltpu.VMEM((1, width), f32),
            pltpu.VMEM((n,) + cell, f32),
            pltpu.VMEM((n - 1,) + cell, f32),
            pltpu.VMEM(cell, f32),
            pltpu.VMEM((groups - 1,) + cell, f32),
            dma((slots, pieces)), dma((slots, pieces)), dma((lines, pieces)),
            dma((2, chips)), dma((2, chips)), dma((2, chips)), dma((2, far)), dma((2, far)),
            dma((n - 1,)), dma((n - 1,)), dma((n - 1,)), dma((n - 1,)), dma((groups - 1,)), dma((groups - 1,)),
        ],
        compiler_params=pltpu.CompilerParams(
            collective_id=collective_id, has_side_effects=True, vmem_limit_bytes=50 << 20
        ),
        cost_estimate=work(110),
        name="finish_rows",
    )(part, head, wide, tokens, mid_grad, gains, gain_term, own_gains)


def slots_of(w, experts, capacity):
    tokens = w.shape[1]
    taken = w > 0
    before = lax.broadcasted_iota(jnp.int32, (tokens, tokens), 0) <= lax.broadcasted_iota(jnp.int32, (tokens, tokens), 1)
    rank = jnp.dot(
        taken.astype(jnp.float32).astype(jnp.bfloat16), before.astype(jnp.float32).astype(jnp.bfloat16),
        preferred_element_type=jnp.float32,
    )
    rank = jnp.where(taken, rank - 1.0, -1.0)
    slot = lax.broadcasted_iota(jnp.int32, (capacity, tokens), 0).astype(jnp.float32)
    hits, weights = [], []
    for e in range(experts):
        hit = slot == rank[e : e + 1, :]
        hits.append(hit.astype(jnp.float32).astype(jnp.bfloat16))
        weights.append(jnp.sum(jnp.where(hit, w[e : e + 1, :], 0.0), axis=1, keepdims=True))
    return jnp.concatenate(hits, axis=0), weights


def place_kernel(experts, w_ref, x_ref, o_ref, s_ref):
    capacity = o_ref.shape[1]
    hits, weights = slots_of(w_ref[0], experts, capacity)
    out = jnp.dot(hits, x_ref[0], preferred_element_type=jnp.float32)
    for e in range(experts):
        o_ref[e] = out[e * capacity : (e + 1) * capacity].astype(jnp.bfloat16)
        s_ref[e] = weights[e]


def place(weights, x, experts, capacity):
    n, tokens, width = x.shape
    return pl.pallas_call(
        functools.partial(place_kernel, experts),
        grid=(n,),
        out_shape=(
            jax.ShapeDtypeStruct((experts, n * capacity, width), x.dtype),
            jax.ShapeDtypeStruct((experts, n * capacity, 1), jnp.float32),
        ),
        in_specs=[
            pl.BlockSpec((1, 8, tokens), lambda c: (c, 0, 0)),
            pl.BlockSpec((1, tokens, width), lambda c: (c, 0, 0)),
        ],
        out_specs=[
            pl.BlockSpec((experts, capacity, width), lambda c: (0, c, 0)),
            pl.BlockSpec((experts, capacity, 1), lambda c: (0, c, 0)),
        ],
        cost_estimate=work(10),
        name="place",
    )(weights, x)


def place_weighted_kernel(experts, w_ref, *refs):
    pieces, o_ref, x_buf = refs[:-2], refs[-2], refs[-1]
    capacity = o_ref.shape[1]
    half = pieces[0].shape[0]
    for k in range(len(pieces) // 2):

        @pl.when(pl.program_id(0) == k)
        def _():
            x_buf[:half] = pieces[2 * k][...]
            x_buf[half:] = pieces[2 * k + 1][...]

    hits, weights = slots_of(w_ref[0], experts, capacity)
    out = jnp.dot(hits, x_buf[...], preferred_element_type=jnp.float32)
    for e in range(experts):
        o_ref[e] = (out[e * capacity : (e + 1) * capacity] * weights[e]).astype(jnp.bfloat16)


def place_weighted(weights, pieces, experts, capacity):
    n, _, tokens = weights.shape
    half, width = pieces[0].shape
    return pl.pallas_call(
        functools.partial(place_weighted_kernel, experts),
        grid=(n,),
        out_shape=jax.ShapeDtypeStruct((experts, n * capacity, width), pieces[0].dtype),
        in_specs=[pl.BlockSpec((1, 8, tokens), lambda c: (c, 0, 0))]
        + [pl.BlockSpec((half, width), lambda c: (0, 0), pipeline_mode=pl.Buffered(1))] * len(pieces),
        out_specs=pl.BlockSpec((experts, capacity, width), lambda c: (0, c, 0)),
        scratch_shapes=[pltpu.VMEM((2 * half, width), pieces[0].dtype)],
        cost_estimate=work(12),
        name="place_weighted",
    )(weights, *pieces)


def unplace_kernel(experts, w_ref, y_ref, o_ref):
    capacity, width = y_ref.shape[1:]
    hits, _ = slots_of(w_ref[0], experts, capacity)
    o_ref[0] = down_rows(hits, y_ref[...].reshape(experts * capacity, width)).astype(o_ref.dtype)


def unplace(weights, y, capacity):
    n, _, tokens = weights.shape
    experts, _, width = y.shape
    return pl.pallas_call(
        functools.partial(unplace_kernel, experts),
        grid=(n,),
        out_shape=jax.ShapeDtypeStruct((n, tokens, width), y.dtype),
        in_specs=[
            pl.BlockSpec((1, 8, tokens), lambda c: (c, 0, 0)),
            pl.BlockSpec((experts, capacity, width), lambda c: (0, c, 0)),
        ],
        out_specs=pl.BlockSpec((1, tokens, width), lambda c: (c, 0, 0)),
        cost_estimate=work(10),
        name="unplace",
    )(weights, y)


def unplace_split_kernel(experts, w_ref, y_ref, *outs):
    capacity, width = y_ref.shape[1:]
    hits, _ = slots_of(w_ref[0], experts, capacity)
    out = down_rows(hits, y_ref[...].reshape(experts * capacity, width)).astype(y_ref.dtype)
    for k, o_ref in enumerate(outs):

        @pl.when(pl.program_id(0) == k)
        def _():
            o_ref[...] = out


def unplace_split(weights, y, capacity):
    n, _, tokens = weights.shape
    experts, _, width = y.shape
    return pl.pallas_call(
        functools.partial(unplace_split_kernel, experts),
        grid=(n,),
        out_shape=[jax.ShapeDtypeStruct((tokens, width), y.dtype)] * n,
        in_specs=[
            pl.BlockSpec((1, 8, tokens), lambda c: (c, 0, 0)),
            pl.BlockSpec((experts, capacity, width), lambda c: (0, c, 0)),
        ],
        out_specs=[pl.BlockSpec((tokens, width), lambda c: (0, 0))] * n,
        compiler_params=pltpu.CompilerParams(vmem_limit_bytes=40 << 20),
        cost_estimate=work(12),
        name="unplace_split",
    )(weights, y)


def widen_kernel(x_ref, o_ref):
    for e in range(x_ref.shape[0]):
        o_ref[:, e, :] = x_ref[e].astype(jnp.float32)


def widen(x):
    experts, rows, columns = x.shape
    step = min(256, rows)
    return pl.pallas_call(
        widen_kernel,
        grid=(rows // step,),
        out_shape=jax.ShapeDtypeStruct((rows, experts, columns), jnp.float32),
        in_specs=[pl.BlockSpec((experts, step, columns), lambda i: (0, i, 0))],
        out_specs=pl.BlockSpec((step, experts, columns), lambda i: (i, 0, 0)),
        cost_estimate=work(5),
        name="widen",
    )(x)


def masked(block):
    keys = lax.broadcasted_iota(jnp.int32, (block, block), 0)
    rows = lax.broadcasted_iota(jnp.int32, (block, block), 1)
    return keys <= rows


def across_lanes(a, b):
    return lax.dot_general(a, b, (((1,), (1,)), ((), ())), preferred_element_type=jnp.float32)


def down_rows(a, b):
    return lax.dot_general(a, b, (((0,), (0,)), ((), ())), preferred_element_type=jnp.float32)


LOG2E = 1.4426950408889634


def attend_kernel(block, scale, q_ref, k_ref, v_ref, o_ref, lse_ref, s_ref, acc_ref):
    length, _ = q_ref.shape

    def rows(i):
        return pl.ds(pl.multiple_of(i * block, block), block)

    def one_block(i, _):
        q = q_ref[rows(i), :]
        diag = across_lanes(k_ref[rows(i), :], q) * (scale * LOG2E)
        diag = jnp.where(masked(block), diag, -1e30)
        s_ref[rows(i), :] = diag
        peak = jnp.max(diag, axis=0, keepdims=True)

        def score(j, peak):
            s = across_lanes(k_ref[rows(j), :], q) * (scale * LOG2E)
            s_ref[rows(j), :] = s
            return jnp.maximum(peak, jnp.max(s, axis=0, keepdims=True))

        peak = lax.fori_loop(0, i, score, peak)
        acc_ref[...] = jnp.zeros_like(acc_ref)

        def weigh(j, total):
            p = jnp.exp2(s_ref[rows(j), :] - peak)
            acc_ref[...] += down_rows(v_ref[rows(j), :], p.astype(jnp.bfloat16))
            return total + jnp.sum(p, axis=0, keepdims=True)

        total = lax.fori_loop(0, i + 1, weigh, jnp.zeros_like(peak))
        o_ref[rows(i), :] = (acc_ref[...] / total).T.astype(o_ref.dtype)
        lse_ref[0, :, rows(i)] = peak + jnp.log2(total)
        return 0

    lax.fori_loop(0, length // block, one_block, 0)


def attend(q, k, v, heads, block, scale):
    length, width = q.shape
    dim = width // heads
    spec = pl.BlockSpec((length, dim), lambda h: (0, h))
    return pl.pallas_call(
        functools.partial(attend_kernel, block, scale),
        grid=(heads,),
        out_shape=(
            jax.ShapeDtypeStruct(q.shape, q.dtype),
            jax.ShapeDtypeStruct((heads, 1, length), jnp.float32),
        ),
        in_specs=[spec] * 3,
        out_specs=[spec, pl.BlockSpec((1, 1, length), lambda h: (h, 0, 0))],
        scratch_shapes=[
            pltpu.VMEM((length, block), jnp.float32),
            pltpu.VMEM((dim, block), jnp.float32),
        ],
        cost_estimate=work(25),
        name="attend",
    )(q, k, v)


def attend_back_kernel(
    block, scale, q_ref, k_ref, v_ref, g_ref, o_ref, lse_ref, dq_ref, dk_ref, dv_ref, dk_acc, dv_acc, dq_acc
):
    length, dim = q_ref.shape
    dk_acc[...] = jnp.zeros_like(dk_acc)
    dv_acc[...] = jnp.zeros_like(dv_acc)

    def rows(i):
        return pl.ds(pl.multiple_of(i * block, block), block)

    def one_block(i, _):
        q, g = q_ref[rows(i), :], g_ref[rows(i), :]
        lse = lse_ref[0, :, rows(i)]
        products = g.astype(jnp.float32) * o_ref[rows(i), :].astype(jnp.float32)
        shift = lax.dot_general(
            jnp.ones((8, dim), jnp.float32), products, (((1,), (1,)), ((), ())),
            precision=lax.Precision.HIGHEST, preferred_element_type=jnp.float32,
        )[:1]

        def pair(j, keep):
            k, v = k_ref[rows(j), :], v_ref[rows(j), :]
            p = jnp.exp2(across_lanes(k, q) * (scale * LOG2E) - lse)
            if keep is not None:
                p = jnp.where(keep, p, 0.0)
            ds = (p * (across_lanes(v, g) - shift) * scale).astype(jnp.bfloat16)
            dv_acc[rows(j), :] += jnp.dot(p.astype(jnp.bfloat16), g, preferred_element_type=jnp.float32)
            dk_acc[rows(j), :] += jnp.dot(ds, q, preferred_element_type=jnp.float32)
            dq_acc[...] += down_rows(k, ds)

        dq_acc[...] = jnp.zeros_like(dq_acc)
        pair(i, masked(block))

        def body(j, _):
            pair(j, None)
            return 0

        lax.fori_loop(0, i, body, 0)
        dq_ref[rows(i), :] = dq_acc[...].T.astype(dq_ref.dtype)
        return 0

    lax.fori_loop(0, length // block, one_block, 0)
    dk_ref[...] = dk_acc[...].astype(dk_ref.dtype)
    dv_ref[...] = dv_acc[...].astype(dv_ref.dtype)


def attend_back(q, k, v, g, o, lse, heads, block, scale):
    length, width = q.shape
    dim = width // heads
    spec = pl.BlockSpec((length, dim), lambda h: (0, h))
    return pl.pallas_call(
        functools.partial(attend_back_kernel, block, scale),
        grid=(heads,),
        out_shape=(jax.ShapeDtypeStruct(q.shape, q.dtype),) * 3,
        in_specs=[spec] * 5 + [pl.BlockSpec((1, 1, length), lambda h: (h, 0, 0))],
        out_specs=[spec] * 3,
        scratch_shapes=[
            pltpu.VMEM((length, dim), jnp.float32),
            pltpu.VMEM((length, dim), jnp.float32),
            pltpu.VMEM((dim, block), jnp.float32),
        ],
        cost_estimate=work(60),
        name="attend_back",
    )(q, k, v, g, o, lse)


def rows_kernel(a_ref, b_ref, wa_ref, wb_ref, o_ref):
    o_ref[0] = (across_lanes(a_ref[0], wa_ref[0]) + across_lanes(b_ref[0], wb_ref[0])).astype(o_ref.dtype)


def rows_sum(a, b, wa, wb, tile):
    experts, rows, hidden = a.shape
    width = wa.shape[1]
    rows_spec = pl.BlockSpec((1, tile, hidden), lambda e, i: (e, i, 0))
    weights = pl.BlockSpec((1, width, hidden), lambda e, i: (e, 0, 0))
    return pl.pallas_call(
        rows_kernel,
        grid=(experts, rows // tile),
        out_shape=jax.ShapeDtypeStruct((experts, rows, width), jnp.bfloat16),
        in_specs=[rows_spec] * 2 + [weights] * 2,
        out_specs=pl.BlockSpec((1, tile, width), lambda e, i: (e, i, 0)),
        compiler_params=pltpu.CompilerParams(vmem_limit_bytes=50 << 20),
        cost_estimate=work(36),
        name="rows_sum",
    )(a, b, wa, wb)


def slopes_kernel(g_ref, w_ref, gate_ref, up_ref, dg_ref, du_ref):
    back = jnp.dot(g_ref[0], w_ref[0], preferred_element_type=jnp.float32)
    gate, up = gate_ref[0].astype(jnp.float32), up_ref[0].astype(jnp.float32)
    s = jax.nn.sigmoid(gate)
    dg_ref[0] = (back * up * (s * (1.0 + gate * (1.0 - s)))).astype(dg_ref.dtype)
    du_ref[0] = (back * (gate * s)).astype(du_ref.dtype)


def slopes(g, w, gate, up, tile):
    experts, rows, width = g.shape
    hidden = w.shape[2]
    wide = pl.BlockSpec((1, tile, width), lambda e, i: (e, i, 0))
    narrow = pl.BlockSpec((1, tile, hidden), lambda e, i: (e, i, 0))
    out = jax.ShapeDtypeStruct((experts, rows, hidden), jnp.bfloat16)
    return pl.pallas_call(
        slopes_kernel,
        grid=(experts, rows // tile),
        out_shape=(out, out),
        in_specs=[wide, pl.BlockSpec((1, width, hidden), lambda e, i: (e, 0, 0)), narrow, narrow],
        out_specs=[narrow] * 2,
        compiler_params=pltpu.CompilerParams(vmem_limit_bytes=50 << 20),
        cost_estimate=work(20),
        name="slopes",
    )(g, w, gate, up)


def project_kernel(
    n, groups, pieces, own, w_query, w_key, w_value, gain_own,
    normed, proj, squares, w_ref, gains, held, send_sem, recv_sem, side_send, side_recv, copy_sem
):
    pair = 2
    lines = n // pair
    me, group = lax.axis_index("seq"), lax.axis_index("fsdp")
    a, b = me // pair, me % pair
    column = [((a + k) % lines) * pair + b for k in range(1, lines)]
    back = [((a + lines - k) % lines) * pair + b for k in range(1, lines)]
    across = a * pair + (1 - b)
    mates = [(group + k) % groups for k in range(1, groups)]
    barrier = pltpu.get_barrier_semaphore()
    for peer in column + [across]:
        pl.semaphore_signal(barrier, inc=1, device_id={"seq": peer}, device_id_type=MESH)
    for mate in mates:
        pl.semaphore_signal(barrier, inc=1, device_id={"fsdp": mate}, device_id_type=MESH)
    pl.semaphore_wait(barrier, lines + groups - 1)
    rows, _ = own.shape
    step = rows // pieces
    span = w_ref.shape[1] // 3
    shard = w_query.shape[0]

    def piece(p):
        return pl.ds(p * step, step)

    sends = []
    for p in range(pieces):
        for k in range(lines):
            peer = across if k == 0 else column[k - 1]
            copy = push(own.at[piece(p)], held.at[me, piece(p)], send_sem.at[k, p], recv_sem.at[k, p], peer)
            copy.start()
            sends.append(copy)

    shard_rows = pl.ds(pl.multiple_of(group * shard, shard), shard)
    mine = pl.ds(pl.multiple_of(me * span, span), span)
    blocks = [
        (w.at[:, mine], w_ref.at[shard_rows, part * span : (part + 1) * span])
        for part, w in enumerate((w_query, w_key, w_value))
    ]
    blocks.append((gain_own, gains.at[:, shard_rows]))
    locals_, sides = [], []

    def side_copy(i, src, dst, slot, mate):
        return pltpu.make_async_remote_copy(
            src_ref=src, dst_ref=dst, send_sem=side_send.at[i, slot], recv_sem=side_recv.at[i, slot],
            device_id={"fsdp": mate}, device_id_type=MESH)

    def side_block(i, g):
        place = pl.ds(pl.multiple_of(g * shard, shard), shard)
        return gains.at[:, place] if i == 3 else w_ref.at[place, i * span : (i + 1) * span]

    chips = groups // 2
    partner = group // 2 * 2 + 1 - group % 2
    alike = [(group + 2 * k) % groups for k in range(1, chips)]
    behind = [(group + groups - 2 * k) % groups for k in range(1, chips)]
    for i, (src, dst) in enumerate(blocks):
        for k in range(chips):
            side = side_copy(i, src, dst, k, partner if k == 0 else alike[k - 1])
            side.start()
            sides.append(side)
        local = pltpu.make_async_copy(src, dst, copy_sem.at[i])
        local.start()
        locals_.append(local)
    for k in range(1, chips):
        for i in range(4):
            block = side_block(i, behind[k - 1])
            side_copy(i, block, block, k, partner).wait_recv()
            side = side_copy(i, block, block, chips + k - 1, partner)
            side.start()
            sides.append(side)

    def project(src, chunk):
        x = chunk[...].astype(jnp.float32)
        factor = lax.rsqrt(jnp.mean(x * x, axis=-1, keepdims=True) + epsilon)
        place = pl.ds(pl.multiple_of(src * rows, rows), rows)
        normed[place, :] = (x * factor * gains[0:1, :]).astype(jnp.bfloat16)
        for part in range(3):
            cols = slice(part * span, (part + 1) * span)
            out = jnp.dot(normed[place, :], w_ref[:, cols], preferred_element_type=jnp.float32)
            proj[place, cols] = out
            if part < 2:
                sums = lax.dot_general(
                    jnp.ones((8, span), jnp.float32), out * out, (((1,), (1,)), ((), ())),
                    precision=lax.Precision.HIGHEST, preferred_element_type=jnp.float32,
                )
                squares[pl.ds(part * n + src, 1), :] = sums[:1]

    relays = []
    for p in range(pieces):
        for k in range(1, lines):
            src = back[k - 1]
            push(own.at[piece(p)], held.at[src, piece(p)], send_sem.at[k, p], recv_sem.at[k, p], across).wait_recv()
            slot = lines + k - 1
            copy = push(held.at[src, piece(p)], held.at[src, piece(p)], send_sem.at[slot, p], recv_sem.at[slot, p], across)
            copy.start()
            relays.append(copy)
    for copy in locals_:
        copy.wait()
    for i in range(4):
        for k in [0] + list(range(chips, 2 * chips - 1)):
            side_copy(i, blocks[i][0], blocks[i][1], k, partner).wait_recv()
    project(me, own)
    for p in range(pieces):
        push(own.at[piece(p)], held.at[across, piece(p)], send_sem.at[0, p], recv_sem.at[0, p], across).wait_recv()
    project(across, held.at[across])
    for k in range(1, lines):
        project(back[k - 1], held.at[back[k - 1]])
    for k in range(1, lines):
        for p in range(pieces):
            relays[p * (lines - 1) + k - 1].wait_recv()
        src = ((a + lines - k) % lines) * pair + 1 - b
        project(src, held.at[src])
    for copy in sends + relays + sides:
        copy.wait_send()


def project_rows(x, w_query, w_key, w_value, gains, n, groups, pieces, collective_id):
    rows, width = x.shape
    span = w_query.shape[1] // n
    slots = n // 2 + n // 2 - 1
    vmem = pl.BlockSpec(memory_space=pltpu.VMEM)
    hbm = pl.BlockSpec(memory_space=ANY)
    return pl.pallas_call(
        functools.partial(project_kernel, n, groups, pieces),
        out_shape=(
            jax.ShapeDtypeStruct((n * rows, width), jnp.bfloat16),
            jax.ShapeDtypeStruct((n * rows, 3 * span), jnp.float32),
            jax.ShapeDtypeStruct((2 * n, rows), jnp.float32),
            jax.ShapeDtypeStruct((width, 3 * span), jnp.bfloat16),
            jax.ShapeDtypeStruct((8, width), jnp.float32),
        ),
        in_specs=[vmem, hbm, hbm, hbm, vmem],
        out_specs=[vmem] * 5,
        scratch_shapes=[
            pltpu.VMEM((n, rows, width), jnp.bfloat16),
            pltpu.SemaphoreType.DMA((slots, pieces)),
            pltpu.SemaphoreType.DMA((slots, pieces)),
            pltpu.SemaphoreType.DMA((4, groups - 1)),
            pltpu.SemaphoreType.DMA((4, groups - 1)),
            pltpu.SemaphoreType.DMA((4,)),
        ],
        compiler_params=pltpu.CompilerParams(
            collective_id=collective_id, has_side_effects=True, vmem_limit_bytes=50 << 20
        ),
        cost_estimate=work(110),
        name="project_rows",
    )(x, w_query, w_key, w_value, gains)


def as_columns(row, lanes):
    return jnp.broadcast_to(row, (lanes, row.shape[1])).T


def turn_tables(c, near_cos, near_sin, far_cos, far_sin):
    far_c, far_s = far_cos[pl.ds(c, 1), :], far_sin[pl.ds(c, 1), :]
    cosine = near_cos[...] * far_c - near_sin[...] * far_s
    sine = near_sin[...] * far_c + near_cos[...] * far_s
    first = lax.broadcasted_iota(jnp.int32, sine.shape, 1) < sine.shape[1] // 2
    return cosine, jnp.where(first, -sine, sine)


def add_over_seq(n, own, landed, send_sem, recv_sem, peers):
    copies = []
    for k in range(1, n):
        copy = push(own, landed.at[k - 1], send_sem.at[k - 1], recv_sem.at[k - 1], peers[k - 1])
        copy.start()
        copies.append(copy)
    return copies


def rotate_kernel(
    n, full, squares, sent, proj, gains, near_cos, near_sin, far_cos, far_sin,
    queries, keys, values, factors, taken, landed, send_sem, recv_sem, copy_sem
):
    me = lax.axis_index("seq")
    peers = [(me + k) % n for k in range(1, n)]
    greet(peers)
    local = pltpu.make_async_copy(sent.at[me], taken.at[me], copy_sem)
    local.start()
    copies = add_over_seq(n, squares, landed, send_sem.at[0], recv_sem.at[0], peers)
    swaps = []
    for k in range(1, n):
        swap = push(sent.at[peers[k - 1]], taken.at[me], send_sem.at[1, k - 1], recv_sem.at[1, k - 1], peers[k - 1])
        swap.start()
        swaps.append(swap)
    span = queries.shape[1]
    rows = squares.shape[1]
    lanes = near_cos.shape[1]
    total = squares[...]
    for k in range(1, n):
        copies[k - 1].wait_recv()
        total = total + landed[k - 1]
    factors[...] = lax.rsqrt(total / full + epsilon)

    def chunk(c, _):
        place = pl.ds(pl.multiple_of(c * rows, rows), rows)
        cosine, sine = turn_tables(c, near_cos, near_sin, far_cos, far_sin)
        for part, out in ((0, queries), (1, keys)):
            factor = as_columns(factors[pl.ds(part * n + c, 1), :], lanes)
            for h in range(span // lanes):
                cols = slice(part * span + h * lanes, part * span + (h + 1) * lanes)
                x = proj[place, cols] * factor * gains[part : part + 1, h * lanes : (h + 1) * lanes]
                turned = x * cosine + pltpu.roll(x, lanes // 2, 1) * sine
                out[place, h * lanes : (h + 1) * lanes] = turned.astype(jnp.bfloat16)
        values[place, :] = proj[place, 2 * span :].astype(jnp.bfloat16)
        return 0

    lax.fori_loop(0, n, chunk, 0)
    for copy in copies:
        copy.wait_send()
    for swap in swaps:
        swap.wait()
    local.wait()


def rotate_rows(squares, sent, proj, gains, tables, n, full, collective_id):
    length, outs = proj.shape
    span = outs // 3
    vmem = pl.BlockSpec(memory_space=pltpu.VMEM)
    heads = jax.ShapeDtypeStruct((length, span), jnp.bfloat16)
    return pl.pallas_call(
        functools.partial(rotate_kernel, n, full),
        out_shape=(
            heads, heads, heads,
            jax.ShapeDtypeStruct(squares.shape, jnp.float32),
            jax.ShapeDtypeStruct(sent.shape, sent.dtype),
        ),
        in_specs=[vmem] * 8,
        out_specs=[vmem] * 5,
        scratch_shapes=[
            pltpu.VMEM((n - 1,) + squares.shape, jnp.float32),
            pltpu.SemaphoreType.DMA((2, n - 1)),
            pltpu.SemaphoreType.DMA((2, n - 1)),
            pltpu.SemaphoreType.DMA,
        ],
        compiler_params=pltpu.CompilerParams(
            collective_id=collective_id, has_side_effects=True, vmem_limit_bytes=40 << 20
        ),
        cost_estimate=work(15),
        name="rotate_rows",
    )(squares, sent, proj, gains, *tables)


def heads_back_kernel(
    n, full, dq, dk, dv, proj, factors, gains, near_cos, near_sin, far_cos, far_sin,
    grads, gain_grads, sums, landed, send_sem, recv_sem
):
    me = lax.axis_index("seq")
    peers = [(me + k) % n for k in range(1, n)]
    greet(peers)
    span = dq.shape[1]
    rows = sums.shape[1]
    lanes = near_cos.shape[1]
    count = span // lanes

    def parts(c, part, h, grad):
        place = pl.ds(pl.multiple_of(c * rows, rows), rows)
        cosine, sine = turn_tables(c, near_cos, near_sin, far_cos, far_sin)
        g = grad[place, h * lanes : (h + 1) * lanes].astype(jnp.float32)
        up = g * cosine + pltpu.roll(g * sine, lanes // 2, 1)
        factor = as_columns(factors[pl.ds(part * n + c, 1), :], lanes)
        cols = slice(part * span + h * lanes, part * span + (h + 1) * lanes)
        normal = proj[place, cols] * factor
        weighted = up * gains[part : part + 1, h * lanes : (h + 1) * lanes]
        return place, cols, up, factor, normal, weighted

    def first(c, _):
        for part, grad in ((0, dq), (1, dk)):
            products = 0.0
            for h in range(count):
                _, _, _, _, normal, weighted = parts(c, part, h, grad)
                products = products + weighted * normal
            total = lax.dot_general(
                jnp.ones((8, lanes), jnp.float32), products, (((1,), (1,)), ((), ())),
                precision=lax.Precision.HIGHEST, preferred_element_type=jnp.float32,
            )
            sums[pl.ds(part * n + c, 1), :] = total[:1]
        return 0

    lax.fori_loop(0, n, first, 0)
    copies = add_over_seq(n, sums, landed, send_sem, recv_sem, peers)
    gain_grads[...] = jnp.zeros_like(gain_grads)

    def gain_sum(c, _):
        for part, grad in ((0, dq), (1, dk)):
            for h in range(count):
                _, _, up, _, normal, _ = parts(c, part, h, grad)
                cell = (slice(part + 2, part + 3), slice(h * lanes, (h + 1) * lanes))
                gain_grads[cell] += jnp.sum(up * normal, axis=0, keepdims=True)
        place = pl.ds(pl.multiple_of(c * rows, rows), rows)
        grads[place, 2 * span :] = dv[place, :]
        return 0

    lax.fori_loop(0, n, gain_sum, 0)
    total = sums[...]
    for k in range(1, n):
        copies[k - 1].wait_recv()
        total = total + landed[k - 1]
    landed[0] = total / full

    def last(c, _):
        for part, grad in ((0, dq), (1, dk)):
            mean = as_columns(landed[0, pl.ds(part * n + c, 1), :], lanes)
            for h in range(count):
                place, cols, _, factor, normal, weighted = parts(c, part, h, grad)
                grads[place, cols] = (factor * (weighted - normal * mean)).astype(jnp.bfloat16)
        return 0

    lax.fori_loop(0, n, last, 0)
    for copy in copies:
        copy.wait_send()


def heads_back(dq, dk, dv, proj, factors, gains, tables, n, full, collective_id):
    length, span = dq.shape
    vmem = pl.BlockSpec(memory_space=pltpu.VMEM)
    return pl.pallas_call(
        functools.partial(heads_back_kernel, n, full),
        out_shape=(
            jax.ShapeDtypeStruct((length, 3 * span), jnp.bfloat16),
            jax.ShapeDtypeStruct((8, span), jnp.float32),
        ),
        in_specs=[vmem] * 10,
        out_specs=[vmem] * 2,
        scratch_shapes=[
            pltpu.VMEM(factors.shape, jnp.float32),
            pltpu.VMEM((n - 1,) + factors.shape, jnp.float32),
            pltpu.SemaphoreType.DMA((n - 1,)),
            pltpu.SemaphoreType.DMA((n - 1,)),
        ],
        compiler_params=pltpu.CompilerParams(
            collective_id=collective_id, has_side_effects=True, vmem_limit_bytes=40 << 20
        ),
        cost_estimate=work(20),
        name="heads_back",
    )(dq, dk, dv, proj, factors, gains, *tables)


def turn_parts(rows, n, dim):
    half = dim // 2
    frequency = jnp.power(10000.0, -2.0 * jnp.arange(half, dtype=jnp.float32) / dim)
    frequency = jnp.concatenate([frequency, frequency])[None]
    near = jnp.arange(rows, dtype=jnp.float32)[:, None] * frequency
    far = (rows * jnp.arange(n)).astype(jnp.float32)[:, None] * frequency
    return jnp.cos(near), jnp.sin(near), jnp.cos(far), jnp.sin(far)


def inverse_norm(values):
    return lax.rsqrt(jnp.mean(values * values, axis=-1, keepdims=True) + epsilon)


def norm_backward(values, factor, gain, upstream):
    normal = values * factor
    weighted = upstream * gain
    gain_term = jnp.sum(upstream * normal, axis=0)
    back = factor * (weighted - normal * jnp.mean(weighted * normal, axis=-1, keepdims=True))
    return (back, gain_term)


def across_pairs(lines, pair):
    return [(a * pair + b, a * pair + 1 - b) for a in range(lines) for b in range(pair)]


def along_lines(lines, pair, k):
    return [(a * pair + b, (a + k) % lines * pair + b) for a in range(lines) for b in range(pair)]


def by_place(v, n):
    lines = n // 2
    me = lax.axis_index("seq")
    a, b = me // 2, me % 2
    column = [((a + lines - k) % lines) * 2 for k in range(lines)]
    order = jnp.stack([c + b for c in column] + [c + 1 - b for c in column])
    return v[order]


def gather_column(x, n):
    lines = n // 2
    return [lax.ppermute(x, "seq", along_lines(lines, 2, k)) for k in range(1, lines)]


def gather_across(column, n):
    return [lax.ppermute(c, "seq", across_pairs(n // 2, 2)) for c in column]


def reduce_column(v, k, n):
    return lax.ppermute(v, "seq", along_lines(n // 2, 2, n // 2 - k))


def local(
    tokens, routes, route_weights, cotangent, attn_gain, query_gain, key_gain, ffn_gain,
    w_query, w_key, w_value, w_out, w_gate, w_up, w_down,
):
    n = lax.axis_size("seq")
    groups = lax.axis_size("fsdp")
    me = lax.axis_index("seq")
    width = tokens.shape[-1]
    own_tokens = tokens.reshape(-1, width)
    rows = own_tokens.shape[0]
    length = rows * n
    picks = routes.shape[-1]
    local_experts = w_gate.shape[1]
    experts = local_experts * n
    capacity = 3 * rows * picks // (2 * experts)
    head_dim = width // H
    heads = H // n
    span = heads * head_dim
    part = width // (n * groups)
    scale = head_dim ** (-0.5)
    bf, f32 = jnp.bfloat16, jnp.float32
    barrier = lax.optimization_barrier

    own_gains = jnp.stack([attn_gain, query_gain, key_gain, ffn_gain]).astype(f32)
    own_gains = jnp.pad(own_gains, ((0, 4), (0, 0)))
    full_out = lax.all_gather(w_out, "fsdp", axis=0, tiled=True)
    by_expert = lambda w: lax.all_gather(jnp.swapaxes(w, 0, 1), "fsdp", axis=1, tiled=True)
    full_gate = by_expert(w_gate)
    normed, proj, squares, w_heads, gains = project_rows(
        own_tokens, w_query, w_key, w_value, own_gains, n, groups, 8, 0
    )
    w_up, w_down, squares = barrier((w_up, w_down, squares))
    full_up, full_down = by_expert(w_up), by_expert(w_down)
    gain_ffn = gains[3]
    head_gains = lax.dynamic_slice(gains, (1, me * span), (2, span))

    expert_ids = jnp.arange(experts, dtype=jnp.int32)
    named = routes.reshape(rows, picks)[None] == expert_ids[:, None, None]
    mixing = route_weights.reshape(rows, picks)[None]
    sent = jnp.sum(jnp.where(named, mixing, 0.0), axis=-1).reshape(n, local_experts, rows)
    tables = turn_parts(rows, n, head_dim)
    queries, keys, values, factors, weights = rotate_rows(
        squares, sent, proj, head_gains, tables, n, width, 1
    )
    block = min(512, length)
    heads_out, log_totals = attend(queries, keys, values, heads, block, scale)
    context = lax.all_to_all(heads_out, "seq", split_axis=0, concat_axis=1, tiled=True)
    inputs = own_tokens.astype(f32)
    mid = inputs + jnp.dot(context, full_out, preferred_element_type=f32)
    norm_two = inverse_norm(mid)
    ffn_in = (mid * norm_two * gain_ffn).astype(bf)

    ffn_all = gather_rows(ffn_in, n, 8, False, 2)
    cot_own, ffn_all = barrier((cotangent.reshape(rows, width), ffn_all))
    half = rows // 2
    cot_halves = [cot_own[:half], cot_own[half:]]
    cot_columns = [gather_column(cot_halves[0], n)]
    cot_columns.append(gather_column(cot_halves[1], n))
    cot_others = [gather_across([v], n) for v in cot_halves]
    weights = jnp.pad(by_place(weights, n), ((0, 0), (0, 8 - local_experts), (0, 0)))
    received, slot_weight = place(weights, ffn_all, local_experts, capacity)
    gate_low = jnp.einsum("erd,edf->erf", received, full_gate, preferred_element_type=f32).astype(bf)
    cot_others[0] += gather_across(cot_columns[0], n)
    cot_others[1] += gather_across(cot_columns[1], n)
    up_part = jnp.einsum("erd,edf->erf", received, full_up, preferred_element_type=f32)
    gate = gate_low.astype(f32)
    hidden = (gate * jax.nn.sigmoid(gate) * up_part).astype(bf)
    up_low = up_part.astype(bf)
    expert_out = jnp.einsum("erf,edf->erd", hidden, full_down, preferred_element_type=f32)
    expert_out = (expert_out * slot_weight).astype(bf)
    ffn_part = unplace_split(weights, expert_out, capacity)
    ffn_part, cot_others = barrier((ffn_part, cot_others))
    cot_pieces = [
        v for pair in zip(*(([h] + c + o) for h, c, o in zip(cot_halves, cot_columns, cot_others))) for v in pair
    ]
    lines = n // 2
    ffn_got = {k: gather_across([ffn_part[lines + k]], n)[0] for k in list(range(1, lines)) + [0]}
    ffn_sum = lambda k: (ffn_part[k].astype(f32) + ffn_got[k].astype(f32)).astype(bf)

    out_grad = cotangent.reshape(rows, width).astype(f32)
    down_received = place_weighted(weights, cot_pieces, local_experts, capacity)
    down_term = jnp.einsum("erd,erf->edf", down_received, hidden, preferred_element_type=f32).astype(bf)
    gate_grad, up_grad = slopes(down_received, full_down, gate_low, up_low, 256)
    gate_grad, up_grad, got = barrier((gate_grad, up_grad, [ffn_got[k] for k in range(1, lines)]))
    ffn_got.update(zip(range(1, lines), got))
    ffn_pieces = [reduce_column(ffn_sum(k), k, n) for k in range(1, lines)]
    rows_part = unplace(weights, rows_sum(gate_grad, up_grad, full_gate, full_up, n * capacity), capacity)
    scatter = lambda v: lax.psum_scatter(v, "fsdp", scatter_dimension=1, tiled=True)
    ffn_in_grad, gate_term, up_term = reduce_terms(
        rows_part, received, gate_grad, up_grad, n, 8, 512, 4
    )
    scattered = [scatter(down_term)]
    scattered += [scatter(gate_term), scatter(up_term)]
    mid_back, ffn_gain_term = norm_backward(mid, norm_two, gain_ffn, ffn_in_grad)
    mid_grad = out_grad + mid_back
    branch_grad = mid_grad.astype(bf)

    branch_all = gather_rows(branch_grad, n, 8, True, 5).reshape(length, width)
    out_rows = lax.dynamic_slice_in_dim(full_out, me * span, span, 0)
    heads_grad = jnp.einsum("te,de->td", branch_all, out_rows, preferred_element_type=f32).astype(bf)
    out_term = jnp.einsum("td,te->de", heads_out, branch_all, preferred_element_type=f32).astype(bf)
    query_back, key_back, value_back = attend_back(
        queries, keys, values, heads_grad, heads_out, log_totals, heads, block, scale
    )
    proj_grad, gain_terms = heads_back(
        query_back, key_back, value_back, proj, factors, head_gains, tables, n, width, 6
    )
    normed_part = jnp.einsum("te,de->td", proj_grad, w_heads, preferred_element_type=f32).astype(bf)
    head_term = jnp.einsum("td,te->de", normed, proj_grad, preferred_element_type=f32).astype(bf)
    head_term = head_term.reshape(n, groups, part, 3 * span).swapaxes(0, 1)
    block_out = mid + sum(piece.astype(f32) for piece in [ffn_part[0], ffn_got[0]] + ffn_pieces)
    tokens_grad, *head_sums, out_sum, gain_sums = finish_rows(
        normed_part.reshape(n, rows, width),
        head_term.reshape(groups, n * part, 3 * span),
        out_term.reshape(groups, part, width),
        own_tokens, mid_grad, gains, ffn_gain_term[None], gain_terms, n, groups, 8, 7,
    )
    scattered, tokens_grad = barrier((scattered, tokens_grad))
    down_sum, gate_sum, up_sum = [widen(v) for v in scattered]
    gain_sums = lax.dynamic_slice_in_dim(gain_sums, lax.axis_index("fsdp") * part, part, 1)
    return (
        block_out.astype(bf).reshape(tokens.shape),
        tokens_grad.reshape(tokens.shape),
        gain_sums[0],
        gain_sums[2],
        gain_sums[3],
        gain_sums[1],
        head_sums[0],
        head_sums[1],
        head_sums[2],
        out_sum,
        gate_sum,
        up_sum,
        down_sum,
    )


def solution(mesh):
    rows3 = P("fsdp", "seq", None)
    both = P(("seq", "fsdp"))
    both2 = P(("seq", "fsdp"), None)
    placed = (rows3,) * 4 + (P("fsdp"),) * 4 + (P("fsdp", None),) * 4 + (rows3,) * 3
    return jax.shard_map(
        local,
        mesh=mesh,
        in_specs=placed,
        out_specs=(rows3,) * 2 + (both,) * 4 + (both2,) * 4 + (rows3,) * 3,
        check_vma=False,
    )
```
